8 devices in a mesh: part: 1 (over z), data: 2 (over y), seq: 4 (over x, core).
Axes of the slice: x: 2, y: 2, z: 1, core: 2. Of those that a mesh axis runs over, the one named last changes fastest.
Arguments:
- enc_out: bfloat16 [32, 96, 1024], P(('part', 'data'), 'seq')
- pred_out: bfloat16 [32, 24, 1024], P(('part', 'data'))
- w_enc: bfloat16 [1024, 640], replicated
- w_pred: bfloat16 [1024, 640], replicated
- w_out: bfloat16 [640, 1024], replicated
- labels: int32 [32, 23], P(('part', 'data'))
- frame_len: int32 [32], P(('part', 'data'))
- label_len: int32 [32], P(('part', 'data'))
Outputs:
- output 1: float32 [32], P(('part', 'data'))
- output 2: bfloat16 [32, 96, 1024], P(('part', 'data'), 'seq')
- output 3: float32 [32, 24, 1024], P(('part', 'data'))
- output 4: float32 [1024, 640], P('part')
- output 5: float32 [1024, 640], P('part')
- output 6: float32 [640, 1024], P('part')
All inputs are finite; a program needn't handle non-finite values.
Results may differ from the reference program's by a relative error of at most 0.013132.
Values are sent between devices in bfloat16 or wider.
A program may use at most 1 GiB of HBM per device.

```python
import jax
import jax.numpy as jnp
from jax import lax

H = 1024
J = 640
V = 1024
UPOS = 24
B = 32
T = 96
T_BLK = 24
LABELS = UPOS - 1
NEG_FILL = -1e30


def setup_inputs(seed: int = 0, part: int = 0) -> dict:
    key = jax.random.key(seed)
    shared = jax.random.split(key, 3)
    own = jax.random.split(jax.random.fold_in(key, part), 5)
    enc_out = jax.random.normal(own[0], (B, T, H), jnp.float32)
    pred_out = jax.random.normal(own[1], (B, UPOS, H), jnp.float32)
    w_enc = jax.random.normal(shared[0], (H, J), jnp.float32) * H ** -0.5
    w_pred = jax.random.normal(shared[1], (H, J), jnp.float32) * H ** -0.5
    w_out = jax.random.normal(shared[2], (J, V), jnp.float32) * J ** -0.5
    labels = jax.random.randint(own[2], (B, LABELS), 1, V, jnp.int32)
    frame_len = jax.random.randint(own[3], (B,), T // 4 + 1, T + 1, jnp.int32).at[0].set(T)
    label_len = jax.random.randint(own[4], (B,), max(1, LABELS // 4), LABELS + 1, jnp.int32).at[B - 1].set(LABELS)
    return {"enc_out": enc_out.astype(jnp.bfloat16), "pred_out": pred_out.astype(jnp.bfloat16), "w_enc": w_enc.astype(jnp.bfloat16), "w_pred": w_pred.astype(jnp.bfloat16), "w_out": w_out.astype(jnp.bfloat16), "labels": labels, "frame_len": frame_len, "label_len": label_len}


def joint_block(enc_blk, pred_utt, w_enc, w_pred, w_out):
    act_enc = jnp.dot(enc_blk, w_enc, preferred_element_type=jnp.float32).astype(jnp.bfloat16)
    act_pred = jnp.dot(pred_utt, w_pred, preferred_element_type=jnp.float32).astype(jnp.bfloat16)
    hidden = jnp.tanh(act_enc.astype(jnp.float32)[:, None, :] + act_pred.astype(jnp.float32)[None, :, :]).astype(jnp.bfloat16).reshape(T_BLK * UPOS, J)
    logits = jnp.dot(hidden, w_out, preferred_element_type=jnp.float32)
    return hidden, logits


def lattice_terms(enc_utt, pred_utt, lab_ids, w_enc, w_pred, w_out):
    flat_ids = jnp.tile(lab_ids, T_BLK)

    def per_blk(enc_blk):
        _, logits = joint_block(enc_blk, pred_utt, w_enc, w_pred, w_out)
        log_probs = jax.nn.log_softmax(logits, axis=-1)
        picked = jnp.take_along_axis(log_probs, flat_ids[:, None], axis=1)[:, 0]
        return log_probs[:, 0].reshape(T_BLK, UPOS), picked.reshape(T_BLK, UPOS)

    blank, label_lp = lax.map(per_blk, enc_utt)
    return blank.reshape(T, UPOS), label_lp.reshape(T, UPOS)


def lattice_loss(blank, label_lp, frame_len, label_len):
    label_pos = jnp.arange(UPOS)
    lab_cum = jnp.concatenate([jnp.zeros((B, T, 1), jnp.float32), jnp.cumsum(label_lp[:, :, :-1], axis=2)], axis=2)
    start_row = jnp.broadcast_to(jnp.where(label_pos == 0, 0.0, NEG_FILL), (B, UPOS)).astype(jnp.float32)

    def frame_step(carry, frame_in):
        blank_t, cum_t = frame_in
        alpha_t = cum_t + lax.cumlogsumexp(carry - cum_t, axis=1)
        return alpha_t + blank_t, alpha_t

    blank_tm = jnp.swapaxes(blank, 0, 1)
    _, alpha = lax.scan(frame_step, start_row, (blank_tm, jnp.swapaxes(lab_cum, 0, 1)))
    last_cell = (jnp.arange(T)[:, None, None] == frame_len[None, :, None] - 1) & (label_pos[None, None, :] == label_len[None, :, None])
    return -jnp.sum(jnp.where(last_cell, alpha + blank_tm, 0.0), axis=(0, 2))


def reference(enc_out, pred_out, w_enc, w_pred, w_out, labels, frame_len, label_len):
    lab_ids = jnp.concatenate([labels, jnp.zeros((B, 1), jnp.int32)], axis=1)
    n_blocks = T // T_BLK
    enc_blocks = enc_out.reshape(B, n_blocks, T_BLK, H)
    blank, label_lp = lax.map(lambda utt_in: lattice_terms(utt_in[0], utt_in[1], utt_in[2], w_enc, w_pred, w_out), (enc_blocks, pred_out, lab_ids))
    loss, loss_vjp = jax.vjp(lambda blank_in, label_in: lattice_loss(blank_in, label_in, frame_len, label_len), blank, label_lp)
    d_blank, d_label = loss_vjp(jnp.ones_like(loss))
    vocab_idx = jnp.arange(V)

    def per_utt(carry, utt_in):
        enc_utt, pred_utt, utt_ids, d_blank_utt, d_label_utt = utt_in
        flat_ids = jnp.tile(utt_ids, T_BLK)

        def per_blk(inner, blk_in):
            pred_acc, enc_acc, out_acc = inner
            enc_blk, d_blank_blk, d_label_blk = blk_in
            hidden, logits = joint_block(enc_blk, pred_utt, w_enc, w_pred, w_out)
            softmax_p = jax.nn.softmax(logits, axis=-1)
            blank_col = d_blank_blk.reshape(T_BLK * UPOS, 1)
            label_col = d_label_blk.reshape(T_BLK * UPOS, 1)
            grad_logits = (jnp.where(vocab_idx[None, :] == 0, blank_col, 0.0) + jnp.where(vocab_idx[None, :] == flat_ids[:, None], label_col, 0.0) - softmax_p * (blank_col + label_col)).astype(jnp.bfloat16)
            grad_hidden = jnp.dot(grad_logits, w_out.T, preferred_element_type=jnp.float32)
            grad_pre = (grad_hidden * (1.0 - jnp.square(hidden.astype(jnp.float32)))).reshape(T_BLK, UPOS, J)
            grad_act_enc = jnp.sum(grad_pre, axis=1).astype(jnp.bfloat16)
            grad_enc_blk = jnp.dot(grad_act_enc, w_enc.T, preferred_element_type=jnp.float32).astype(jnp.bfloat16)
            pred_acc = pred_acc + jnp.sum(grad_pre, axis=0)
            enc_acc = enc_acc + jnp.dot(enc_blk.T, grad_act_enc, preferred_element_type=jnp.float32)
            out_acc = out_acc + jnp.dot(hidden.T, grad_logits, preferred_element_type=jnp.float32)
            return (pred_acc, enc_acc, out_acc), grad_enc_blk

        start_acc = (jnp.zeros((UPOS, J), jnp.float32), carry[0], carry[1])
        (pred_acc, enc_acc, out_acc), grad_enc_utt = lax.scan(per_blk, start_acc, (enc_utt, d_blank_utt, d_label_utt))
        return (enc_acc, out_acc), (grad_enc_utt, pred_acc)

    acc_init = (jnp.zeros((H, J), jnp.float32), jnp.zeros((J, V), jnp.float32))
    scan_in = (enc_blocks, pred_out, lab_ids, d_blank.reshape(B, n_blocks, T_BLK, UPOS), d_label.reshape(B, n_blocks, T_BLK, UPOS))
    (grad_w_enc, grad_w_out), (grad_enc, grad_act_pred) = lax.scan(per_utt, acc_init, scan_in)
    act_pred_grad = grad_act_pred.astype(jnp.bfloat16).reshape(B * UPOS, J)
    grad_pred = jnp.dot(act_pred_grad, w_pred.T, preferred_element_type=jnp.float32).reshape(B, UPOS, H)
    grad_w_pred = jnp.dot(pred_out.reshape(B * UPOS, H).T, act_pred_grad, preferred_element_type=jnp.float32)
    return loss, grad_enc.reshape(B, T, H), grad_pred, grad_w_enc, grad_w_pred, grad_w_out
```

```python
import functools

import jax
import jax.numpy as jnp
from jax import lax
from jax.experimental import pallas as pl
from jax.experimental.pallas import tpu as pltpu
from jax.sharding import PartitionSpec as P

NEG = -1e30
LOG2E = 1.4426950408889634
LN2 = 0.6931471805599453
F32 = jnp.float32
BF16 = jnp.bfloat16
MESH = pl.DeviceIdType.MESH
VMEM_FULL = 67_000_000
N_UTT = 16
T_LOC = 24
N_UP = 24
UG = 3
N_SEQ = 4
T_ALL = T_LOC * N_SEQ
N_DIAG = T_ALL + N_UP - 1
ROWS = 8 * T_LOC


def dot(lhs, rhs, dims=((1,), (0,))):
    return lax.dot_general(lhs, rhs, (dims, ((), ())), preferred_element_type=F32)


def forward_kernel(enc, pred, w_enc, w_pred, w_out, lab, e_out, h_out, stat_out, sum_out, act_e, act_p):
    utt = pl.program_id(0)

    @pl.when(utt == 0)
    def _():
        act_e[...] = dot(enc[...], w_enc[...]).astype(BF16).astype(F32)
        act_p[...] = dot(pred[...], w_pred[...]).astype(BF16).astype(F32)
        stat_out[...] = jnp.zeros_like(stat_out)
        sum_out[...] = jnp.ones_like(sum_out)

    row = pl.multiple_of(utt * N_UP, 8)
    a_utt = act_e[pl.ds(row, T_LOC), :]
    lane = lax.broadcasted_iota(jnp.int32, (8, 128), 1)
    for ug in range(UG):
        c_grp = act_p[pl.ds(row + 8 * ug, 8), :]
        lab_grp = lab[pl.ds(row + 8 * ug, 8), :]
        pre = jnp.concatenate([a_utt[t:t + 1, :] + c_grp for t in range(T_LOC)], axis=0)
        hid = jnp.tanh(pre).astype(BF16)
        h_out[0, ug] = hid
        z = dot(hid, w_out[...])
        top = jnp.max(z, axis=1, keepdims=True)
        e = jnp.exp2((z - top) * LOG2E)
        e_out[0, ug] = e
        tot = jnp.sum(e, axis=1, keepdims=True)
        mask = jnp.concatenate([lab_grp - 128 * k == lane for k in range(z.shape[1] // 128)], axis=1)
        z3 = z.reshape(T_LOC, 8, z.shape[1])
        picked = jnp.sum(jnp.where(mask[None], z3, 0.0), axis=2, keepdims=True).reshape(ROWS, 1)
        log_tot = jnp.log2(tot)
        blank = (z[:, 0:1] - top) * LOG2E - log_tot
        label = (picked - top) * LOG2E - log_tot
        for t4 in range(T_LOC // 4):
            cur = stat_out[ug * 6 + t4]
            for k in range(4):
                rows = slice((t4 * 4 + k) * 8, (t4 * 4 + k) * 8 + 8)
                cur = jnp.where(lane == utt + 32 * k, blank[rows], cur)
                cur = jnp.where(lane == utt + 32 * k + 16, label[rows], cur)
            stat_out[ug * 6 + t4] = cur
        for t in range(T_LOC):
            sum_out[ug * T_LOC + t] = jnp.where(lane == utt, tot[t * 8:t * 8 + 8], sum_out[ug * T_LOC + t])


def joint_forward(enc, pred, w_enc, w_pred, w_out, lab):
    n_v = w_out.shape[1]
    n_j = w_out.shape[0]
    full = lambda shape: pl.BlockSpec(shape, lambda i: (0,) * len(shape), pipeline_mode=pl.Buffered(1))
    return pl.pallas_call(
        forward_kernel,
        grid=(N_UTT,),
        in_specs=[full(enc.shape), full(pred.shape), full(w_enc.shape), full(w_pred.shape), full(w_out.shape), full(lab.shape)],
        out_specs=[
            pl.BlockSpec((1, UG, ROWS, n_v), lambda i: (i, 0, 0, 0)),
            pl.BlockSpec((1, UG, ROWS, n_j), lambda i: (i, 0, 0, 0)),
            pl.BlockSpec((UG * 6, 8, 128), lambda i: (0, 0, 0)),
            pl.BlockSpec((UG * T_LOC, 8, 128), lambda i: (0, 0, 0)),
        ],
        out_shape=[
            jax.ShapeDtypeStruct((N_UTT, UG, ROWS, n_v), F32),
            jax.ShapeDtypeStruct((N_UTT, UG, ROWS, n_j), BF16),
            jax.ShapeDtypeStruct((UG * 6, 8, 128), F32),
            jax.ShapeDtypeStruct((UG * T_LOC, 8, 128), F32),
        ],
        scratch_shapes=[pltpu.VMEM((N_UTT * T_LOC, n_j), F32), pltpu.VMEM((N_UTT * N_UP, n_j), F32)],
        compiler_params=pltpu.CompilerParams(vmem_limit_bytes=VMEM_FULL),
        name="joint_forward",
    )(enc, pred, w_enc, w_pred, w_out, lab)


def lae2(x, y):
    return jnp.maximum(x, y) + jnp.log2(1.0 + jnp.exp2(-jnp.abs(x - y)))


def lattice_kernel(stat, sums, flen, llen, q0_out, q1_out, r_out, loss_out, gath, s_blank, s_label, s_alpha, s_beta, send_sem, recv_sem):
    me = lax.axis_index("seq")
    barrier = pltpu.get_barrier_semaphore()
    for off in range(1, N_SEQ):
        pl.semaphore_signal(barrier, inc=1, device_id={"seq": lax.rem(me + off, N_SEQ)}, device_id_type=MESH)
    pl.semaphore_wait(barrier, N_SEQ - 1)
    copies = []
    for off in range(1, N_SEQ):
        cp = pltpu.make_async_remote_copy(
            src_ref=stat, dst_ref=gath.at[off - 1], send_sem=send_sem.at[off - 1], recv_sem=recv_sem.at[off - 1],
            device_id={"seq": lax.rem(me + off, N_SEQ)}, device_id_type=MESH)
        cp.start()
        copies.append(cp)

    sub = lax.broadcasted_iota(jnp.int32, (8, 128), 0)
    sub24 = lax.broadcasted_iota(jnp.int32, (N_UP, 128), 0)
    tb = flen[...]
    ub = llen[...]
    n_pad = s_blank.shape[0]

    def fill(i, c):
        s_blank[pl.ds(pl.multiple_of(i * 8, 8), 8), :] = jnp.full((8, 128), NEG, F32)
        s_label[pl.ds(pl.multiple_of(i * 8, 8), 8), :] = jnp.full((8, 128), NEG, F32)
        return c

    lax.fori_loop(0, n_pad // 8, fill, 0, unroll=8)
    end_grp = [jnp.where(sub + 8 * ug == ub, 0.0, NEG) for ug in range(UG)]
    for t in range(T_ALL, T_ALL + N_UP):
        for ug in range(UG):
            s_blank[pl.ds(t * N_UP + 200 * ug, 8, stride=25), :] = end_grp[ug]

    def place(src, src_seq):
        for t4 in range(T_LOC // 4):
            for ug in range(UG):
                val = src[ug * 6 + t4]
                in_u = sub + 8 * ug <= ub
                in_l = sub + 8 * ug < ub
                for k in range(4):
                    t = src_seq * T_LOC + t4 * 4 + k
                    bl = val if k == 0 else pltpu.roll(val, 128 - 32 * k, 1)
                    la = pltpu.roll(val, 112 - 32 * k, 1)
                    ok = t < tb
                    s_blank[pl.ds(t * N_UP + 200 * ug, 8, stride=25), :] = jnp.where(ok, jnp.where(in_u, bl, NEG), end_grp[ug])
                    s_label[pl.ds(t * N_UP + 200 * ug, 8, stride=25), :] = jnp.where(ok & in_l, la, NEG)

    place(stat, me)
    for off in range(1, N_SEQ):
        copies[off - 1].wait_recv()
        place(gath.at[off - 1], lax.rem(me + N_SEQ - off, N_SEQ))

    alpha0 = jnp.where(sub24 == 0, 0.0, NEG)
    s_alpha[pl.ds(0, N_UP), :] = alpha0
    beta_end = jnp.where(sub24 == jnp.concatenate([ub] * UG, axis=0), 0.0, NEG)
    s_beta[pl.ds(N_DIAG * N_UP, N_UP), :] = beta_end
    s_beta[pl.ds((N_DIAG + 1) * N_UP, 8), :] = jnp.full((8, 128), NEG, F32)

    def wave(i, carry):
        alpha, beta = carry
        row = pl.multiple_of(i * N_UP, 8)
        x = alpha + s_blank[pl.ds(row, N_UP), :]
        y = alpha + s_label[pl.ds(row, N_UP), :]
        y = jnp.where(sub24 == 0, NEG, pltpu.roll(y, 1, 0))
        alpha = lae2(x, y)
        s_alpha[pl.ds(pl.multiple_of(row + N_UP, 8), N_UP), :] = alpha
        brow = pl.multiple_of((N_DIAG - 1 - i) * N_UP, 8)
        bx = beta + s_blank[pl.ds(brow, N_UP), :]
        by = pltpu.roll(beta, N_UP - 1, 0) + s_label[pl.ds(brow, N_UP), :]
        beta = lae2(bx, by)
        s_beta[pl.ds(brow, N_UP), :] = beta
        return alpha, beta

    _, beta = lax.fori_loop(0, N_DIAG, wave, (alpha0, beta_end), unroll=7)
    log_p = beta[0:1, :]
    loss_out[...] = jnp.broadcast_to(-LN2 * log_p, (8, 128))
    for t in range(T_LOC):
        tg = me * T_LOC + t
        for ug in range(UG):
            base = tg * N_UP + 200 * ug
            grp = lambda ref, off: ref[pl.ds(base + off, 8, stride=25), :]
            al = grp(s_alpha, 0) - log_p
            ok = (tg < tb) & (sub + 8 * ug <= ub)
            q0 = jnp.where(ok, jnp.exp2(al + grp(s_blank, 0) + grp(s_beta, 24)), 0.0)
            q1 = jnp.where(ok, jnp.exp2(al + grp(s_label, 0) + grp(s_beta, 25)), 0.0)
            idx = ug * T_LOC + t
            q0_out[idx] = q0
            q1_out[idx] = q1
            r_out[idx] = (q0 + q1) / sums[idx]
    for cp in copies:
        cp.wait_send()


def lattice(stat, sums, flen, llen):
    vm = pl.BlockSpec(memory_space=pltpu.VMEM)
    n_rows = (T_ALL + 2 * N_UP) * N_UP
    return pl.pallas_call(
        lattice_kernel,
        in_specs=[vm] * 4,
        out_specs=[vm] * 4,
        out_shape=[jax.ShapeDtypeStruct(sums.shape, F32)] * 3 + [jax.ShapeDtypeStruct((8, 128), F32)],
        scratch_shapes=[pltpu.VMEM((N_SEQ - 1,) + stat.shape, F32)] + [pltpu.VMEM((n_rows, 128), F32)] * 4
        + [pltpu.SemaphoreType.DMA((N_SEQ - 1,)), pltpu.SemaphoreType.DMA((N_SEQ - 1,))],
        compiler_params=pltpu.CompilerParams(collective_id=0, has_side_effects=True),
        name="lattice",
    )(stat, sums, flen, llen)


U_STEP = 4


def backward_kernel(e_ref, h_ref, q0_ref, q1_ref, r_ref, lab, w_out_t, da_out, dc_out, dw_out, dz_scr):
    step = pl.program_id(0)
    lane = lax.broadcasted_iota(jnp.int32, (8, 128), 1)
    n_v = w_out_t.shape[0]
    n_j = w_out_t.shape[1]
    for i in range(U_STEP):
        utt = step * U_STEP + i
        row = pl.multiple_of(utt * N_UP, 8)
        acc = None
        for ug in range(UG):
            shift = 128 - utt
            col = lambda ref: pltpu.roll(ref[ug * T_LOC:(ug + 1) * T_LOC].reshape(ROWS, 128), shift, 1)[:, 0:1].reshape(T_LOC, 8, 1)
            q0, q1, r = col(q0_ref), col(q1_ref), col(r_ref)
            lab_grp = lab[pl.ds(row + 8 * ug, 8), :]
            mask = jnp.concatenate([lab_grp - 128 * k == lane for k in range(n_v // 128)], axis=1)
            first = jnp.concatenate([lane + 128 * k == 0 for k in range(n_v // 128)], axis=1)
            e3 = e_ref[i, ug].reshape(T_LOC, 8, n_v)
            dz = e3 * r - jnp.where(mask[None], q1, 0.0) - jnp.where(first[None], q0, 0.0)
            dz = dz.reshape(ROWS, n_v).astype(BF16)
            base = (i * UG + ug) * ROWS
            dz_scr[base:base + ROWS, :] = dz
            dh = dot(dz, w_out_t[...])
            hid = h_ref[i, ug].astype(F32)
            ds = (dh * (1.0 - hid * hid)).reshape(T_LOC, 8, n_j)
            dc_out[i, ug * 8:ug * 8 + 8, :] = jnp.sum(ds, axis=0)
            acc = ds if acc is None else acc + ds
        da_out[i] = jnp.sum(acc, axis=1).astype(BF16)
    part = dot(h_ref[...].reshape(U_STEP * UG * ROWS, n_j), dz_scr[...], ((0,), (0,)))

    @pl.when(step == 0)
    def _():
        dw_out[...] = part

    @pl.when(step > 0)
    def _():
        dw_out[...] += part


def joint_backward(e, h, q0, q1, r, lab, w_out_t):
    n_v, n_j = w_out_t.shape
    full = lambda shape: pl.BlockSpec(shape, lambda i: (0,) * len(shape), pipeline_mode=pl.Buffered(1))
    return pl.pallas_call(
        backward_kernel,
        grid=(N_UTT // U_STEP,),
        in_specs=[
            pl.BlockSpec((U_STEP, UG, ROWS, n_v), lambda i: (i, 0, 0, 0)),
            pl.BlockSpec((U_STEP, UG, ROWS, n_j), lambda i: (i, 0, 0, 0)),
            full(q0.shape), full(q1.shape), full(r.shape), full(lab.shape), full(w_out_t.shape),
        ],
        out_specs=[
            pl.BlockSpec((U_STEP, T_LOC, n_j), lambda i: (i, 0, 0)),
            pl.BlockSpec((U_STEP, N_UP, n_j), lambda i: (i, 0, 0)),
            pl.BlockSpec((n_j, n_v), lambda i: (0, 0)),
        ],
        out_shape=[
            jax.ShapeDtypeStruct((N_UTT, T_LOC, n_j), BF16),
            jax.ShapeDtypeStruct((N_UTT, N_UP, n_j), F32),
            jax.ShapeDtypeStruct((n_j, n_v), F32),
        ],
        scratch_shapes=[pltpu.VMEM((U_STEP * UG * ROWS, n_v), BF16)],
        compiler_params=pltpu.CompilerParams(vmem_limit_bytes=VMEM_FULL),
        name="joint_backward",
    )(e, h, q0, q1, r, lab, w_out_t)


def solution(mesh):
    utt_rows = P(("part", "data"))
    utt_mats = P(("part", "data"), None)
    utt_cube = P(("part", "data"), None, None)
    enc_spec = P(("part", "data"), "seq", None)
    weight_in = P(None, None)
    weight_out = P("part", None)

    def body(enc_loc, pred_loc, w_enc, w_pred, w_out, labels, frame_len, label_len):
        n_h = enc_loc.shape[2]
        lab_ids = jnp.concatenate([labels, jnp.zeros((N_UTT, 1), jnp.int32)], axis=1)
        lab = jnp.broadcast_to(lab_ids.reshape(N_UTT * N_UP, 1), (N_UTT * N_UP, 128))
        enc2 = enc_loc.reshape(N_UTT * T_LOC, n_h)
        pred2 = pred_loc.reshape(N_UTT * N_UP, n_h)
        e, h, stat, sums = joint_forward(enc2, pred2, w_enc, w_pred, w_out, lab)
        lens = lambda v: jnp.broadcast_to(jnp.tile(v, 8)[None], (8, 128))
        q0, q1, r, loss = lattice(stat, sums, lens(frame_len), lens(label_len))
        da, dc, grad_w_out = joint_backward(e, h, q0, q1, r, lab, w_out.T)
        da2 = da.reshape(N_UTT * T_LOC, -1)
        grad_enc = dot(da2, w_enc, ((1,), (1,))).astype(BF16).reshape(enc_loc.shape)
        grad_w_enc = dot(enc2, da2, ((0,), (0,)))
        dc = lax.psum(dc, "seq").astype(BF16).reshape(N_UTT * N_UP, -1)
        grad_pred = dot(dc, w_pred, ((1,), (1,))).reshape(pred_loc.shape)
        grad_w_pred = dot(pred2, dc, ((0,), (0,)))
        grad_w_enc = lax.psum(grad_w_enc, ("data", "seq"))
        grad_w_out = lax.psum(grad_w_out, ("data", "seq"))
        grad_w_pred = lax.psum(grad_w_pred, "data")
        return loss[0, :N_UTT], grad_enc, grad_pred, grad_w_enc, grad_w_pred, grad_w_out

    return jax.shard_map(body, mesh=mesh, in_specs=(enc_spec, utt_cube, weight_in, weight_in, weight_in, utt_mats, utt_rows, utt_rows), out_specs=(utt_rows, enc_spec, utt_cube, weight_out, weight_out, weight_out), check_vma=False)
```

```python
import functools

import jax
import jax.numpy as jnp
from jax import lax
from jax.experimental import pallas as pl
from jax.experimental.pallas import tpu as pltpu
from jax.sharding import PartitionSpec as P

NEG = -1e30
LOG2E = 1.4426950408889634
LN2 = 0.6931471805599453
F32 = jnp.float32
BF16 = jnp.bfloat16
MESH = pl.DeviceIdType.MESH
VMEM_FULL = 67_000_000
N_UTT = 16
T_LOC = 24
N_UP = 24
UG = 3
N_SEQ = 4
T_ALL = T_LOC * N_SEQ
N_DIAG = T_ALL + N_UP - 1
ROWS = 8 * T_LOC


def dot(lhs, rhs, dims=((1,), (0,))):
    return lax.dot_general(lhs, rhs, (dims, ((), ())), preferred_element_type=F32)


def forward_kernel(enc, pred, w_enc, w_pred, w_out, lab, e_out, h_out, stat_out, sum_out, act_e, act_p):
    utt = pl.program_id(0)

    @pl.when(utt == 0)
    def _():
        act_e[...] = dot(enc[...], w_enc[...]).astype(BF16).astype(F32)
        act_p[...] = dot(pred[...], w_pred[...]).astype(BF16).astype(F32)
        stat_out[...] = jnp.zeros_like(stat_out)
        sum_out[...] = jnp.ones_like(sum_out)

    row = pl.multiple_of(utt * N_UP, 8)
    a_utt = act_e[pl.ds(row, T_LOC), :]
    lane = lax.broadcasted_iota(jnp.int32, (8, 128), 1)
    for ug in range(UG):
        c_grp = act_p[pl.ds(row + 8 * ug, 8), :]
        lab_grp = lab[pl.ds(row + 8 * ug, 8), :]
        pre = jnp.concatenate([a_utt[t:t + 1, :] + c_grp for t in range(T_LOC)], axis=0)
        hid = jnp.tanh(pre).astype(BF16)
        h_out[0, ug] = hid
        z = dot(hid, w_out[...])
        top = jnp.max(z, axis=1, keepdims=True)
        e = jnp.exp2((z - top) * LOG2E)
        e_out[0, ug] = e
        tot = jnp.sum(e, axis=1, keepdims=True)
        mask = jnp.concatenate([lab_grp - 128 * k == lane for k in range(z.shape[1] // 128)], axis=1)
        z3 = z.reshape(T_LOC, 8, z.shape[1])
        picked = jnp.sum(jnp.where(mask[None], z3, 0.0), axis=2, keepdims=True).reshape(ROWS, 1)
        log_tot = jnp.log2(tot)
        blank = (z[:, 0:1] - top) * LOG2E - log_tot
        label = (picked - top) * LOG2E - log_tot
        for t4 in range(T_LOC // 4):
            cur = stat_out[ug * 6 + t4]
            for k in range(4):
                rows = slice((t4 * 4 + k) * 8, (t4 * 4 + k) * 8 + 8)
                cur = jnp.where(lane == utt + 32 * k, blank[rows], cur)
                cur = jnp.where(lane == utt + 32 * k + 16, label[rows], cur)
            stat_out[ug * 6 + t4] = cur
        for t in range(T_LOC):
            sum_out[ug * T_LOC + t] = jnp.where(lane == utt, tot[t * 8:t * 8 + 8], sum_out[ug * T_LOC + t])


def joint_forward(enc, pred, w_enc, w_pred, w_out, lab):
    n_v = w_out.shape[1]
    n_j = w_out.shape[0]
    full = lambda shape: pl.BlockSpec(shape, lambda i: (0,) * len(shape), pipeline_mode=pl.Buffered(1))
    return pl.pallas_call(
        forward_kernel,
        grid=(N_UTT,),
        in_specs=[full(enc.shape), full(pred.shape), full(w_enc.shape), full(w_pred.shape), full(w_out.shape), full(lab.shape)],
        out_specs=[
            pl.BlockSpec((1, UG, ROWS, n_v), lambda i: (i, 0, 0, 0)),
            pl.BlockSpec((1, UG, ROWS, n_j), lambda i: (i, 0, 0, 0)),
            pl.BlockSpec((UG * 6, 8, 128), lambda i: (0, 0, 0)),
            pl.BlockSpec((UG * T_LOC, 8, 128), lambda i: (0, 0, 0)),
        ],
        out_shape=[
            jax.ShapeDtypeStruct((N_UTT, UG, ROWS, n_v), F32),
            jax.ShapeDtypeStruct((N_UTT, UG, ROWS, n_j), BF16),
            jax.ShapeDtypeStruct((UG * 6, 8, 128), F32),
            jax.ShapeDtypeStruct((UG * T_LOC, 8, 128), F32),
        ],
        scratch_shapes=[pltpu.VMEM((N_UTT * T_LOC, n_j), F32), pltpu.VMEM((N_UTT * N_UP, n_j), F32)],
        compiler_params=pltpu.CompilerParams(vmem_limit_bytes=VMEM_FULL),
        name="joint_forward",
    )(enc, pred, w_enc, w_pred, w_out, lab)


def lae2(x, y):
    return jnp.maximum(x, y) + jnp.log2(1.0 + jnp.exp2(-jnp.abs(x - y)))


def lattice_kernel(stat, sums, flen, llen, q0_out, q1_out, r_out, loss_out, gath, s_blank, s_label, s_alpha, s_beta, send_sem, recv_sem):
    me = lax.axis_index("seq")
    barrier = pltpu.get_barrier_semaphore()
    for off in range(1, N_SEQ):
        pl.semaphore_signal(barrier, inc=1, device_id={"seq": lax.rem(me + off, N_SEQ)}, device_id_type=MESH)
    pl.semaphore_wait(barrier, N_SEQ - 1)
    copies = []
    for off in range(1, N_SEQ):
        cp = pltpu.make_async_remote_copy(
            src_ref=stat, dst_ref=gath.at[off - 1], send_sem=send_sem.at[off - 1], recv_sem=recv_sem.at[off - 1],
            device_id={"seq": lax.rem(me + off, N_SEQ)}, device_id_type=MESH)
        cp.start()
        copies.append(cp)

    sub = lax.broadcasted_iota(jnp.int32, (8, 128), 0)
    sub24 = lax.broadcasted_iota(jnp.int32, (N_UP, 128), 0)
    tb = flen[...]
    ub = llen[...]
    n_pad = s_blank.shape[0]

    def fill(i, c):
        s_blank[pl.ds(pl.multiple_of(i * 8, 8), 8), :] = jnp.full((8, 128), NEG, F32)
        s_label[pl.ds(pl.multiple_of(i * 8, 8), 8), :] = jnp.full((8, 128), NEG, F32)
        return c

    lax.fori_loop(0, n_pad // 8, fill, 0, unroll=8)
    end_grp = [jnp.where(sub + 8 * ug == ub, 0.0, NEG) for ug in range(UG)]
    for t in range(T_ALL, T_ALL + N_UP):
        for ug in range(UG):
            s_blank[pl.ds(t * N_UP + 200 * ug, 8, stride=25), :] = end_grp[ug]

    def place(src, src_seq):
        for t4 in range(T_LOC // 4):
            for ug in range(UG):
                val = src[ug * 6 + t4]
                in_u = sub + 8 * ug <= ub
                in_l = sub + 8 * ug < ub
                for k in range(4):
                    t = src_seq * T_LOC + t4 * 4 + k
                    bl = val if k == 0 else pltpu.roll(val, 128 - 32 * k, 1)
                    la = pltpu.roll(val, 112 - 32 * k, 1)
                    ok = t < tb
                    s_blank[pl.ds(t * N_UP + 200 * ug, 8, stride=25), :] = jnp.where(ok, jnp.where(in_u, bl, NEG), end_grp[ug])
                    s_label[pl.ds(t * N_UP + 200 * ug, 8, stride=25), :] = jnp.where(ok & in_l, la, NEG)

    place(stat, me)
    for off in range(1, N_SEQ):
        copies[off - 1].wait_recv()
        place(gath.at[off - 1], lax.rem(me + N_SEQ - off, N_SEQ))

    alpha0 = jnp.where(sub24 == 0, 0.0, NEG)
    s_alpha[pl.ds(0, N_UP), :] = alpha0
    beta_end = jnp.where(sub24 == jnp.concatenate([ub] * UG, axis=0), 0.0, NEG)
    s_beta[pl.ds(N_DIAG * N_UP, N_UP), :] = beta_end
    s_beta[pl.ds((N_DIAG + 1) * N_UP, 8), :] = jnp.full((8, 128), NEG, F32)

    def wave(i, carry):
        alpha, beta = carry
        row = pl.multiple_of(i * N_UP, 8)
        x = alpha + s_blank[pl.ds(row, N_UP), :]
        y = alpha + s_label[pl.ds(row, N_UP), :]
        y = jnp.where(sub24 == 0, NEG, pltpu.roll(y, 1, 0))
        alpha = lae2(x, y)
        s_alpha[pl.ds(pl.multiple_of(row + N_UP, 8), N_UP), :] = alpha
        brow = pl.multiple_of((N_DIAG - 1 - i) * N_UP, 8)
        bx = beta + s_blank[pl.ds(brow, N_UP), :]
        by = pltpu.roll(beta, N_UP - 1, 0) + s_label[pl.ds(brow, N_UP), :]
        beta = lae2(bx, by)
        s_beta[pl.ds(brow, N_UP), :] = beta
        return alpha, beta

    _, beta = lax.fori_loop(0, N_DIAG, wave, (alpha0, beta_end), unroll=7)
    log_p = beta[0:1, :]
    loss_out[...] = jnp.broadcast_to(-LN2 * log_p, (8, 128))
    for t in range(T_LOC):
        tg = me * T_LOC + t
        for ug in range(UG):
            base = tg * N_UP + 200 * ug
            grp = lambda ref, off: ref[pl.ds(base + off, 8, stride=25), :]
            al = grp(s_alpha, 0) - log_p
            ok = (tg < tb) & (sub + 8 * ug <= ub)
            q0 = jnp.where(ok, jnp.exp2(al + grp(s_blank, 0) + grp(s_beta, 24)), 0.0)
            q1 = jnp.where(ok, jnp.exp2(al + grp(s_label, 0) + grp(s_beta, 25)), 0.0)
            idx = ug * T_LOC + t
            q0_out[idx] = q0
            q1_out[idx] = q1
            r_out[idx] = (q0 + q1) / sums[idx]
    for cp in copies:
        cp.wait_send()


def lattice(stat, sums, flen, llen):
    vm = pl.BlockSpec(memory_space=pltpu.VMEM)
    n_rows = (T_ALL + 2 * N_UP) * N_UP
    return pl.pallas_call(
        lattice_kernel,
        in_specs=[vm] * 4,
        out_specs=[vm] * 4,
        out_shape=[jax.ShapeDtypeStruct(sums.shape, F32)] * 3 + [jax.ShapeDtypeStruct((8, 128), F32)],
        scratch_shapes=[pltpu.VMEM((N_SEQ - 1,) + stat.shape, F32)] + [pltpu.VMEM((n_rows, 128), F32)] * 4
        + [pltpu.SemaphoreType.DMA((N_SEQ - 1,)), pltpu.SemaphoreType.DMA((N_SEQ - 1,))],
        compiler_params=pltpu.CompilerParams(collective_id=0, has_side_effects=True),
        name="lattice",
    )(stat, sums, flen, llen)


U_STEP = 4


def backward_kernel(e_ref, h_ref, q0_ref, q1_ref, r_ref, lab, w_out_t, enc, da_out, dc_out, dw_out, dz_scr, da_all):
    step = pl.program_id(0)
    lane = lax.broadcasted_iota(jnp.int32, (8, 128), 1)
    n_v = w_out_t.shape[0]
    n_j = w_out_t.shape[1]
    for i in range(U_STEP):
        utt = step * U_STEP + i
        row = pl.multiple_of(utt * N_UP, 8)
        acc = None
        for ug in range(UG):
            shift = 128 - utt
            col = lambda ref: pltpu.roll(ref[ug * T_LOC:(ug + 1) * T_LOC].reshape(ROWS, 128), shift, 1)[:, 0:1].reshape(T_LOC, 8, 1)
            q0, q1, r = col(q0_ref), col(q1_ref), col(r_ref)
            lab_grp = lab[pl.ds(row + 8 * ug, 8), :]
            mask = jnp.concatenate([lab_grp - 128 * k == lane for k in range(n_v // 128)], axis=1)
            first = jnp.concatenate([lane + 128 * k == 0 for k in range(n_v // 128)], axis=1)
            e3 = e_ref[i, ug].reshape(T_LOC, 8, n_v)
            dz = e3 * r - jnp.where(mask[None], q1, 0.0) - jnp.where(first[None], q0, 0.0)
            dz = dz.reshape(ROWS, n_v).astype(BF16)
            base = (i * UG + ug) * ROWS
            dz_scr[base:base + ROWS, :] = dz
            dh = dot(dz, w_out_t[...])
            hid = h_ref[i, ug].astype(F32)
            ds = (dh * (1.0 - hid * hid)).reshape(T_LOC, 8, n_j)
            dc_out[i, ug * 8:ug * 8 + 8, :] = jnp.sum(ds, axis=0)
            acc = ds if acc is None else acc + ds
        da = jnp.sum(acc, axis=1).astype(BF16)
        da_out[i] = da
        da_all[pl.ds(pl.multiple_of(step * U_STEP * T_LOC, 16) + i * T_LOC, T_LOC), :] = da.astype(F32)
    part = dot(h_ref[...].reshape(U_STEP * UG * ROWS, n_j), dz_scr[...], ((0,), (0,)))

    @pl.when(step == 0)
    def _():
        dw_out[n_j:, :] = part

    @pl.when(step > 0)
    def _():
        dw_out[n_j:, :] += part

    @pl.when(step == pl.num_programs(0) - 1)
    def _():
        dw_out[:n_j, :] = dot(da_all[...].astype(BF16), enc[...], ((0,), (0,)))


def joint_backward(e, h, q0, q1, r, lab, w_out_t, enc):
    n_v, n_j = w_out_t.shape
    full = lambda shape: pl.BlockSpec(shape, lambda i: (0,) * len(shape), pipeline_mode=pl.Buffered(1))
    return pl.pallas_call(
        backward_kernel,
        grid=(N_UTT // U_STEP,),
        in_specs=[
            pl.BlockSpec((U_STEP, UG, ROWS, n_v), lambda i: (i, 0, 0, 0)),
            pl.BlockSpec((U_STEP, UG, ROWS, n_j), lambda i: (i, 0, 0, 0)),
            full(q0.shape), full(q1.shape), full(r.shape), full(lab.shape), full(w_out_t.shape), full(enc.shape),
        ],
        out_specs=[
            pl.BlockSpec((U_STEP, T_LOC, n_j), lambda i: (i, 0, 0)),
            pl.BlockSpec((U_STEP, N_UP, n_j), lambda i: (i, 0, 0)),
            pl.BlockSpec((2 * n_j, n_v), lambda i: (0, 0)),
        ],
        out_shape=[
            jax.ShapeDtypeStruct((N_UTT, T_LOC, n_j), BF16),
            jax.ShapeDtypeStruct((N_UTT, N_UP, n_j), F32),
            jax.ShapeDtypeStruct((2 * n_j, n_v), F32),
        ],
        scratch_shapes=[pltpu.VMEM((U_STEP * UG * ROWS, n_v), BF16), pltpu.VMEM((N_UTT * T_LOC, n_j), F32)],
        compiler_params=pltpu.CompilerParams(vmem_limit_bytes=VMEM_FULL),
        name="joint_backward",
    )(e, h, q0, q1, r, lab, w_out_t, enc)


class Links:
    def __init__(self, send_sem, recv_sem):
        self.send_sem, self.recv_sem, self.used, self.copies = send_sem, recv_sem, 0, []
        seq = lax.axis_index("seq")
        self.core = lax.rem(seq, 2)
        self.x = lax.div(seq, 2)
        self.y = lax.axis_index("data")
        self.seq = seq
        self.dev = {
            "core": {"seq": seq + 1 - 2 * self.core},
            "x": {"seq": lax.rem(seq + 2, N_SEQ)},
            "y": {"data": 1 - self.y},
        }

    def greet(self):
        barrier = pltpu.get_barrier_semaphore()
        for dev in self.dev.values():
            pl.semaphore_signal(barrier, inc=1, device_id=dev, device_id_type=MESH)
        pl.semaphore_wait(barrier, 3)

    def send(self, src, dst, axis):
        i = self.used
        self.used += 1
        cp = pltpu.make_async_remote_copy(src_ref=src, dst_ref=dst, send_sem=self.send_sem.at[i], recv_sem=self.recv_sem.at[i],
                                          device_id=self.dev[axis], device_id_type=MESH)
        cp.start()
        self.copies.append(cp)
        return cp


def rows_at(start, size):
    return pl.ds(pl.multiple_of(start, 16), size)


def sum_stages(links, src, acc, gat, stg, rcv):
    n_row, n_col = src.shape
    half = n_row // 2
    h0 = links.core * half
    box = []
    for q in range(2):
        first, second = ("x", "y") if q == 0 else ("y", "x")
        k1, k2 = (links.x, links.y) if q == 0 else (links.y, links.x)
        box.append((first, second, k1, k2, h0, half, pl.ds(q * (n_col // 2), n_col // 2)))
    live = {}

    def s1():
        stg[0][...] = src[rows_at((1 - links.core) * half, half), :].astype(BF16)
        live["c"] = links.send(stg[0], rcv[0], "core")

    def s2():
        live["c"].wait_recv()
        acc[...] = src[rows_at(h0, half), :] + rcv[0][...].astype(F32)
        for q, (first, second, k1, k2, base, n, cols) in enumerate(box):
            stg[1][q] = acc[rows_at((1 - k1) * (n // 2), n // 2), cols].astype(BF16)
            live[q] = links.send(stg[1].at[q], rcv[1].at[q], first)

    def s3():
        for q, (first, second, k1, k2, base, n, cols) in enumerate(box):
            live[q].wait_recv()
            part = rows_at((1 - k2) * (n // 4), n // 4)
            stg[2][q] = (acc[rows_at(k1 * (n // 2) + (1 - k2) * (n // 4), n // 4), cols] + rcv[1][q, part].astype(F32)).astype(BF16)
            live[q] = links.send(stg[2].at[q], rcv[2].at[q], second)

    def s4():
        for q, (first, second, k1, k2, base, n, cols) in enumerate(box):
            live[q].wait_recv()
            own = rows_at(base + k1 * (n // 2) + k2 * (n // 4), n // 4)
            part = rows_at(k2 * (n // 4), n // 4)
            total = acc[rows_at(k1 * (n // 2) + k2 * (n // 4), n // 4), cols] + rcv[1][q, part].astype(F32) + rcv[2][q].astype(F32)
            gat[own, cols] = total.astype(BF16)
            live[q] = links.send(gat.at[own, cols], gat.at[own, cols], second)

    def s5():
        for q, (first, second, k1, k2, base, n, cols) in enumerate(box):
            live[q].wait_recv()
            own = rows_at(base + k1 * (n // 2), n // 2)
            live[q] = links.send(gat.at[own, cols], gat.at[own, cols], first)

    def s6():
        for q in range(2):
            live[q].wait_recv()
        own = rows_at(h0, half)
        live["c"] = links.send(gat.at[own, :], gat.at[own, :], "core")

    def s7():
        live["c"].wait_recv()

    return [s1, s2, s3, s4, s5, s6, s7]


def dc_stages(links, src, gat, stg, rcv):
    n_row, n_col = src.shape
    half, quar = n_row // 2, n_row // 4
    h0 = links.core * half
    r0 = h0 + links.x * quar
    live = {}

    def s1():
        stg[0][...] = src[rows_at((1 - links.core) * half, half), :].astype(BF16)
        live["c"] = links.send(stg[0], rcv[0], "core")

    def s2():
        live["c"].wait_recv()
        part = rows_at((1 - links.x) * quar, quar)
        stg[1][...] = (src[rows_at(h0 + (1 - links.x) * quar, quar), :] + rcv[0][part, :].astype(F32)).astype(BF16)
        live["x"] = links.send(stg[1], rcv[1], "x")

    y_own, y_far = links.y * n_row, (1 - links.y) * n_row

    def hop(start, size, axis):
        rows = rows_at(start, size)
        return links.send(gat.at[rows, :], gat.at[rows, :], axis)

    def s3():
        live["x"].wait_recv()
        part = rows_at(links.x * quar, quar)
        total = src[rows_at(r0, quar), :] + rcv[0][part, :].astype(F32) + rcv[1][...].astype(F32)
        gat[rows_at(y_own + r0, quar), :] = total.astype(BF16)
        live["y"] = hop(y_own + r0, quar, "y")

    def s4():
        live["own"] = hop(y_own + r0, quar, "x")
        live["y"].wait_recv()
        live["far"] = hop(y_far + r0, quar, "x")

    def s5():
        live["own"].wait_recv()
        live["own"] = hop(y_own + h0, half, "core")
        live["far"].wait_recv()
        live["far"] = hop(y_far + h0, half, "core")

    def s6():
        live["own"].wait_recv()
        live["far"].wait_recv()

    return [s1, s2, s3, s4, s5, s6]


N_COPY = 10 + 7


def exchange_kernel(dw, dc, g_w, g_dc, acc_w, ws0, ws1, ws2, wr0, wr1, wr2, ds0, ds1, dr0, dr1, send_sem, recv_sem):
    links = Links(send_sem, recv_sem)
    links.greet()
    st_w = sum_stages(links, dw, acc_w, g_w, (ws0, ws1, ws2), (wr0, wr1, wr2))
    st_dc = dc_stages(links, dc, g_dc, (ds0, ds1), (dr0, dr1))
    for i in range(7):
        for stages in (st_dc, st_w):
            if i < len(stages):
                stages[i]()
    for cp in links.copies:
        cp.wait_send()


def sum_scratch(n_row, n_col):
    half = n_row // 2
    return [pltpu.VMEM((half, n_col), BF16), pltpu.VMEM((2, half // 2, n_col // 2), BF16), pltpu.VMEM((2, half // 4, n_col // 2), BF16)]


def exchange(dw, dc):
    n_r, n_j = dc.shape
    vm = pl.BlockSpec(memory_space=pltpu.VMEM)
    dc_bufs = [pltpu.VMEM((n_r // 2, n_j), BF16), pltpu.VMEM((n_r // 4, n_j), BF16)]
    return pl.pallas_call(
        exchange_kernel,
        in_specs=[vm] * 2,
        out_specs=[vm] * 2,
        out_shape=[jax.ShapeDtypeStruct(dw.shape, BF16), jax.ShapeDtypeStruct((2 * n_r, n_j), BF16)],
        scratch_shapes=[pltpu.VMEM((dw.shape[0] // 2, dw.shape[1]), F32)] + sum_scratch(*dw.shape) * 2 + dc_bufs * 2
        + [pltpu.SemaphoreType.DMA((N_COPY,)), pltpu.SemaphoreType.DMA((N_COPY,))],
        compiler_params=pltpu.CompilerParams(collective_id=1, has_side_effects=True, vmem_limit_bytes=VMEM_FULL),
        name="exchange",
    )(dw, dc)


def finish_kernel(g_w, g_dc, pred, pred_far, w_pred, da, w_enc, o_enc, o_pred, o_wenc, o_wpred, o_wout,
                  v_enc, v_pred, v_wenc, v_wpred, v_wout, sem):
    y = lax.axis_index("data")
    jobs = []

    def put(src, dst, i):
        cp = pltpu.make_async_copy(src, dst, sem.at[i])
        cp.start()
        jobs.append(cp)

    n_j = w_pred.shape[1]
    v_wenc[...] = g_w[:n_j, :].astype(F32).T
    put(v_wenc, o_wenc, 0)
    v_wout[...] = g_w[n_j:, :].astype(F32)
    put(v_wout, o_wout, 1)
    n_r = pred.shape[0]
    dc_own, dc_far = g_dc[rows_at(y * n_r, n_r), :], g_dc[rows_at((1 - y) * n_r, n_r), :]
    v_wpred[...] = dot(pred[...], dc_own, ((0,), (0,))) + dot(pred_far[...], dc_far, ((0,), (0,)))
    put(v_wpred, o_wpred, 2)
    v_pred[...] = dot(dc_own, w_pred[...], ((1,), (1,)))
    put(v_pred, o_pred, 3)
    v_enc[...] = dot(da[...], w_enc[...], ((1,), (1,))).astype(BF16)
    put(v_enc, o_enc, 4)
    for cp in jobs:
        cp.wait()


def finish(g_w, g_dc, pred, pred_far, w_pred, da, w_enc):
    vm = pl.BlockSpec(memory_space=pltpu.VMEM)
    outs = [(pred.shape, BF16), (pred.shape, F32), (w_pred.shape, F32), (w_pred.shape, F32), (w_pred.shape[::-1], F32)]
    return pl.pallas_call(
        finish_kernel,
        in_specs=[vm] * 7,
        out_specs=[pl.BlockSpec(memory_space=pl.ANY)] * 5,
        out_shape=[jax.ShapeDtypeStruct(*o) for o in outs],
        scratch_shapes=[pltpu.VMEM(*o) for o in outs] + [pltpu.SemaphoreType.DMA((5,))],
        compiler_params=pltpu.CompilerParams(vmem_limit_bytes=VMEM_FULL),
        name="finish",
    )(g_w, g_dc, pred, pred_far, w_pred, da, w_enc)


def solution(mesh):
    utt_rows = P(("part", "data"))
    utt_mats = P(("part", "data"), None)
    utt_cube = P(("part", "data"), None, None)
    enc_spec = P(("part", "data"), "seq", None)
    weight_in = P(None, None)
    weight_out = P("part", None)

    def body(enc_loc, pred_loc, w_enc, w_pred, w_out, labels, frame_len, label_len):
        n_h = enc_loc.shape[2]
        lab_ids = jnp.concatenate([labels, jnp.zeros((N_UTT, 1), jnp.int32)], axis=1)
        lab = jnp.broadcast_to(lab_ids.reshape(N_UTT * N_UP, 1), (N_UTT * N_UP, 128))
        enc2 = enc_loc.reshape(N_UTT * T_LOC, n_h)
        pred2 = pred_loc.reshape(N_UTT * N_UP, n_h)
        pred_far = lax.ppermute(pred2, "data", [(0, 1), (1, 0)])
        e, h, stat, sums = joint_forward(enc2, pred2, w_enc, w_pred, w_out, lab)
        lens = lambda v: jnp.broadcast_to(jnp.tile(v, 8)[None], (8, 128))
        q0, q1, r, loss = lattice(stat, sums, lens(frame_len), lens(label_len))
        da, dc, dw = joint_backward(e, h, q0, q1, r, lab, w_out.T, enc2)
        da2 = da.reshape(N_UTT * T_LOC, -1)
        g_w, g_dc = exchange(dw, dc.reshape(N_UTT * N_UP, -1))
        grad_enc, grad_pred, grad_w_enc, grad_w_pred, grad_w_out = finish(g_w, g_dc, pred2, pred_far, w_pred, da2, w_enc)
        return loss[0, :N_UTT], grad_enc.reshape(enc_loc.shape), grad_pred.reshape(pred_loc.shape), grad_w_enc, grad_w_pred, grad_w_out

    return jax.shard_map(body, mesh=mesh, in_specs=(enc_spec, utt_cube, weight_in, weight_in, weight_in, utt_mats, utt_rows, utt_rows), out_specs=(utt_rows, enc_spec, utt_cube, weight_out, weight_out, weight_out), check_vma=False)
```

```python
import functools

import jax
import jax.numpy as jnp
from jax import lax
from jax.experimental import pallas as pl
from jax.experimental.pallas import tpu as pltpu
from jax.sharding import PartitionSpec as P

NEG = -1e30
SUB = 8
LANES = 128
LOG2E = 1.4426950408889634
LN2 = 0.6931471805599453
F32 = jnp.float32
BF16 = jnp.bfloat16
MESH = pl.DeviceIdType.MESH
VMEM_FULL = 67_000_000
N_UTT = 16
T_LOC = 24
N_UP = 24
UG = 3
N_SEQ = 4
T_ALL = T_LOC * N_SEQ
RING = 4
N_DIAG = T_ALL + N_UP - 1
ROWS = SUB * T_LOC


def dot(lhs, rhs, dims=((1,), (0,))):
    return lax.dot_general(lhs, rhs, (dims, ((), ())), preferred_element_type=F32)


def label_column(labels, utt, ug, sub):
    col = jnp.zeros((SUB, LANES), jnp.int32)
    for k in range(SUB):
        if ug * SUB + k < N_UP - 1:
            col = jnp.where(sub == k, labels[utt, ug * SUB + k], col)
    return col


def forward_kernel(labels, enc, pred, w_enc, w_pred, w_out, z_hbm, h_hbm, stat_out, norm_out, act_e, act_p, h_next, z_last, z_ring, h_ring, z_sem, h_sem):
    step = pl.program_id(0)
    lane = lax.broadcasted_iota(jnp.int32, (SUB, LANES), 1)
    sub = lax.broadcasted_iota(jnp.int32, (SUB, LANES), 0)
    n_v = w_out.shape[1]

    @pl.when(step == 0)
    def _():
        act_e[...] = dot(enc[...], w_enc[...]).astype(BF16).astype(F32)
        act_p[...] = dot(pred[...], w_pred[...]).astype(BF16).astype(F32)
        stat_out[...] = jnp.zeros_like(stat_out)
        norm_out[...] = jnp.zeros_like(norm_out)

    def hidden(utt, ug, dst):
        row = pl.multiple_of(utt * N_UP, SUB)
        c_grp = act_p[pl.ds(row + SUB * ug, SUB), :]
        a_utt = act_e[pl.ds(row, T_LOC), :]
        for t in range(0, T_LOC, 2):
            pre = jnp.concatenate([a_utt[t:t + 1, :] + c_grp, a_utt[t + 1:t + 2, :] + c_grp], axis=0)
            dst[t * SUB:t * SUB + 16, :] = jnp.tanh(pre).astype(BF16)

    def soften(utt, ug, src):
        lab_grp = label_column(labels, jnp.maximum(utt, 0), ug, sub)
        masks = [lab_grp - LANES * k == lane for k in range(n_v // LANES)]
        for t4 in range(T_LOC // 4):
            cur = stat_out[ug * 6 + t4]
            for k in range(4):
                t = t4 * 4 + k
                z = [src[t * SUB:t * SUB + SUB, c * LANES:c * LANES + LANES] for c in range(n_v // LANES)]
                top = functools.reduce(jnp.maximum, z)
                tot = functools.reduce(jnp.add, [jnp.exp2((v - top) * LOG2E) for v in z])
                picked = functools.reduce(jnp.add, [jnp.where(m, v, 0.0) for m, v in zip(masks, z)])
                row_top = jnp.max(top, axis=1, keepdims=True)
                row_tot = jnp.sum(tot * jnp.exp2((top - row_top) * LOG2E), axis=1, keepdims=True)
                norm = row_top * LOG2E + jnp.log2(row_tot)
                blank = z[0][:, 0:1] * LOG2E - norm
                label = jnp.sum(picked, axis=1, keepdims=True) * LOG2E - norm
                cur = jnp.where(lane == utt + 32 * k, blank, cur)
                cur = jnp.where(lane == utt + 32 * k + 16, label, cur)
                norm_out[ug * T_LOC + t] = jnp.where(lane == utt, norm, norm_out[ug * T_LOC + t])
            stat_out[ug * 6 + t4] = cur

    def puts(utt):
        at = lax.rem(utt, RING)
        return (pltpu.make_async_copy(z_ring.at[at], z_hbm.at[utt], z_sem.at[at]),
                pltpu.make_async_copy(h_ring.at[at], h_hbm.at[utt], h_sem.at[at]))

    @pl.when(step == 0)
    def _():
        hidden(0, 0, h_next)

    @pl.when(step >= RING)
    def _():
        for cp in puts(step - RING):
            cp.wait()

    slot = lax.rem(step, RING)
    z_out, h_out = z_ring.at[pl.ds(slot, 1)], h_ring.at[pl.ds(slot, 1)]
    h_out[0, 0] = h_next[...]
    z_out[0, 0] = dot(h_next[...], w_out[...])
    hidden(step, 1, h_out.at[0, 1])
    soften(step - 1, 2, z_last)
    z_out[0, 1] = dot(h_out[0, 1], w_out[...])
    hidden(step, 2, h_out.at[0, 2])
    soften(step, 0, z_out.at[0, 0])
    z_two = dot(h_out[0, 2], w_out[...])
    z_last[...] = z_two
    z_out[0, 2] = z_two
    hidden(jnp.minimum(step + 1, N_UTT - 1), 0, h_next)
    soften(step, 1, z_out.at[0, 1])
    for cp in puts(step):
        cp.start()

    @pl.when(step == N_UTT - 1)
    def _():
        soften(step, 2, z_last)
        for back in range(RING - 1, -1, -1):
            for cp in puts(step - back):
                cp.wait()


def joint_forward(labels, enc, pred, w_enc, w_pred, w_out):
    n_j, n_v = w_out.shape
    full = lambda shape: pl.BlockSpec(shape, lambda i: (0,) * len(shape), pipeline_mode=pl.Buffered(1))
    return pl.pallas_call(
        forward_kernel,
        grid=(N_UTT,),
        in_specs=[pl.BlockSpec(memory_space=pltpu.SMEM)] + [full(v.shape) for v in (enc, pred, w_enc, w_pred, w_out)],
        out_specs=[
            pl.BlockSpec(memory_space=pl.ANY),
            pl.BlockSpec(memory_space=pl.ANY),
            pl.BlockSpec((UG * 6, SUB, LANES), lambda i: (0, 0, 0)),
            pl.BlockSpec((UG * T_LOC, SUB, LANES), lambda i: (0, 0, 0)),
        ],
        out_shape=[
            jax.ShapeDtypeStruct((N_UTT, UG, ROWS, n_v), F32),
            jax.ShapeDtypeStruct((N_UTT, UG, ROWS, n_j), BF16),
            jax.ShapeDtypeStruct((UG * 6, SUB, LANES), F32),
            jax.ShapeDtypeStruct((UG * T_LOC, SUB, LANES), F32),
        ],
        scratch_shapes=[pltpu.VMEM((N_UTT * T_LOC, n_j), F32), pltpu.VMEM((N_UTT * N_UP, n_j), F32), pltpu.VMEM((ROWS, n_j), BF16), pltpu.VMEM((ROWS, n_v), F32),
            pltpu.VMEM((RING, UG, ROWS, n_v), F32), pltpu.VMEM((RING, UG, ROWS, n_j), BF16),
            pltpu.SemaphoreType.DMA((RING,)), pltpu.SemaphoreType.DMA((RING,))],
        compiler_params=pltpu.CompilerParams(vmem_limit_bytes=VMEM_FULL),
        name="joint_forward",
    )(labels, enc, pred, w_enc, w_pred, w_out)


def lae2(x, y):
    return jnp.maximum(x, y) + jnp.log2(1.0 + jnp.exp2(-jnp.abs(x - y)))


def lattice_kernel(stat, norm, flen, llen, q0_out, q1_out, norm_out, loss_out, gath, s_blank, s_label, s_alpha, s_beta, send_sem, recv_sem):
    me = lax.axis_index("seq")
    barrier = pltpu.get_barrier_semaphore()
    for off in range(1, N_SEQ):
        pl.semaphore_signal(barrier, inc=1, device_id={"seq": lax.rem(me + off, N_SEQ)}, device_id_type=MESH)
    pl.semaphore_wait(barrier, N_SEQ - 1)
    copies = []
    for off in range(1, N_SEQ):
        cp = pltpu.make_async_remote_copy(
            src_ref=stat, dst_ref=gath.at[off - 1], send_sem=send_sem.at[off - 1], recv_sem=recv_sem.at[off - 1],
            device_id={"seq": lax.rem(me + off, N_SEQ)}, device_id_type=MESH)
        cp.start()
        copies.append(cp)

    sub = lax.broadcasted_iota(jnp.int32, (SUB, LANES), 0)
    sub24 = lax.broadcasted_iota(jnp.int32, (N_UP, LANES), 0)
    lane = lax.broadcasted_iota(jnp.int32, (SUB, LANES), 1)
    tb = jnp.zeros((SUB, LANES), jnp.int32)
    ub = jnp.zeros((SUB, LANES), jnp.int32)
    for b in range(N_UTT):
        at_b = lax.rem(lane, N_UTT) == b
        tb = jnp.where(at_b, flen[b], tb)
        ub = jnp.where(at_b, llen[b], ub)
    n_pad = s_blank.shape[0]

    def fill(i, c):
        s_blank[pl.ds(pl.multiple_of(i * SUB, SUB), SUB), :] = jnp.full((SUB, LANES), NEG, F32)
        s_label[pl.ds(pl.multiple_of(i * SUB, SUB), SUB), :] = jnp.full((SUB, LANES), NEG, F32)
        return c

    lax.fori_loop(0, n_pad // SUB, fill, 0, unroll=SUB)
    end_grp = [jnp.where(sub + SUB * ug == ub, 0.0, NEG) for ug in range(UG)]
    for t in range(T_ALL, T_ALL + N_UP):
        for ug in range(UG):
            s_blank[pl.ds(t * N_UP + 200 * ug, SUB, stride=25), :] = end_grp[ug]

    def place(src, src_seq):
        for t4 in range(T_LOC // 4):
            for ug in range(UG):
                val = src[ug * 6 + t4]
                in_u = sub + SUB * ug <= ub
                in_l = sub + SUB * ug < ub
                for k in range(4):
                    t = src_seq * T_LOC + t4 * 4 + k
                    bl = val if k == 0 else pltpu.roll(val, LANES - 32 * k, 1)
                    la = pltpu.roll(val, 112 - 32 * k, 1)
                    ok = t < tb
                    s_blank[pl.ds(t * N_UP + 200 * ug, SUB, stride=25), :] = jnp.where(ok, jnp.where(in_u, bl, NEG), end_grp[ug])
                    s_label[pl.ds(t * N_UP + 200 * ug, SUB, stride=25), :] = jnp.where(ok & in_l, la, NEG)

    place(stat, me)
    for off in range(1, N_SEQ):
        copies[off - 1].wait_recv()
        place(gath.at[off - 1], lax.rem(me + N_SEQ - off, N_SEQ))

    alpha0 = jnp.where(sub24 == 0, 0.0, NEG)
    s_alpha[pl.ds(0, N_UP), :] = alpha0
    beta_end = jnp.where(sub24 == jnp.concatenate([ub] * UG, axis=0), 0.0, NEG)
    s_beta[pl.ds(N_DIAG * N_UP, N_UP), :] = beta_end
    s_beta[pl.ds((N_DIAG + 1) * N_UP, SUB), :] = jnp.full((SUB, LANES), NEG, F32)

    def wave(i, carry):
        alpha, beta = carry
        row = pl.multiple_of(i * N_UP, SUB)
        x = alpha + s_blank[pl.ds(row, N_UP), :]
        y = alpha + s_label[pl.ds(row, N_UP), :]
        y = jnp.where(sub24 == 0, NEG, pltpu.roll(y, 1, 0))
        alpha = lae2(x, y)
        s_alpha[pl.ds(pl.multiple_of(row + N_UP, SUB), N_UP), :] = alpha
        brow = pl.multiple_of((N_DIAG - 1 - i) * N_UP, SUB)
        bx = beta + s_blank[pl.ds(brow, N_UP), :]
        by = pltpu.roll(beta, N_UP - 1, 0) + s_label[pl.ds(brow, N_UP), :]
        beta = lae2(bx, by)
        s_beta[pl.ds(brow, N_UP), :] = beta
        return alpha, beta

    _, beta = lax.fori_loop(0, N_DIAG, wave, (alpha0, beta_end), unroll=7)
    log_p = beta[0:1, :]
    loss_out[...] = jnp.broadcast_to(-LN2 * log_p, (SUB, LANES))
    for t in range(T_LOC):
        tg = me * T_LOC + t
        for ug in range(UG):
            base = tg * N_UP + 200 * ug
            grp = lambda ref, off: ref[pl.ds(base + off, SUB, stride=25), :]
            al = grp(s_alpha, 0) - log_p
            ok = (tg < tb) & (sub + SUB * ug <= ub)
            q0 = jnp.where(ok, jnp.exp2(al + grp(s_blank, 0) + grp(s_beta, 24)), 0.0)
            q1 = jnp.where(ok, jnp.exp2(al + grp(s_label, 0) + grp(s_beta, 25)), 0.0)
            idx = ug * T_LOC + t
            q0_out[idx] = q0
            q1_out[idx] = q1
            norm_out[idx] = norm[idx] - jnp.log2(q0 + q1)
    for cp in copies:
        cp.wait_send()


def lattice(stat, norm, flen, llen):
    vm = pl.BlockSpec(memory_space=pltpu.VMEM)
    n_rows = (T_ALL + 2 * N_UP) * N_UP
    return pl.pallas_call(
        lattice_kernel,
        in_specs=[vm] * 2 + [pl.BlockSpec(memory_space=pltpu.SMEM)] * 2,
        out_specs=[vm] * 4,
        out_shape=[jax.ShapeDtypeStruct((UG * T_LOC, SUB, LANES), F32)] * 3 + [jax.ShapeDtypeStruct((SUB, LANES), F32)],
        scratch_shapes=[pltpu.VMEM((N_SEQ - 1,) + stat.shape, F32)] + [pltpu.VMEM((n_rows, LANES), F32)] * 4
        + [pltpu.SemaphoreType.DMA((N_SEQ - 1,)), pltpu.SemaphoreType.DMA((N_SEQ - 1,))],
        compiler_params=pltpu.CompilerParams(collective_id=0, has_side_effects=True),
        name="lattice",
    )(stat, norm, flen, llen)


class Links:
    def __init__(self, send_sem, recv_sem):
        self.send_sem, self.recv_sem, self.copies = send_sem, recv_sem, []
        seq = lax.axis_index("seq")
        self.core = lax.rem(seq, 2)
        self.x = lax.div(seq, 2)
        self.y = lax.axis_index("data")
        self.dev = {
            "core": {"seq": seq + 1 - 2 * self.core},
            "x": {"seq": lax.rem(seq + 2, N_SEQ)},
            "y": {"data": 1 - self.y},
        }

    def greet(self):
        barrier = pltpu.get_barrier_semaphore()
        for dev in self.dev.values():
            pl.semaphore_signal(barrier, inc=1, device_id=dev, device_id_type=MESH)
        pl.semaphore_wait(barrier, 3)

    def copy(self, ends, axis):
        i = len(self.copies)

        def make():
            src, dst = ends()
            return pltpu.make_async_remote_copy(src_ref=src, dst_ref=dst, send_sem=self.send_sem.at[i], recv_sem=self.recv_sem.at[i],
                                                device_id=self.dev[axis], device_id_type=MESH)

        self.copies.append(make)
        return make


def rows_at(start, size):
    return pl.ds(pl.multiple_of(start, 16), size)


def sum_stages(links, acc, gat, stg, rcv, col0, n_col):
    half = acc.shape[0] // 2
    h0 = links.core * half
    every = pl.ds(col0, n_col)
    box = []
    for q in range(2):
        first, second = ("x", "y") if q == 0 else ("y", "x")
        k1, k2 = (links.x, links.y) if q == 0 else (links.y, links.x)
        box.append((q, first, second, k1, k2, pl.ds(col0 + q * (n_col // 2), n_col // 2)))
    n2, n4 = half // 2, half // 4

    def same(rows, cols):
        def ends():
            ref = gat.at[rows(), cols]
            return ref, ref
        return ends

    swap = links.copy(lambda: (stg[0], rcv[0]), "core")
    back = links.copy(same(lambda: rows_at(h0, half), every), "core")
    hops = [(
        links.copy(lambda q=q: (stg[1].at[q], rcv[1].at[q]), first),
        links.copy(lambda q=q: (stg[2].at[q], rcv[2].at[q]), second),
        links.copy(same(lambda k1=k1, k2=k2: rows_at(h0 + k1 * n2 + k2 * n4, n4), cols), second),
        links.copy(same(lambda k1=k1: rows_at(h0 + k1 * n2, n2), cols), first),
    ) for q, first, second, k1, k2, cols in box]

    def s1():
        stg[0][...] = acc[rows_at((1 - links.core) * half, half), every].astype(BF16)
        swap().start()

    def s2():
        swap().wait_recv()
        own = rows_at(h0, half)
        acc[own, every] = acc[own, every] + rcv[0][...].astype(F32)
        for q, first, second, k1, k2, cols in box:
            stg[1][q] = acc[rows_at(h0 + (1 - k1) * n2, n2), cols].astype(BF16)
            hops[q][0]().start()

    def s3():
        for q, first, second, k1, k2, cols in box:
            hops[q][0]().wait_recv()
            part = rows_at((1 - k2) * n4, n4)
            stg[2][q] = (acc[rows_at(h0 + k1 * n2 + (1 - k2) * n4, n4), cols] + rcv[1][q, part].astype(F32)).astype(BF16)
            hops[q][1]().start()

    def s4():
        for q, first, second, k1, k2, cols in box:
            hops[q][1]().wait_recv()
            part = rows_at(k2 * n4, n4)
            own = rows_at(h0 + k1 * n2 + k2 * n4, n4)
            gat[own, cols] = (acc[own, cols] + rcv[1][q, part].astype(F32) + rcv[2][q].astype(F32)).astype(BF16)
            hops[q][2]().start()

    def s5():
        for hop in hops:
            hop[2]().wait_recv()
            hop[3]().start()

    def s6():
        for hop in hops:
            hop[3]().wait_recv()
        back().start()

    def s7():
        back().wait_recv()

    return [s1, s2, s3, s4, s5, s6, s7]


def dc_stages(links, src, gat, stg, rcv):
    n_row = src.shape[0]
    half, quar, eigh = n_row // 2, n_row // 4, n_row // SUB
    h0 = links.core * half
    r0 = h0 + links.x * quar
    r_far = h0 + (1 - links.x) * quar
    y_own, y_far = links.y * n_row, (1 - links.y) * n_row

    def hop(start, size, axis):
        def ends():
            ref = gat.at[rows_at(start(), size), :]
            return ref, ref
        return links.copy(ends, axis)

    swap = links.copy(lambda: (stg[0], rcv[0]), "core")
    cross = links.copy(lambda: (stg[1], rcv[1]), "x")
    up_y = hop(lambda: y_own + r0, eigh, "y")
    down_x = hop(lambda: y_own + r0 + eigh, eigh, "x")
    up_x = hop(lambda: y_own + r0, eigh, "x")
    down_y = hop(lambda: y_own + r0 + eigh, eigh, "y")
    up_far = hop(lambda: y_far + r0, eigh, "x")
    down_far = hop(lambda: y_own + r_far + eigh, eigh, "y")
    back = [hop(lambda: y_own + h0, half, "core"), hop(lambda: y_far + h0, half, "core")]

    def s1():
        stg[0][...] = src[rows_at((1 - links.core) * half, half), :].astype(BF16)
        swap().start()

    def s2():
        swap().wait_recv()
        part = rows_at((1 - links.x) * quar, quar)
        stg[1][...] = (src[rows_at(r_far, quar), :] + rcv[0][part, :].astype(F32)).astype(BF16)
        cross().start()

    def s3():
        cross().wait_recv()
        part = rows_at(links.x * quar, quar)
        total = src[rows_at(r0, quar), :] + rcv[0][part, :].astype(F32) + rcv[1][...].astype(F32)
        gat[rows_at(y_own + r0, quar), :] = total.astype(BF16)
        for cp in (up_y, down_x, up_x, down_y):
            cp().start()

    def s4():
        up_y().wait_recv()
        up_far().start()
        down_x().wait_recv()
        down_far().start()

    def s5():
        for cp in (up_x, down_y, up_far, down_far):
            cp().wait_recv()
        for cp in back:
            cp().start()

    def s6():
        for cp in back:
            cp().wait_recv()

    return [s1, s2, s3, s4, s5, s6]


N_COPY = 10 * 4 + 1


def sum_scratch(n_row, n_col):
    half = n_row // 2
    return [pltpu.VMEM((half, n_col), BF16), pltpu.VMEM((2, half // 2, n_col // 2), BF16), pltpu.VMEM((2, half // 4, n_col // 2), BF16)]


W_CHUNK = 256


def backward_kernel(labels, pred, z_hbm, h_hbm, q0_ref, q1_ref, norm_ref, w_out, enc, da_out, g_enc_out, g_out_out, g_dc_out, far_out,
                    dz_all, h_all, da_all, da_part, dz0, dz1, dz2, dh0, dh1, dh2, w_out_t, z_ring, dw_enc, dw_out, dc_out, g_enc, g_out, g_dc,
                    es0, es1, es2, er0, er1, er2, ps0, ps1, ps2, pr0, pr1, pr2, qs0, qs1, qs2, qr0, qr1, qr2, ds0, ds1, dr0, dr1,
                    h_sem, z_sem, o_sem, send_sem, recv_sem):
    step = pl.program_id(0)
    lane = lax.broadcasted_iota(jnp.int32, (SUB, LANES), 1)
    sub = lax.broadcasted_iota(jnp.int32, (SUB, LANES), 0)
    n_j, n_v = w_out.shape
    utt_rows = UG * ROWS

    dzs, dhs = (dz0, dz1, dz2), (dh0, dh1, dh2)
    prev = jnp.maximum(step - 1, 0)
    z_slot = lax.rem(step, RING)

    def multiply(ug):
        dhs[ug][...] = dot(dzs[ug][...], w_out_t[...])[:, :n_j]

    def h_copy(utt):
        rows = pl.ds(pl.multiple_of(utt * utt_rows, 16), utt_rows)
        return pltpu.make_async_copy(h_hbm.at[rows, :], h_all.at[rows, :], h_sem.at[utt])

    def z_copy(utt):
        slot = lax.rem(utt, RING)
        return pltpu.make_async_copy(z_hbm.at[utt], z_ring.at[slot], z_sem.at[slot])

    links = Links(send_sem, recv_sem)
    far = links.copy(lambda: (pred, far_out), "y")
    e_st = sum_stages(links, dw_enc, g_enc, (es0, es1, es2), (er0, er1, er2), 0, n_v)
    p_st = sum_stages(links, dw_out, g_out, (ps0, ps1, ps2), (pr0, pr1, pr2), 0, n_v // 2)
    q_st = sum_stages(links, dw_out, g_out, (qs0, qs1, qs2), (qr0, qr1, qr2), n_v // 2, n_v // 2)
    c_st = dc_stages(links, dc_out, g_dc, (ds0, ds1), (dr0, dr1))

    @pl.when(step == 0)
    def _():
        links.greet()
        far().start()
        for utt in range(RING - 1):
            z_copy(utt).start()
            h_copy(utt).start()
        w_out_t[:, :n_j] = w_out[...].T
        w_out_t[:, n_j:] = jnp.zeros((n_v, w_out_t.shape[1] - n_j), BF16)

    def logit_grads(ug):
        shift = LANES - step
        lab_grp = label_column(labels, step, ug, sub)
        masks = [lab_grp - LANES * k == lane for k in range(n_v // LANES)]
        for t in range(0, T_LOC, 2):
            pair = []
            for idx in (ug * T_LOC + t, ug * T_LOC + t + 1):
                q0, q1, norm = [jnp.broadcast_to(pltpu.roll(ref[idx], shift, 1)[:, 0:1], (SUB, LANES)) for ref in (q0_ref, q1_ref, norm_ref)]
                row = (idx - ug * T_LOC) * SUB
                tiles = []
                for k in range(n_v // LANES):
                    z = z_ring[z_slot, ug, row:row + SUB, k * LANES:k * LANES + LANES]
                    g = jnp.exp2(z * LOG2E - norm) - jnp.where(masks[k], q1, 0.0)
                    tiles.append(g - jnp.where(lane == 0, q0, 0.0) if k == 0 else g)
                pair.append(jnp.concatenate(tiles, axis=1))
            rows = pl.ds(pl.multiple_of(step * utt_rows + ug * ROWS + t * SUB, 16), 16)
            dz = jnp.concatenate(pair, axis=0).astype(BF16)
            dz_all[rows, :] = dz
            dzs[ug][t * SUB:t * SUB + 16, :] = dz

    def hidden_grads(utt, ug):
        dc = None
        for t in range(0, T_LOC, 2):
            hid = h_all[pl.ds(pl.multiple_of(utt * utt_rows + ug * ROWS + t * SUB, 16), 16), :].astype(F32)
            ds = dhs[ug][t * SUB:t * SUB + 16, :] * (1.0 - hid * hid)
            both = ds[:SUB] + ds[SUB:]
            dc = both if dc is None else dc + both
            if ug > 0:
                ds = ds + da_part[t * SUB:t * SUB + 16, :]
            if ug < UG - 1:
                da_part[t * SUB:t * SUB + 16, :] = ds
            else:
                for k in range(2):
                    da_all[pl.ds(utt * T_LOC + t + k, 1), :] = jnp.sum(ds[SUB * k:SUB * k + SUB], axis=0, keepdims=True)
        dc_out[pl.ds(pl.multiple_of(utt * N_UP + ug * SUB, SUB), SUB), :] = dc

    @pl.when(step + RING - 1 < N_UTT)
    def _():
        z_copy(step + RING - 1).start()
        h_copy(step + RING - 1).start()

    @pl.when(step < N_UTT)
    def _():
        h_copy(step).wait()
        z_copy(step).wait()
        multiply(2)
        logit_grads(0)
        hidden_grads(prev, 1)
        multiply(0)
        logit_grads(1)
        hidden_grads(prev, 2)
        multiply(1)
        logit_grads(2)
        hidden_grads(step, 0)

    @pl.when(step == N_UTT)
    def _():
        multiply(2)
        hidden_grads(prev, 1)
        hidden_grads(prev, 2)
        da = da_all[...].astype(BF16)
        da_out[...] = da
        dw_enc[...] = dot(da, enc[...], ((0,), (0,)))
        e_st[0]()
        c_st[0]()

    plan = [
        ((e_st[1], c_st[1]), ()),
        ((), (p_st[0],)),
        ((e_st[2], c_st[2], p_st[1]), ()),
        ((e_st[3], c_st[3], p_st[2]), (q_st[0], e_st[4], p_st[3], c_st[4], q_st[1], e_st[5], p_st[4], q_st[2], c_st[5], q_st[3], p_st[5], e_st[6], q_st[4])),
    ]
    for part, (lo, hi) in enumerate(((0, 3 * LANES), (3 * LANES, n_j))):
        @pl.when(step > N_UTT)
        def _(lo=lo, hi=hi):
            cols = pl.ds(pl.multiple_of((step - N_UTT - 1) * W_CHUNK, W_CHUNK), W_CHUNK)
            dw_out[lo:hi, cols] = dot(h_all[:, lo:hi], dz_all[:, cols], ((0,), (0,)))

        for n, stages in enumerate(plan):
            if stages[part]:
                @pl.when(step == N_UTT + 1 + n)
                def _(stages=stages[part]):
                    for stage in stages:
                        stage()

    @pl.when(step == N_UTT + len(plan))
    def _():
        out_dc = pltpu.make_async_copy(g_dc, g_dc_out, o_sem.at[0])
        out_dc.start()
        out_enc = pltpu.make_async_copy(g_enc, g_enc_out, o_sem.at[1])
        out_enc.start()
        p_st[6]()
        q_st[5]()
        q_st[6]()
        out_out = pltpu.make_async_copy(g_out, g_out_out, o_sem.at[2])
        out_out.start()
        far().wait_recv()
        for cp in links.copies:
            cp().wait_send()
        out_dc.wait()
        out_enc.wait()
        out_out.wait()


def joint_backward(labels, pred, z, h, q0, q1, norm, w_out, enc):
    n_j, n_v = w_out.shape
    n_cell = N_UTT * UG * ROWS
    n_dc = N_UTT * N_UP
    full = lambda shape: pl.BlockSpec(shape, lambda i: (0,) * len(shape), pipeline_mode=pl.Buffered(1))
    return pl.pallas_call(
        backward_kernel,
        grid=(N_UTT + 1 + n_v // W_CHUNK,),
        in_specs=[
            pl.BlockSpec(memory_space=pltpu.SMEM),
            *[pl.BlockSpec(memory_space=pl.ANY)] * 3,
            full(q0.shape), full(q1.shape), full(norm.shape), full(w_out.shape), full(enc.shape),
        ],
        out_specs=[full((N_UTT * T_LOC, n_j))] + [pl.BlockSpec(memory_space=pl.ANY)] * 4,
        out_shape=[
            jax.ShapeDtypeStruct((N_UTT * T_LOC, n_j), BF16),
            jax.ShapeDtypeStruct((n_j, n_v), BF16),
            jax.ShapeDtypeStruct((n_j, n_v), BF16),
            jax.ShapeDtypeStruct((2 * n_dc, n_j), BF16),
            jax.ShapeDtypeStruct(pred.shape, BF16),
        ],
        scratch_shapes=[
            pltpu.VMEM((n_cell, n_v), BF16), pltpu.VMEM((n_cell, n_j), BF16), pltpu.VMEM((N_UTT * T_LOC, n_j), F32),
            pltpu.VMEM((ROWS, n_j), F32),
            *[pltpu.VMEM((ROWS, n_v), BF16)] * 3, *[pltpu.VMEM((ROWS, n_j), F32)] * 3,
            pltpu.VMEM((n_v, n_j + (-n_j) % 256), BF16), pltpu.VMEM((RING, UG, ROWS, n_v), F32),
            pltpu.VMEM((n_j, n_v), F32), pltpu.VMEM((n_j, n_v), F32), pltpu.VMEM((n_dc, n_j), F32),
            pltpu.VMEM((n_j, n_v), BF16), pltpu.VMEM((n_j, n_v), BF16), pltpu.VMEM((2 * n_dc, n_j), BF16),
            *sum_scratch(n_j, n_v) * 2, *sum_scratch(n_j, n_v // 2) * 4,
            *[pltpu.VMEM((n_dc // 2, n_j), BF16), pltpu.VMEM((n_dc // 4, n_j), BF16)] * 2,
            pltpu.SemaphoreType.DMA((N_UTT,)), pltpu.SemaphoreType.DMA((RING,)), pltpu.SemaphoreType.DMA((3,)),
            pltpu.SemaphoreType.DMA((N_COPY,)), pltpu.SemaphoreType.DMA((N_COPY,)),
        ],
        compiler_params=pltpu.CompilerParams(collective_id=1, has_side_effects=True, vmem_limit_bytes=VMEM_FULL),
        name="joint_backward",
    )(labels, pred, z, h.reshape(n_cell, n_j), q0, q1, norm, w_out, enc)


def finish_kernel(loss, g_enc, g_out, g_dc, pred, pred_far, w_pred, da, w_enc, o_loss, o_enc, o_pred, o_wenc, o_wpred, o_wout,
                  v_enc, v_pred, v_wenc, v_wpred, v_wout, sem):
    y = lax.axis_index("data")
    o_loss[...] = loss[0:1, :N_UTT]
    jobs = []

    def put(src, dst, i):
        cp = pltpu.make_async_copy(src, dst, sem.at[i])
        cp.start()
        jobs.append(cp)

    v_wenc[...] = g_enc[...].astype(F32).T
    put(v_wenc, o_wenc, 0)
    v_wout[...] = g_out[...].astype(F32)
    put(v_wout, o_wout, 1)
    n_r = pred.shape[0]
    dc_own, dc_far = g_dc[rows_at(y * n_r, n_r), :], g_dc[rows_at((1 - y) * n_r, n_r), :]
    v_wpred[...] = dot(pred[...], dc_own, ((0,), (0,))) + dot(pred_far[...], dc_far, ((0,), (0,)))
    put(v_wpred, o_wpred, 2)
    v_pred[...] = dot(dc_own, w_pred[...], ((1,), (1,)))
    put(v_pred, o_pred, 3)
    v_enc[...] = dot(da[...], w_enc[...], ((1,), (1,))).astype(BF16)
    put(v_enc, o_enc, 4)
    for cp in jobs:
        cp.wait()


def finish(loss, g_enc, g_out, g_dc, pred, pred_far, w_pred, da, w_enc):
    vm = pl.BlockSpec(memory_space=pltpu.VMEM)
    outs = [(pred.shape, BF16), (pred.shape, F32), (w_pred.shape, F32), (w_pred.shape, F32), (w_pred.shape[::-1], F32)]
    return pl.pallas_call(
        finish_kernel,
        in_specs=[vm] * 9,
        out_specs=[vm] + [pl.BlockSpec(memory_space=pl.ANY)] * 5,
        out_shape=[jax.ShapeDtypeStruct((1, N_UTT), F32)] + [jax.ShapeDtypeStruct(*o) for o in outs],
        scratch_shapes=[pltpu.VMEM(*o) for o in outs] + [pltpu.SemaphoreType.DMA((5,))],
        compiler_params=pltpu.CompilerParams(vmem_limit_bytes=VMEM_FULL),
        name="finish",
    )(loss, g_enc, g_out, g_dc, pred, pred_far, w_pred, da, w_enc)


def solution(mesh):
    utt_rows = P(("part", "data"))
    utt_mats = P(("part", "data"), None)
    utt_cube = P(("part", "data"), None, None)
    enc_spec = P(("part", "data"), "seq", None)
    weight_in = P(None, None)
    weight_out = P("part", None)

    def body(enc_loc, pred_loc, w_enc, w_pred, w_out, labels, frame_len, label_len):
        n_h = enc_loc.shape[2]
        enc2 = enc_loc.reshape(N_UTT * T_LOC, n_h)
        pred2 = pred_loc.reshape(N_UTT * N_UP, n_h)
        z, h, stat, norm = joint_forward(labels, enc2, pred2, w_enc, w_pred, w_out)
        q0, q1, norm, loss = lattice(stat, norm, frame_len, label_len)
        da, g_enc, g_out, g_dc, pred_far = joint_backward(labels, pred2, z, h, q0, q1, norm, w_out, enc2)
        loss, grad_enc, grad_pred, grad_w_enc, grad_w_pred, grad_w_out = finish(loss, g_enc, g_out, g_dc, pred2, pred_far, w_pred, da, w_enc)
        return loss.reshape(N_UTT), grad_enc.reshape(enc_loc.shape), grad_pred.reshape(pred_loc.shape), grad_w_enc, grad_w_pred, grad_w_out

    return jax.shard_map(body, mesh=mesh, in_specs=(enc_spec, utt_cube, weight_in, weight_in, weight_in, utt_mats, utt_rows, utt_rows), out_specs=(utt_rows, enc_spec, utt_cube, weight_out, weight_out, weight_out), check_vma=False)
```

```python
import functools

import jax
import jax.numpy as jnp
from jax import lax
from jax.experimental import pallas as pl
from jax.experimental.pallas import tpu as pltpu
from jax.sharding import PartitionSpec as P

NEG = -1e30
SUB = 8
LANES = 128
LOG2E = 1.4426950408889634
LN2 = 0.6931471805599453
F32 = jnp.float32
BF16 = jnp.bfloat16
MESH = pl.DeviceIdType.MESH
VMEM_FULL = 67_000_000
N_UTT = 16
T_LOC = 24
N_UP = 24
UG = 3
N_SEQ = 4
T_ALL = T_LOC * N_SEQ
RING = 4
N_DIAG = T_ALL + N_UP - 1
ROWS = SUB * T_LOC


def dot(lhs, rhs, dims=((1,), (0,))):
    return lax.dot_general(lhs, rhs, (dims, ((), ())), preferred_element_type=F32)


def label_column(labels, utt, ug, sub):
    col = jnp.zeros((SUB, LANES), jnp.int32)
    for k in range(SUB):
        col = jnp.where(sub == k, labels[utt, jnp.minimum(ug * SUB + k, N_UP - 2)], col)
    return col


def forward_kernel(labels, llen, enc, pred, w_enc, w_pred, w_out, z_hbm, h_hbm, stat_out, norm_out, act_e, act_p, h_next, z_last, z_ring, h_ring, z_sem, h_sem):
    step = pl.program_id(0)
    lane = lax.broadcasted_iota(jnp.int32, (SUB, LANES), 1)
    sub = lax.broadcasted_iota(jnp.int32, (SUB, LANES), 0)
    n_v = w_out.shape[1]

    @pl.when(step == 0)
    def _():
        act_e[...] = dot(enc[...], w_enc[...]).astype(BF16).astype(F32)
        act_p[...] = dot(pred[...], w_pred[...]).astype(BF16).astype(F32)
        stat_out[...] = jnp.zeros_like(stat_out)
        norm_out[...] = jnp.zeros_like(norm_out)

    def hidden(utt, ug, dst):
        row = pl.multiple_of(utt * N_UP, SUB)
        c_grp = act_p[pl.ds(row + SUB * ug, SUB), :]
        a_utt = act_e[pl.ds(row, T_LOC), :]
        for t in range(0, T_LOC, 2):
            pre = jnp.concatenate([a_utt[t:t + 1, :] + c_grp, a_utt[t + 1:t + 2, :] + c_grp], axis=0)
            dst[t * SUB:t * SUB + 16, :] = jnp.tanh(pre).astype(BF16)

    def soften(utt, ug, src):
        lab_grp = label_column(labels, jnp.maximum(utt, 0), ug, sub)
        masks = [lab_grp - LANES * k == lane for k in range(n_v // LANES)]
        for t4 in range(T_LOC // 4):
            cur = stat_out[ug * 6 + t4]
            for k in range(4):
                t = t4 * 4 + k
                z = [src[t * SUB:t * SUB + SUB, c * LANES:c * LANES + LANES] for c in range(n_v // LANES)]
                top = functools.reduce(jnp.maximum, z)
                tot = functools.reduce(jnp.add, [jnp.exp2((v - top) * LOG2E) for v in z])
                picked = functools.reduce(jnp.add, [jnp.where(m, v, 0.0) for m, v in zip(masks, z)])
                row_top = jnp.max(top, axis=1, keepdims=True)
                row_tot = jnp.sum(tot * jnp.exp2((top - row_top) * LOG2E), axis=1, keepdims=True)
                norm = row_top * LOG2E + jnp.log2(row_tot)
                blank = z[0][:, 0:1] * LOG2E - norm
                label = jnp.sum(picked, axis=1, keepdims=True) * LOG2E - norm
                cur = jnp.where(lane == utt + 32 * k, blank, cur)
                cur = jnp.where(lane == utt + 32 * k + 16, label, cur)
                norm_out[ug * T_LOC + t] = jnp.where(lane == utt, norm, norm_out[ug * T_LOC + t])
            stat_out[ug * 6 + t4] = cur

    def puts(utt):
        at = lax.rem(utt, RING)
        return (pltpu.make_async_copy(z_ring.at[at], z_hbm.at[utt], z_sem.at[at]),
                pltpu.make_async_copy(h_ring.at[at], h_hbm.at[utt], h_sem.at[at]))

    @pl.when(step == 0)
    def _():
        hidden(0, 0, h_next)

    @pl.when(step >= RING)
    def _():
        for cp in puts(step - RING):
            cp.wait()

    slot = lax.rem(step, RING)
    z_out, h_out = z_ring.at[slot], h_ring.at[slot]
    groups = lax.div(llen[step], SUB) + 1
    last_of = lambda utt: lax.div(llen[utt], SUB)

    def utterance(n_grp):
        h_out[0] = h_next[...]
        for ug in range(n_grp):
            z = dot(h_out[ug] if ug else h_next[...], w_out[...])
            z_out[ug] = z
            if ug == 0:
                soften(step - 1, last_of(jnp.maximum(step - 1, 0)), z_last)
            else:
                soften(step, ug - 1, z_out.at[ug - 1])
            if ug < n_grp - 1:
                hidden(step, ug + 1, h_out.at[ug + 1])
            else:
                z_last[...] = z
                hidden(jnp.minimum(step + 1, N_UTT - 1), 0, h_next)

        if n_grp < UG:
            @pl.when(step < RING)
            def _():
                for ug in range(n_grp, UG):
                    z_out[ug] = jnp.zeros(z_out.shape[1:], F32)
                    h_out[ug] = jnp.zeros(h_out.shape[1:], BF16)

    for n_grp in range(1, UG + 1):
        pl.when(groups == n_grp)(functools.partial(utterance, n_grp))
    for cp in puts(step):
        cp.start()

    @pl.when(step == N_UTT - 1)
    def _():
        soften(step, last_of(step), z_last)
        for back in range(RING - 1, -1, -1):
            for cp in puts(step - back):
                cp.wait()


def joint_forward(labels, llen, enc, pred, w_enc, w_pred, w_out):
    n_j, n_v = w_out.shape
    full = lambda shape: pl.BlockSpec(shape, lambda i: (0,) * len(shape), pipeline_mode=pl.Buffered(1))
    return pl.pallas_call(
        forward_kernel,
        grid=(N_UTT,),
        in_specs=[pl.BlockSpec(memory_space=pltpu.SMEM)] * 2 + [full(v.shape) for v in (enc, pred, w_enc, w_pred, w_out)],
        out_specs=[
            pl.BlockSpec(memory_space=pl.ANY),
            pl.BlockSpec(memory_space=pl.ANY),
            pl.BlockSpec((UG * 6, SUB, LANES), lambda i: (0, 0, 0)),
            pl.BlockSpec((UG * T_LOC, SUB, LANES), lambda i: (0, 0, 0)),
        ],
        out_shape=[
            jax.ShapeDtypeStruct((N_UTT, UG, ROWS, n_v), F32),
            jax.ShapeDtypeStruct((N_UTT, UG, ROWS, n_j), BF16),
            jax.ShapeDtypeStruct((UG * 6, SUB, LANES), F32),
            jax.ShapeDtypeStruct((UG * T_LOC, SUB, LANES), F32),
        ],
        scratch_shapes=[pltpu.VMEM((N_UTT * T_LOC, n_j), F32), pltpu.VMEM((N_UTT * N_UP, n_j), F32), pltpu.VMEM((ROWS, n_j), BF16), pltpu.VMEM((ROWS, n_v), F32),
            pltpu.VMEM((RING, UG, ROWS, n_v), F32), pltpu.VMEM((RING, UG, ROWS, n_j), BF16),
            pltpu.SemaphoreType.DMA((RING,)), pltpu.SemaphoreType.DMA((RING,))],
        compiler_params=pltpu.CompilerParams(vmem_limit_bytes=VMEM_FULL),
        name="joint_forward",
    )(labels, llen, enc, pred, w_enc, w_pred, w_out)


def lae2(x, y):
    return jnp.maximum(x, y) + jnp.log2(1.0 + jnp.exp2(-jnp.abs(x - y)))


def lattice_kernel(stat, norm, flen, llen, q0_out, q1_out, norm_out, loss_out, gath, s_blank, s_label, s_alpha, s_beta, send_sem, recv_sem):
    me = lax.axis_index("seq")
    barrier = pltpu.get_barrier_semaphore()
    for off in range(1, N_SEQ):
        pl.semaphore_signal(barrier, inc=1, device_id={"seq": lax.rem(me + off, N_SEQ)}, device_id_type=MESH)
    pl.semaphore_wait(barrier, N_SEQ - 1)
    copies = []
    for off in range(1, N_SEQ):
        cp = pltpu.make_async_remote_copy(
            src_ref=stat, dst_ref=gath.at[off - 1], send_sem=send_sem.at[off - 1], recv_sem=recv_sem.at[off - 1],
            device_id={"seq": lax.rem(me + off, N_SEQ)}, device_id_type=MESH)
        cp.start()
        copies.append(cp)

    sub = lax.broadcasted_iota(jnp.int32, (SUB, LANES), 0)
    sub24 = lax.broadcasted_iota(jnp.int32, (N_UP, LANES), 0)
    lane = lax.broadcasted_iota(jnp.int32, (SUB, LANES), 1)
    tb = jnp.zeros((SUB, LANES), jnp.int32)
    ub = jnp.zeros((SUB, LANES), jnp.int32)
    for b in range(N_UTT):
        at_b = lax.rem(lane, N_UTT) == b
        tb = jnp.where(at_b, flen[b], tb)
        ub = jnp.where(at_b, llen[b], ub)
    n_pad = s_blank.shape[0]

    def fill(i, c):
        s_blank[pl.ds(pl.multiple_of(i * SUB, SUB), SUB), :] = jnp.full((SUB, LANES), NEG, F32)
        s_label[pl.ds(pl.multiple_of(i * SUB, SUB), SUB), :] = jnp.full((SUB, LANES), NEG, F32)
        return c

    lax.fori_loop(0, n_pad // SUB, fill, 0, unroll=SUB)
    end_grp = [jnp.where(sub + SUB * ug == ub, 0.0, NEG) for ug in range(UG)]
    for t in range(T_ALL, T_ALL + N_UP):
        for ug in range(UG):
            s_blank[pl.ds(t * N_UP + 200 * ug, SUB, stride=25), :] = end_grp[ug]

    def place(src, src_seq):
        for t4 in range(T_LOC // 4):
            for ug in range(UG):
                val = src[ug * 6 + t4]
                in_u = sub + SUB * ug <= ub
                in_l = sub + SUB * ug < ub
                for k in range(4):
                    t = src_seq * T_LOC + t4 * 4 + k
                    bl = val if k == 0 else pltpu.roll(val, LANES - 32 * k, 1)
                    la = pltpu.roll(val, 112 - 32 * k, 1)
                    ok = t < tb
                    s_blank[pl.ds(t * N_UP + 200 * ug, SUB, stride=25), :] = jnp.where(ok, jnp.where(in_u, bl, NEG), end_grp[ug])
                    s_label[pl.ds(t * N_UP + 200 * ug, SUB, stride=25), :] = jnp.where(ok & in_l, la, NEG)

    place(stat, me)
    for off in range(1, N_SEQ):
        copies[off - 1].wait_recv()
        place(gath.at[off - 1], lax.rem(me + N_SEQ - off, N_SEQ))

    alpha0 = jnp.where(sub24 == 0, 0.0, NEG)
    s_alpha[pl.ds(0, N_UP), :] = alpha0
    beta_end = jnp.where(sub24 == jnp.concatenate([ub] * UG, axis=0), 0.0, NEG)
    s_beta[pl.ds(N_DIAG * N_UP, N_UP), :] = beta_end
    s_beta[pl.ds((N_DIAG + 1) * N_UP, SUB), :] = jnp.full((SUB, LANES), NEG, F32)

    def wave(i, carry):
        alpha, beta = carry
        row = pl.multiple_of(i * N_UP, SUB)
        x = alpha + s_blank[pl.ds(row, N_UP), :]
        y = alpha + s_label[pl.ds(row, N_UP), :]
        y = jnp.where(sub24 == 0, NEG, pltpu.roll(y, 1, 0))
        alpha = lae2(x, y)
        s_alpha[pl.ds(pl.multiple_of(row + N_UP, SUB), N_UP), :] = alpha
        brow = pl.multiple_of((N_DIAG - 1 - i) * N_UP, SUB)
        bx = beta + s_blank[pl.ds(brow, N_UP), :]
        by = pltpu.roll(beta, N_UP - 1, 0) + s_label[pl.ds(brow, N_UP), :]
        beta = lae2(bx, by)
        s_beta[pl.ds(brow, N_UP), :] = beta
        return alpha, beta

    _, beta = lax.fori_loop(0, N_DIAG, wave, (alpha0, beta_end), unroll=7)
    log_p = beta[0:1, :]
    loss_out[...] = jnp.broadcast_to(-LN2 * log_p, (SUB, LANES))
    for t in range(T_LOC):
        tg = me * T_LOC + t
        for ug in range(UG):
            base = tg * N_UP + 200 * ug
            grp = lambda ref, off: ref[pl.ds(base + off, SUB, stride=25), :]
            al = grp(s_alpha, 0) - log_p
            ok = (tg < tb) & (sub + SUB * ug <= ub)
            q0 = jnp.where(ok, jnp.exp2(al + grp(s_blank, 0) + grp(s_beta, 24)), 0.0)
            q1 = jnp.where(ok, jnp.exp2(al + grp(s_label, 0) + grp(s_beta, 25)), 0.0)
            idx = ug * T_LOC + t
            q0_out[idx] = q0
            q1_out[idx] = q1
            norm_out[idx] = norm[idx] - jnp.log2(q0 + q1)
    for cp in copies:
        cp.wait_send()


def lattice(stat, norm, flen, llen):
    vm = pl.BlockSpec(memory_space=pltpu.VMEM)
    n_rows = (T_ALL + 2 * N_UP) * N_UP
    return pl.pallas_call(
        lattice_kernel,
        in_specs=[vm] * 2 + [pl.BlockSpec(memory_space=pltpu.SMEM)] * 2,
        out_specs=[vm] * 4,
        out_shape=[jax.ShapeDtypeStruct((UG * T_LOC, SUB, LANES), F32)] * 3 + [jax.ShapeDtypeStruct((SUB, LANES), F32)],
        scratch_shapes=[pltpu.VMEM((N_SEQ - 1,) + stat.shape, F32)] + [pltpu.VMEM((n_rows, LANES), F32)] * 4
        + [pltpu.SemaphoreType.DMA((N_SEQ - 1,)), pltpu.SemaphoreType.DMA((N_SEQ - 1,))],
        compiler_params=pltpu.CompilerParams(collective_id=0, has_side_effects=True),
        name="lattice",
    )(stat, norm, flen, llen)


class Links:
    def __init__(self, send_sem, recv_sem):
        self.send_sem, self.recv_sem, self.copies = send_sem, recv_sem, []
        seq = lax.axis_index("seq")
        self.core = lax.rem(seq, 2)
        self.x = lax.div(seq, 2)
        self.y = lax.axis_index("data")
        self.dev = {
            "core": {"seq": seq + 1 - 2 * self.core},
            "x": {"seq": lax.rem(seq + 2, N_SEQ)},
            "y": {"data": 1 - self.y},
        }

    def greet(self):
        barrier = pltpu.get_barrier_semaphore()
        for dev in self.dev.values():
            pl.semaphore_signal(barrier, inc=1, device_id=dev, device_id_type=MESH)
        pl.semaphore_wait(barrier, 3)

    def copy(self, ends, axis):
        i = len(self.copies)

        def make():
            src, dst = ends()
            return pltpu.make_async_remote_copy(src_ref=src, dst_ref=dst, send_sem=self.send_sem.at[i], recv_sem=self.recv_sem.at[i],
                                                device_id=self.dev[axis], device_id_type=MESH)

        self.copies.append(make)
        return make


def rows_at(start, size):
    return pl.ds(pl.multiple_of(start, 16), size)


def sum_stages(links, acc, gat, stg, rcv, col0, n_col):
    half = acc.shape[0] // 2
    h0 = links.core * half
    every = pl.ds(col0, n_col)
    box = []
    for q in range(2):
        first, second = ("x", "y") if q == 0 else ("y", "x")
        k1, k2 = (links.x, links.y) if q == 0 else (links.y, links.x)
        box.append((q, first, second, k1, k2, pl.ds(col0 + q * (n_col // 2), n_col // 2)))
    n2, n4 = half // 2, half // 4

    def same(rows, cols):
        def ends():
            ref = gat.at[rows(), cols]
            return ref, ref
        return ends

    swap = links.copy(lambda: (stg[0], rcv[0]), "core")
    back = links.copy(same(lambda: rows_at(h0, half), every), "core")
    hops = [(
        links.copy(lambda q=q: (stg[1].at[q], rcv[1].at[q]), first),
        links.copy(lambda q=q: (stg[2].at[q], rcv[2].at[q]), second),
        links.copy(same(lambda k1=k1, k2=k2: rows_at(h0 + k1 * n2 + k2 * n4, n4), cols), second),
        links.copy(same(lambda k1=k1: rows_at(h0 + k1 * n2, n2), cols), first),
    ) for q, first, second, k1, k2, cols in box]

    def s1():
        stg[0][...] = acc[rows_at((1 - links.core) * half, half), every].astype(BF16)
        swap().start()

    def s2():
        swap().wait_recv()
        own = rows_at(h0, half)
        acc[own, every] = acc[own, every] + rcv[0][...].astype(F32)
        for q, first, second, k1, k2, cols in box:
            stg[1][q] = acc[rows_at(h0 + (1 - k1) * n2, n2), cols].astype(BF16)
            hops[q][0]().start()

    def s3():
        for q, first, second, k1, k2, cols in box:
            hops[q][0]().wait_recv()
            part = rows_at((1 - k2) * n4, n4)
            stg[2][q] = (acc[rows_at(h0 + k1 * n2 + (1 - k2) * n4, n4), cols] + rcv[1][q, part].astype(F32)).astype(BF16)
            hops[q][1]().start()

    def s4():
        for q, first, second, k1, k2, cols in box:
            hops[q][1]().wait_recv()
            part = rows_at(k2 * n4, n4)
            own = rows_at(h0 + k1 * n2 + k2 * n4, n4)
            gat[own, cols] = (acc[own, cols] + rcv[1][q, part].astype(F32) + rcv[2][q].astype(F32)).astype(BF16)
            hops[q][2]().start()

    def s5():
        for hop in hops:
            hop[2]().wait_recv()
            hop[3]().start()

    def s6():
        for hop in hops:
            hop[3]().wait_recv()
        back().start()

    def s7():
        back().wait_recv()

    return [s1, s2, s3, s4, s5, s6, s7]


def dc_stages(links, src, gat, stg, rcv):
    n_row = src.shape[0]
    half, quar, eigh = n_row // 2, n_row // 4, n_row // SUB
    h0 = links.core * half
    r0 = h0 + links.x * quar
    r_far = h0 + (1 - links.x) * quar
    y_own, y_far = links.y * n_row, (1 - links.y) * n_row

    def hop(start, size, axis):
        def ends():
            ref = gat.at[rows_at(start(), size), :]
            return ref, ref
        return links.copy(ends, axis)

    swap = links.copy(lambda: (stg[0], rcv[0]), "core")
    cross = links.copy(lambda: (stg[1], rcv[1]), "x")
    up_y = hop(lambda: y_own + r0, eigh, "y")
    down_x = hop(lambda: y_own + r0 + eigh, eigh, "x")
    up_x = hop(lambda: y_own + r0, eigh, "x")
    down_y = hop(lambda: y_own + r0 + eigh, eigh, "y")
    up_far = hop(lambda: y_far + r0, eigh, "x")
    down_far = hop(lambda: y_own + r_far + eigh, eigh, "y")
    back = [hop(lambda: y_own + h0, half, "core"), hop(lambda: y_far + h0, half, "core")]

    def s1():
        stg[0][...] = src[rows_at((1 - links.core) * half, half), :].astype(BF16)
        swap().start()

    def s2():
        swap().wait_recv()
        part = rows_at((1 - links.x) * quar, quar)
        stg[1][...] = (src[rows_at(r_far, quar), :] + rcv[0][part, :].astype(F32)).astype(BF16)
        cross().start()

    def s3():
        cross().wait_recv()
        part = rows_at(links.x * quar, quar)
        total = src[rows_at(r0, quar), :] + rcv[0][part, :].astype(F32) + rcv[1][...].astype(F32)
        gat[rows_at(y_own + r0, quar), :] = total.astype(BF16)
        for cp in (up_y, down_x, up_x, down_y):
            cp().start()

    def s4():
        up_y().wait_recv()
        up_far().start()
        down_x().wait_recv()
        down_far().start()

    def s5():
        for cp in (up_x, down_y, up_far, down_far):
            cp().wait_recv()
        for cp in back:
            cp().start()

    def s6():
        for cp in back:
            cp().wait_recv()

    return [s1, s2, s3, s4, s5, s6]


N_COPY = 10 * 5 + 1


def sum_scratch(n_row, n_col):
    half = n_row // 2
    return [pltpu.VMEM((half, n_col), BF16), pltpu.VMEM((2, half // 2, n_col // 2), BF16), pltpu.VMEM((2, half // 4, n_col // 2), BF16)]


W_CHUNK = 256


def backward_kernel(labels, pred, z_hbm, h_hbm, q0_ref, q1_ref, norm_ref, w_out, enc, da_out, g_enc_out, g_out_out, g_dc_out, far_out,
                    dz_all, h_all, da_all, da_part, dz0, dz1, dz2, dh0, dh1, dh2, w_out_t, z_ring, dw_enc, dw_out, dc_out, g_enc, g_out, g_dc,
                    es0, es1, es2, er0, er1, er2, ps0, ps1, ps2, pr0, pr1, pr2, qs0, qs1, qs2, qr0, qr1, qr2, rs0, rs1, rs2, rr0, rr1, rr2, ds0, ds1, dr0, dr1,
                    h_sem, z_sem, o_sem, send_sem, recv_sem):
    step = pl.program_id(0)
    lane = lax.broadcasted_iota(jnp.int32, (SUB, LANES), 1)
    sub = lax.broadcasted_iota(jnp.int32, (SUB, LANES), 0)
    n_j, n_v = w_out.shape
    utt_rows = UG * ROWS

    dzs, dhs = (dz0, dz1, dz2), (dh0, dh1, dh2)
    prev = jnp.maximum(step - 1, 0)
    z_slot = lax.rem(step, RING)

    def multiply(ug):
        dhs[ug][...] = dot(dzs[ug][...], w_out_t[...])[:, :n_j]

    def h_copy(utt):
        rows = pl.ds(pl.multiple_of(utt * utt_rows, 16), utt_rows)
        return pltpu.make_async_copy(h_hbm.at[rows, :], h_all.at[rows, :], h_sem.at[utt])

    def z_copy(utt):
        slot = lax.rem(utt, RING)
        return pltpu.make_async_copy(z_hbm.at[utt], z_ring.at[slot], z_sem.at[slot])

    links = Links(send_sem, recv_sem)
    far = links.copy(lambda: (pred, far_out), "y")
    e_st = sum_stages(links, dw_enc, g_enc, (es0, es1, es2), (er0, er1, er2), 0, n_v)
    p_st = sum_stages(links, dw_out, g_out, (ps0, ps1, ps2), (pr0, pr1, pr2), 0, n_v // 2)
    q_st = sum_stages(links, dw_out, g_out, (qs0, qs1, qs2), (qr0, qr1, qr2), n_v // 2, n_v // 4)
    r_st = sum_stages(links, dw_out, g_out, (rs0, rs1, rs2), (rr0, rr1, rr2), n_v // 2 + n_v // 4, n_v // 4)
    c_st = dc_stages(links, dc_out, g_dc, (ds0, ds1), (dr0, dr1))

    @pl.when(step == 0)
    def _():
        links.greet()
        far().start()
        for utt in range(RING - 1):
            z_copy(utt).start()
            h_copy(utt).start()
        w_out_t[:, :n_j] = w_out[...].T
        w_out_t[:, n_j:] = jnp.zeros((n_v, w_out_t.shape[1] - n_j), BF16)

    def logit_grads(ug):
        shift = LANES - step
        lab_grp = label_column(labels, step, ug, sub)
        masks = [lab_grp - LANES * k == lane for k in range(n_v // LANES)]
        for t in range(0, T_LOC, 2):
            pair = []
            for idx in (ug * T_LOC + t, ug * T_LOC + t + 1):
                q0, q1, norm = [jnp.broadcast_to(pltpu.roll(ref[idx], shift, 1)[:, 0:1], (SUB, LANES)) for ref in (q0_ref, q1_ref, norm_ref)]
                row = (idx - ug * T_LOC) * SUB
                tiles = []
                for k in range(n_v // LANES):
                    z = z_ring[z_slot, ug, row:row + SUB, k * LANES:k * LANES + LANES]
                    g = jnp.exp2(z * LOG2E - norm) - jnp.where(masks[k], q1, 0.0)
                    tiles.append(g - jnp.where(lane == 0, q0, 0.0) if k == 0 else g)
                pair.append(jnp.concatenate(tiles, axis=1))
            rows = pl.ds(pl.multiple_of(step * utt_rows + ug * ROWS + t * SUB, 16), 16)
            dz = jnp.concatenate(pair, axis=0).astype(BF16)
            dz_all[rows, :] = dz
            dzs[ug][t * SUB:t * SUB + 16, :] = dz

    def hidden_grads(utt, ug):
        dc = None
        for t in range(0, T_LOC, 2):
            hid = h_all[pl.ds(pl.multiple_of(utt * utt_rows + ug * ROWS + t * SUB, 16), 16), :].astype(F32)
            ds = dhs[ug][t * SUB:t * SUB + 16, :] * (1.0 - hid * hid)
            both = ds[:SUB] + ds[SUB:]
            dc = both if dc is None else dc + both
            if ug > 0:
                ds = ds + da_part[t * SUB:t * SUB + 16, :]
            if ug < UG - 1:
                da_part[t * SUB:t * SUB + 16, :] = ds
            else:
                for k in range(2):
                    da_all[pl.ds(utt * T_LOC + t + k, 1), :] = jnp.sum(ds[SUB * k:SUB * k + SUB], axis=0, keepdims=True)
        dc_out[pl.ds(pl.multiple_of(utt * N_UP + ug * SUB, SUB), SUB), :] = dc

    @pl.when(step + RING - 1 < N_UTT)
    def _():
        z_copy(step + RING - 1).start()
        h_copy(step + RING - 1).start()

    @pl.when(step < N_UTT)
    def _():
        h_copy(step).wait()
        z_copy(step).wait()
        multiply(2)
        logit_grads(0)
        hidden_grads(prev, 1)
        multiply(0)
        logit_grads(1)
        hidden_grads(prev, 2)
        multiply(1)
        logit_grads(2)
        hidden_grads(step, 0)

    @pl.when(step == N_UTT)
    def _():
        multiply(2)
        hidden_grads(prev, 1)
        hidden_grads(prev, 2)
        da = da_all[...].astype(BF16)
        da_out[...] = da
        dw_enc[...] = dot(da, enc[...], ((0,), (0,)))
        e_st[0]()
        c_st[0]()

    plan = [
        ((c_st[1], e_st[1]), ()),
        ((), (c_st[2], p_st[0])),
        ((e_st[2], p_st[1]), ()),
        ((e_st[3], q_st[0]), (
            r_st[0], p_st[2], q_st[1], r_st[1], c_st[3], p_st[3], r_st[2], q_st[2], e_st[4], c_st[4], q_st[3], r_st[3], p_st[4],
            q_st[4], r_st[4], p_st[5], e_st[5], q_st[5])),
    ]
    for part, (lo, hi) in enumerate(((0, 3 * LANES), (3 * LANES, n_j))):
        @pl.when(step > N_UTT)
        def _(lo=lo, hi=hi):
            cols = pl.ds(pl.multiple_of((step - N_UTT - 1) * W_CHUNK, W_CHUNK), W_CHUNK)
            dw_out[lo:hi, cols] = dot(h_all[:, lo:hi], dz_all[:, cols], ((0,), (0,)))

        for n, stages in enumerate(plan):
            if stages[part]:
                @pl.when(step == N_UTT + 1 + n)
                def _(stages=stages[part]):
                    for stage in stages:
                        stage()

    @pl.when(step == N_UTT + len(plan))
    def _():
        p_st[6]()
        r_st[5]()
        r_st[6]()
        e_st[6]()
        out_enc = pltpu.make_async_copy(g_enc, g_enc_out, o_sem.at[1])
        out_enc.start()
        q_st[6]()
        out_out = pltpu.make_async_copy(g_out, g_out_out, o_sem.at[2])
        out_out.start()
        c_st[5]()
        out_dc = pltpu.make_async_copy(g_dc, g_dc_out, o_sem.at[0])
        out_dc.start()
        far().wait_recv()
        for cp in links.copies:
            cp().wait_send()
        out_dc.wait()
        out_enc.wait()
        out_out.wait()


def joint_backward(labels, pred, z, h, q0, q1, norm, w_out, enc):
    n_j, n_v = w_out.shape
    n_cell = N_UTT * UG * ROWS
    n_dc = N_UTT * N_UP
    full = lambda shape: pl.BlockSpec(shape, lambda i: (0,) * len(shape), pipeline_mode=pl.Buffered(1))
    return pl.pallas_call(
        backward_kernel,
        grid=(N_UTT + 1 + n_v // W_CHUNK,),
        in_specs=[
            pl.BlockSpec(memory_space=pltpu.SMEM),
            *[pl.BlockSpec(memory_space=pl.ANY)] * 3,
            full(q0.shape), full(q1.shape), full(norm.shape), full(w_out.shape), full(enc.shape),
        ],
        out_specs=[full((N_UTT * T_LOC, n_j))] + [pl.BlockSpec(memory_space=pl.ANY)] * 4,
        out_shape=[
            jax.ShapeDtypeStruct((N_UTT * T_LOC, n_j), BF16),
            jax.ShapeDtypeStruct((n_j, n_v), BF16),
            jax.ShapeDtypeStruct((n_j, n_v), BF16),
            jax.ShapeDtypeStruct((2 * n_dc, n_j), BF16),
            jax.ShapeDtypeStruct(pred.shape, BF16),
        ],
        scratch_shapes=[
            pltpu.VMEM((n_cell, n_v), BF16), pltpu.VMEM((n_cell, n_j), BF16), pltpu.VMEM((N_UTT * T_LOC, n_j), F32),
            pltpu.VMEM((ROWS, n_j), F32),
            *[pltpu.VMEM((ROWS, n_v), BF16)] * 3, *[pltpu.VMEM((ROWS, n_j), F32)] * 3,
            pltpu.VMEM((n_v, n_j + (-n_j) % 256), BF16), pltpu.VMEM((RING, UG, ROWS, n_v), F32),
            pltpu.VMEM((n_j, n_v), F32), pltpu.VMEM((n_j, n_v), F32), pltpu.VMEM((n_dc, n_j), F32),
            pltpu.VMEM((n_j, n_v), BF16), pltpu.VMEM((n_j, n_v), BF16), pltpu.VMEM((2 * n_dc, n_j), BF16),
            *sum_scratch(n_j, n_v) * 2, *sum_scratch(n_j, n_v // 2) * 2, *sum_scratch(n_j, n_v // 4) * 4,
            *[pltpu.VMEM((n_dc // 2, n_j), BF16), pltpu.VMEM((n_dc // 4, n_j), BF16)] * 2,
            pltpu.SemaphoreType.DMA((N_UTT,)), pltpu.SemaphoreType.DMA((RING,)), pltpu.SemaphoreType.DMA((3,)),
            pltpu.SemaphoreType.DMA((N_COPY,)), pltpu.SemaphoreType.DMA((N_COPY,)),
        ],
        compiler_params=pltpu.CompilerParams(collective_id=1, has_side_effects=True, vmem_limit_bytes=VMEM_FULL),
        name="joint_backward",
    )(labels, pred, z, h.reshape(n_cell, n_j), q0, q1, norm, w_out, enc)


def finish_kernel(loss, *refs):
    ins, o_loss, outs = refs[:FIN_IN], refs[FIN_IN], refs[FIN_IN + 1:FIN_IN + 1 + FIN_OUT]
    bufs, vals, in_sem, out_sem = refs[FIN_IN + 1 + FIN_OUT:-FIN_OUT - 2], refs[-FIN_OUT - 2:-2], refs[-2], refs[-1]
    g_out, g_enc, da, w_enc, g_dc, w_pred, pred, pred_far = bufs
    v_wout, v_wenc, v_enc, v_pred, v_wpred = vals
    loads = [pltpu.make_async_copy(src, dst, in_sem.at[k]) for k, (src, dst) in enumerate(zip(ins, bufs))]
    stores = [pltpu.make_async_copy(src, dst, out_sem.at[k]) for k, (src, dst) in enumerate(zip(vals, outs))]
    for cp in loads:
        cp.start()
    y = lax.axis_index("data")
    n_r = pred.shape[0]
    o_loss[...] = loss[0:1, :N_UTT]
    loads[0].wait()
    v_wout[...] = g_out[...].astype(F32)
    stores[0].start()
    loads[1].wait()
    v_wenc[...] = g_enc[...].astype(F32).T
    stores[1].start()
    loads[2].wait()
    loads[3].wait()
    v_enc[...] = dot(da[...], w_enc[...], ((1,), (1,))).astype(BF16)
    stores[2].start()
    loads[4].wait()
    loads[5].wait()
    dc_own = g_dc[rows_at(y * n_r, n_r), :]
    dc_far = g_dc[rows_at((1 - y) * n_r, n_r), :]
    v_pred[...] = dot(dc_own, w_pred[...], ((1,), (1,)))
    stores[3].start()
    loads[6].wait()
    loads[7].wait()
    v_wpred[...] = dot(pred[...], dc_own, ((0,), (0,))) + dot(pred_far[...], dc_far, ((0,), (0,)))
    stores[4].start()
    for cp in stores:
        cp.wait()


FIN_IN = 8
FIN_OUT = 5


def finish(loss, g_enc, g_out, g_dc, pred, pred_far, w_pred, da, w_enc):
    vm = pl.BlockSpec(memory_space=pltpu.VMEM)
    hbm = pl.BlockSpec(memory_space=pl.ANY)
    ins = (g_out, g_enc, da, w_enc, g_dc, w_pred, pred, pred_far)
    outs = [(g_out.shape, F32), (w_enc.shape, F32), (pred.shape, BF16), (pred.shape, F32), (w_pred.shape, F32)]
    loss, grad_w_out, grad_w_enc, grad_enc, grad_pred, grad_w_pred = pl.pallas_call(
        finish_kernel,
        in_specs=[vm] + [hbm] * FIN_IN,
        out_specs=[vm] + [hbm] * FIN_OUT,
        out_shape=[jax.ShapeDtypeStruct((1, N_UTT), F32)] + [jax.ShapeDtypeStruct(*o) for o in outs],
        scratch_shapes=[pltpu.VMEM(v.shape, v.dtype) for v in ins] + [pltpu.VMEM(*o) for o in outs]
        + [pltpu.SemaphoreType.DMA((FIN_IN,)), pltpu.SemaphoreType.DMA((FIN_OUT,))],
        compiler_params=pltpu.CompilerParams(vmem_limit_bytes=VMEM_FULL),
        name="finish",
    )(loss, *ins)
    return loss, grad_enc, grad_pred, grad_w_enc, grad_w_pred, grad_w_out


def solution(mesh):
    utt_rows = P(("part", "data"))
    utt_mats = P(("part", "data"), None)
    utt_cube = P(("part", "data"), None, None)
    enc_spec = P(("part", "data"), "seq", None)
    weight_in = P(None, None)
    weight_out = P("part", None)

    def body(enc_loc, pred_loc, w_enc, w_pred, w_out, labels, frame_len, label_len):
        n_h = enc_loc.shape[2]
        enc2 = enc_loc.reshape(N_UTT * T_LOC, n_h)
        pred2 = pred_loc.reshape(N_UTT * N_UP, n_h)
        z, h, stat, norm = joint_forward(labels, label_len, enc2, pred2, w_enc, w_pred, w_out)
        q0, q1, norm, loss = lattice(stat, norm, frame_len, label_len)
        da, g_enc, g_out, g_dc, pred_far = joint_backward(labels, pred2, z, h, q0, q1, norm, w_out, enc2)
        loss, grad_enc, grad_pred, grad_w_enc, grad_w_pred, grad_w_out = finish(loss, g_enc, g_out, g_dc, pred2, pred_far, w_pred, da, w_enc)
        return loss.reshape(N_UTT), grad_enc.reshape(enc_loc.shape), grad_pred.reshape(pred_loc.shape), grad_w_enc, grad_w_pred, grad_w_out

    return jax.shard_map(body, mesh=mesh, in_specs=(enc_spec, utt_cube, weight_in, weight_in, weight_in, utt_mats, utt_rows, utt_rows), out_specs=(utt_rows, enc_spec, utt_cube, weight_out, weight_out, weight_out), check_vma=False)
```

```python
import functools

import jax
import jax.numpy as jnp
from jax import lax
from jax.experimental import pallas as pl
from jax.experimental.pallas import tpu as pltpu
from jax.sharding import PartitionSpec as P

NEG = -1e30
SUB = 8
LANES = 128
LOG2E = 1.4426950408889634
LN2 = 0.6931471805599453
F32 = jnp.float32
BF16 = jnp.bfloat16
MESH = pl.DeviceIdType.MESH
VMEM_FULL = 67_000_000
N_UTT = 16
T_LOC = 24
N_UP = 24
UG = 3
N_SEQ = 4
T_ALL = T_LOC * N_SEQ
RING = 4
N_DIAG = T_ALL + N_UP - 1
ROWS = SUB * T_LOC


def dot(lhs, rhs, dims=((1,), (0,))):
    return lax.dot_general(lhs, rhs, (dims, ((), ())), preferred_element_type=F32)


def label_column(labels, utt, ug, sub):
    col = jnp.zeros((SUB, LANES), jnp.int32)
    for k in range(SUB):
        col = jnp.where(sub == k, labels[utt, jnp.minimum(ug * SUB + k, N_UP - 2)], col)
    return col


def forward_kernel(labels, llen, enc, pred, w_enc, w_pred, w_out, z_hbm, h_hbm, stat_out, norm_out, act_e, act_p, h_next, z_last, z_ring, h_ring, z_sem, h_sem):
    step = pl.program_id(0)
    lane = lax.broadcasted_iota(jnp.int32, (SUB, LANES), 1)
    sub = lax.broadcasted_iota(jnp.int32, (SUB, LANES), 0)
    n_v = w_out.shape[1]

    @pl.when(step == 0)
    def _():
        act_e[...] = dot(enc[...], w_enc[...]).astype(BF16).astype(F32)
        act_p[...] = dot(pred[...], w_pred[...]).astype(BF16).astype(F32)
        stat_out[...] = jnp.zeros_like(stat_out)
        norm_out[...] = jnp.zeros_like(norm_out)

    def hidden(utt, ug, dst):
        row = pl.multiple_of(utt * N_UP, SUB)
        c_grp = act_p[pl.ds(row + SUB * ug, SUB), :]
        a_utt = act_e[pl.ds(row, T_LOC), :]
        for t in range(0, T_LOC, 2):
            pre = jnp.concatenate([a_utt[t:t + 1, :] + c_grp, a_utt[t + 1:t + 2, :] + c_grp], axis=0)
            dst[t * SUB:t * SUB + 16, :] = jnp.tanh(pre).astype(BF16)

    def soften(utt, ug, src):
        lab_grp = label_column(labels, jnp.maximum(utt, 0), ug, sub)
        masks = [lab_grp - LANES * k == lane for k in range(n_v // LANES)]
        for t4 in range(T_LOC // 4):
            cur = stat_out[ug * 6 + t4]
            for k in range(4):
                t = t4 * 4 + k
                z = [src[t * SUB:t * SUB + SUB, c * LANES:c * LANES + LANES] for c in range(n_v // LANES)]
                top = functools.reduce(jnp.maximum, z)
                tot = functools.reduce(jnp.add, [jnp.exp2(v - top) for v in z])
                picked = functools.reduce(jnp.add, [jnp.where(m, v, 0.0) for m, v in zip(masks, z)])
                row_top = jnp.max(top, axis=1, keepdims=True)
                row_tot = jnp.sum(tot * jnp.exp2(top - row_top), axis=1, keepdims=True)
                norm = row_top + jnp.log2(row_tot)
                blank = z[0][:, 0:1] - norm
                label = jnp.sum(picked, axis=1, keepdims=True) - norm
                cur = jnp.where(lane == utt + 32 * k, blank, cur)
                cur = jnp.where(lane == utt + 32 * k + 16, label, cur)
                norm_out[ug * T_LOC + t] = jnp.where(lane == utt, norm, norm_out[ug * T_LOC + t])
            stat_out[ug * 6 + t4] = cur

    def puts(utt):
        at = lax.rem(utt, RING)
        return (pltpu.make_async_copy(z_ring.at[at], z_hbm.at[utt], z_sem.at[at]),
                pltpu.make_async_copy(h_ring.at[at], h_hbm.at[utt], h_sem.at[at]))

    @pl.when(step == 0)
    def _():
        hidden(0, 0, h_next)

    @pl.when(step >= RING)
    def _():
        for cp in puts(step - RING):
            cp.wait()

    slot = lax.rem(step, RING)
    z_out, h_out = z_ring.at[slot], h_ring.at[slot]
    groups = lax.div(llen[step], SUB) + 1
    last_of = lambda utt: lax.div(llen[utt], SUB)

    def utterance(n_grp):
        h_out[0] = h_next[...]
        for ug in range(n_grp):
            z = dot(h_out[ug] if ug else h_next[...], w_out[...]) * LOG2E
            z_out[ug] = z
            if ug == 0:
                soften(step - 1, last_of(jnp.maximum(step - 1, 0)), z_last)
            else:
                soften(step, ug - 1, z_out.at[ug - 1])
            if ug < n_grp - 1:
                hidden(step, ug + 1, h_out.at[ug + 1])
            else:
                z_last[...] = z
                hidden(jnp.minimum(step + 1, N_UTT - 1), 0, h_next)

        if n_grp < UG:
            @pl.when(step < RING)
            def _():
                for ug in range(n_grp, UG):
                    z_out[ug] = jnp.zeros(z_out.shape[1:], F32)
                    h_out[ug] = jnp.zeros(h_out.shape[1:], BF16)

    for n_grp in range(1, UG + 1):
        pl.when(groups == n_grp)(functools.partial(utterance, n_grp))
    for cp in puts(step):
        cp.start()

    @pl.when(step == N_UTT - 1)
    def _():
        soften(step, last_of(step), z_last)
        for back in range(RING - 1, -1, -1):
            for cp in puts(step - back):
                cp.wait()


def joint_forward(labels, llen, enc, pred, w_enc, w_pred, w_out):
    n_j, n_v = w_out.shape
    full = lambda shape: pl.BlockSpec(shape, lambda i: (0,) * len(shape), pipeline_mode=pl.Buffered(1))
    return pl.pallas_call(
        forward_kernel,
        grid=(N_UTT,),
        in_specs=[pl.BlockSpec(memory_space=pltpu.SMEM)] * 2 + [full(v.shape) for v in (enc, pred, w_enc, w_pred, w_out)],
        out_specs=[
            pl.BlockSpec(memory_space=pl.ANY),
            pl.BlockSpec(memory_space=pl.ANY),
            pl.BlockSpec((UG * 6, SUB, LANES), lambda i: (0, 0, 0)),
            pl.BlockSpec((UG * T_LOC, SUB, LANES), lambda i: (0, 0, 0)),
        ],
        out_shape=[
            jax.ShapeDtypeStruct((N_UTT, UG, ROWS, n_v), F32),
            jax.ShapeDtypeStruct((N_UTT, UG, ROWS, n_j), BF16),
            jax.ShapeDtypeStruct((UG * 6, SUB, LANES), F32),
            jax.ShapeDtypeStruct((UG * T_LOC, SUB, LANES), F32),
        ],
        scratch_shapes=[pltpu.VMEM((N_UTT * T_LOC, n_j), F32), pltpu.VMEM((N_UTT * N_UP, n_j), F32), pltpu.VMEM((ROWS, n_j), BF16), pltpu.VMEM((ROWS, n_v), F32),
            pltpu.VMEM((RING, UG, ROWS, n_v), F32), pltpu.VMEM((RING, UG, ROWS, n_j), BF16),
            pltpu.SemaphoreType.DMA((RING,)), pltpu.SemaphoreType.DMA((RING,))],
        compiler_params=pltpu.CompilerParams(vmem_limit_bytes=VMEM_FULL),
        name="joint_forward",
    )(labels, llen, enc, pred, w_enc, w_pred, w_out)


def lae2(x, y):
    return jnp.maximum(x, y) + jnp.log2(1.0 + jnp.exp2(-jnp.abs(x - y)))


def lattice_kernel(stat, norm, flen, llen, q0_out, q1_out, norm_out, loss_out, gath, s_blank, s_label, s_alpha, s_beta, send_sem, recv_sem):
    me = lax.axis_index("seq")
    mate = me + 1 - 2 * lax.rem(me, 2)
    across = lax.rem(me + 2, N_SEQ)
    barrier = pltpu.get_barrier_semaphore()
    for dev in (mate, across):
        pl.semaphore_signal(barrier, inc=1, device_id={"seq": dev}, device_id_type=MESH)
    pl.semaphore_wait(barrier, 2)
    copies = [pltpu.make_async_remote_copy(src_ref=src, dst_ref=gath.at[k], send_sem=send_sem.at[k], recv_sem=recv_sem.at[k],
                                           device_id={"seq": dev}, device_id_type=MESH)
              for k, (src, dev) in enumerate(((stat, across), (stat, mate), (gath.at[0], mate)))]
    copies[0].start()
    copies[1].start()

    sub = lax.broadcasted_iota(jnp.int32, (SUB, LANES), 0)
    sub24 = lax.broadcasted_iota(jnp.int32, (N_UP, LANES), 0)
    lane = lax.broadcasted_iota(jnp.int32, (SUB, LANES), 1)
    tb = jnp.zeros((SUB, LANES), jnp.int32)
    ub = jnp.zeros((SUB, LANES), jnp.int32)
    for b in range(N_UTT):
        at_b = lax.rem(lane, N_UTT) == b
        tb = jnp.where(at_b, flen[b], tb)
        ub = jnp.where(at_b, llen[b], ub)
    n_pad = s_blank.shape[0]

    def fill(i, c):
        s_blank[pl.ds(pl.multiple_of(i * SUB, SUB), SUB), :] = jnp.full((SUB, LANES), NEG, F32)
        s_label[pl.ds(pl.multiple_of(i * SUB, SUB), SUB), :] = jnp.full((SUB, LANES), NEG, F32)
        return c

    lax.fori_loop(0, n_pad // SUB, fill, 0, unroll=SUB)
    end_grp = [jnp.where(sub + SUB * ug == ub, 0.0, NEG) for ug in range(UG)]
    for t in range(T_ALL, T_ALL + N_UP):
        for ug in range(UG):
            s_blank[pl.ds(t * N_UP + 200 * ug, SUB, stride=25), :] = end_grp[ug]

    def place(src, src_seq):
        for t4 in range(T_LOC // 4):
            for ug in range(UG):
                val = src[ug * 6 + t4]
                in_u = sub + SUB * ug <= ub
                in_l = sub + SUB * ug < ub
                for k in range(4):
                    t = src_seq * T_LOC + t4 * 4 + k
                    bl = val if k == 0 else pltpu.roll(val, LANES - 32 * k, 1)
                    la = pltpu.roll(val, 112 - 32 * k, 1)
                    ok = t < tb
                    s_blank[pl.ds(t * N_UP + 200 * ug, SUB, stride=25), :] = jnp.where(ok, jnp.where(in_u, bl, NEG), end_grp[ug])
                    s_label[pl.ds(t * N_UP + 200 * ug, SUB, stride=25), :] = jnp.where(ok & in_l, la, NEG)

    place(stat, me)
    copies[1].wait_recv()
    place(gath.at[1], mate)
    copies[0].wait_recv()
    copies[2].start()
    place(gath.at[0], across)
    copies[2].wait_recv()
    place(gath.at[2], lax.rem(mate + 2, N_SEQ))

    alpha0 = jnp.where(sub24 == 0, 0.0, NEG)
    s_alpha[pl.ds(0, N_UP), :] = alpha0
    beta_end = jnp.where(sub24 == jnp.concatenate([ub] * UG, axis=0), 0.0, NEG)
    s_beta[pl.ds(N_DIAG * N_UP, N_UP), :] = beta_end
    s_beta[pl.ds((N_DIAG + 1) * N_UP, SUB), :] = jnp.full((SUB, LANES), NEG, F32)

    def wave(i, carry):
        alpha, beta = carry
        row = pl.multiple_of(i * N_UP, SUB)
        x = alpha + s_blank[pl.ds(row, N_UP), :]
        y = alpha + s_label[pl.ds(row, N_UP), :]
        y = jnp.where(sub24 == 0, NEG, pltpu.roll(y, 1, 0))
        alpha = lae2(x, y)
        s_alpha[pl.ds(pl.multiple_of(row + N_UP, SUB), N_UP), :] = alpha
        brow = pl.multiple_of((N_DIAG - 1 - i) * N_UP, SUB)
        bx = beta + s_blank[pl.ds(brow, N_UP), :]
        by = pltpu.roll(beta, N_UP - 1, 0) + s_label[pl.ds(brow, N_UP), :]
        beta = lae2(bx, by)
        s_beta[pl.ds(brow, N_UP), :] = beta
        return alpha, beta

    _, beta = lax.fori_loop(0, N_DIAG, wave, (alpha0, beta_end), unroll=7)
    log_p = beta[0:1, :]
    loss_out[...] = jnp.broadcast_to(-LN2 * log_p, (SUB, LANES))
    for t in range(T_LOC):
        tg = me * T_LOC + t
        for ug in range(UG):
            base = tg * N_UP + 200 * ug
            grp = lambda ref, off: ref[pl.ds(base + off, SUB, stride=25), :]
            al = grp(s_alpha, 0) - log_p
            ok = (tg < tb) & (sub + SUB * ug <= ub)
            q0 = jnp.where(ok, jnp.exp2(al + grp(s_blank, 0) + grp(s_beta, 24)), 0.0)
            q1 = jnp.where(ok, jnp.exp2(al + grp(s_label, 0) + grp(s_beta, 25)), 0.0)
            idx = ug * T_LOC + t
            q0_out[idx] = q0
            q1_out[idx] = q1
            norm_out[idx] = norm[idx] - jnp.log2(q0 + q1)
    for cp in copies:
        cp.wait_send()


def lattice(stat, norm, flen, llen):
    vm = pl.BlockSpec(memory_space=pltpu.VMEM)
    n_rows = (T_ALL + 2 * N_UP) * N_UP
    return pl.pallas_call(
        lattice_kernel,
        in_specs=[vm] * 2 + [pl.BlockSpec(memory_space=pltpu.SMEM)] * 2,
        out_specs=[vm] * 4,
        out_shape=[jax.ShapeDtypeStruct((UG * T_LOC, SUB, LANES), F32)] * 3 + [jax.ShapeDtypeStruct((SUB, LANES), F32)],
        scratch_shapes=[pltpu.VMEM((N_SEQ - 1,) + stat.shape, F32)] + [pltpu.VMEM((n_rows, LANES), F32)] * 4
        + [pltpu.SemaphoreType.DMA((N_SEQ - 1,)), pltpu.SemaphoreType.DMA((N_SEQ - 1,))],
        compiler_params=pltpu.CompilerParams(collective_id=0, has_side_effects=True),
        name="lattice",
    )(stat, norm, flen, llen)


class Links:
    def __init__(self, send_sem, recv_sem):
        self.send_sem, self.recv_sem, self.copies = send_sem, recv_sem, []
        seq = lax.axis_index("seq")
        self.core = lax.rem(seq, 2)
        self.x = lax.div(seq, 2)
        self.y = lax.axis_index("data")
        self.dev = {
            "core": {"seq": seq + 1 - 2 * self.core},
            "x": {"seq": lax.rem(seq + 2, N_SEQ)},
            "y": {"data": 1 - self.y},
        }

    def greet(self):
        barrier = pltpu.get_barrier_semaphore()
        for dev in self.dev.values():
            pl.semaphore_signal(barrier, inc=1, device_id=dev, device_id_type=MESH)
        pl.semaphore_wait(barrier, 3)

    def copy(self, ends, axis):
        i = len(self.copies)

        def make():
            src, dst = ends()
            return pltpu.make_async_remote_copy(src_ref=src, dst_ref=dst, send_sem=self.send_sem.at[i], recv_sem=self.recv_sem.at[i],
                                                device_id=self.dev[axis], device_id_type=MESH)

        self.copies.append(make)
        return make


def rows_at(start, size):
    return pl.ds(pl.multiple_of(start, 16), size)


def sum_stages(links, acc, gat, stg, rcv, col0, n_col):
    half = acc.shape[0] // 2
    h0 = links.core * half
    every = pl.ds(col0, n_col)
    box = []
    for q in range(2):
        first, second = ("x", "y") if q == 0 else ("y", "x")
        k1, k2 = (links.x, links.y) if q == 0 else (links.y, links.x)
        box.append((q, first, second, k1, k2, pl.ds(col0 + q * (n_col // 2), n_col // 2)))
    n2, n4 = half // 2, half // 4

    def same(rows, cols):
        def ends():
            ref = gat.at[rows(), cols]
            return ref, ref
        return ends

    swap = links.copy(lambda: (stg[0], rcv[0]), "core")
    back = links.copy(same(lambda: rows_at(h0, half), every), "core")
    hops = [(
        links.copy(lambda q=q: (stg[1].at[q], rcv[1].at[q]), first),
        links.copy(lambda q=q: (stg[2].at[q], rcv[2].at[q]), second),
        links.copy(same(lambda k1=k1, k2=k2: rows_at(h0 + k1 * n2 + k2 * n4, n4), cols), second),
        links.copy(same(lambda k1=k1: rows_at(h0 + k1 * n2, n2), cols), first),
    ) for q, first, second, k1, k2, cols in box]

    def s1():
        stg[0][...] = acc[rows_at((1 - links.core) * half, half), every].astype(BF16)
        swap().start()

    def s2():
        swap().wait_recv()
        own = rows_at(h0, half)
        acc[own, every] = acc[own, every] + rcv[0][...].astype(F32)
        for q, first, second, k1, k2, cols in box:
            stg[1][q] = acc[rows_at(h0 + (1 - k1) * n2, n2), cols].astype(BF16)
            hops[q][0]().start()

    def s3():
        for q, first, second, k1, k2, cols in box:
            hops[q][0]().wait_recv()
            part = rows_at((1 - k2) * n4, n4)
            stg[2][q] = (acc[rows_at(h0 + k1 * n2 + (1 - k2) * n4, n4), cols] + rcv[1][q, part].astype(F32)).astype(BF16)
            hops[q][1]().start()

    def s4():
        for q, first, second, k1, k2, cols in box:
            hops[q][1]().wait_recv()
            part = rows_at(k2 * n4, n4)
            own = rows_at(h0 + k1 * n2 + k2 * n4, n4)
            gat[own, cols] = (acc[own, cols] + rcv[1][q, part].astype(F32) + rcv[2][q].astype(F32)).astype(BF16)
            hops[q][2]().start()

    def s5():
        for hop in hops:
            hop[2]().wait_recv()
            hop[3]().start()

    def s6():
        for hop in hops:
            hop[3]().wait_recv()
        back().start()

    def s7():
        back().wait_recv()

    return [s1, s2, s3, s4, s5, s6, s7]


def dc_stages(links, src, gat, stg, rcv):
    n_row = src.shape[0]
    half, quar, eigh = n_row // 2, n_row // 4, n_row // SUB
    h0 = links.core * half
    r0 = h0 + links.x * quar
    r_far = h0 + (1 - links.x) * quar
    y_own, y_far = links.y * n_row, (1 - links.y) * n_row

    def hop(start, size, axis):
        def ends():
            ref = gat.at[rows_at(start(), size), :]
            return ref, ref
        return links.copy(ends, axis)

    swap = links.copy(lambda: (stg[0], rcv[0]), "core")
    cross = links.copy(lambda: (stg[1], rcv[1]), "x")
    up_y = hop(lambda: y_own + r0, eigh, "y")
    down_x = hop(lambda: y_own + r0 + eigh, eigh, "x")
    up_x = hop(lambda: y_own + r0, eigh, "x")
    down_y = hop(lambda: y_own + r0 + eigh, eigh, "y")
    up_far = hop(lambda: y_far + r0, eigh, "x")
    down_far = hop(lambda: y_own + r_far + eigh, eigh, "y")
    back = [hop(lambda: y_own + h0, half, "core"), hop(lambda: y_far + h0, half, "core")]

    def s1():
        stg[0][...] = src[rows_at((1 - links.core) * half, half), :].astype(BF16)
        swap().start()

    def s2():
        swap().wait_recv()
        part = rows_at((1 - links.x) * quar, quar)
        stg[1][...] = (src[rows_at(r_far, quar), :] + rcv[0][part, :].astype(F32)).astype(BF16)
        cross().start()

    def s3():
        cross().wait_recv()
        part = rows_at(links.x * quar, quar)
        total = src[rows_at(r0, quar), :] + rcv[0][part, :].astype(F32) + rcv[1][...].astype(F32)
        gat[rows_at(y_own + r0, quar), :] = total.astype(BF16)
        for cp in (up_y, down_x, up_x, down_y):
            cp().start()

    def s4():
        up_y().wait_recv()
        up_far().start()
        down_x().wait_recv()
        down_far().start()

    def s5():
        for cp in (up_x, down_y, up_far, down_far):
            cp().wait_recv()
        for cp in back:
            cp().start()

    def s6():
        for cp in back:
            cp().wait_recv()

    return [s1, s2, s3, s4, s5, s6]


N_COPY = 10 * 5 + 1


def sum_scratch(n_row, n_col):
    half = n_row // 2
    return [pltpu.VMEM((half, n_col), BF16), pltpu.VMEM((2, half // 2, n_col // 2), BF16), pltpu.VMEM((2, half // 4, n_col // 2), BF16)]


W_CHUNK = 256


def backward_kernel(labels, pred, z_hbm, h_hbm, q0_ref, q1_ref, norm_ref, w_out, enc, da_out, g_enc_out, g_out_out, g_dc_out, far_out,
                    dz_all, h_all, da_all, da_part, dz0, dz1, dz2, dh0, dh1, dh2, w_out_t, z_ring, dw_enc, dw_out, dc_out, g_enc, g_out, g_dc,
                    es0, es1, es2, er0, er1, er2, ps0, ps1, ps2, pr0, pr1, pr2, qs0, qs1, qs2, qr0, qr1, qr2, rs0, rs1, rs2, rr0, rr1, rr2, ds0, ds1, dr0, dr1,
                    h_sem, z_sem, o_sem, send_sem, recv_sem):
    step = pl.program_id(0)
    lane = lax.broadcasted_iota(jnp.int32, (SUB, LANES), 1)
    sub = lax.broadcasted_iota(jnp.int32, (SUB, LANES), 0)
    n_j, n_v = w_out.shape
    utt_rows = UG * ROWS

    dzs, dhs = (dz0, dz1, dz2), (dh0, dh1, dh2)
    prev = jnp.maximum(step - 1, 0)
    z_slot = lax.rem(step, RING)

    def multiply(ug):
        dhs[ug][...] = dot(dzs[ug][...], w_out_t[...])[:, :n_j]

    def h_copy(utt):
        rows = pl.ds(pl.multiple_of(utt * utt_rows, 16), utt_rows)
        return pltpu.make_async_copy(h_hbm.at[rows, :], h_all.at[rows, :], h_sem.at[utt])

    def z_copy(utt):
        slot = lax.rem(utt, RING)
        return pltpu.make_async_copy(z_hbm.at[utt], z_ring.at[slot], z_sem.at[slot])

    links = Links(send_sem, recv_sem)
    far = links.copy(lambda: (pred, far_out), "y")
    e_st = sum_stages(links, dw_enc, g_enc, (es0, es1, es2), (er0, er1, er2), 0, n_v)
    p_st = sum_stages(links, dw_out, g_out, (ps0, ps1, ps2), (pr0, pr1, pr2), 0, n_v // 2)
    q_st = sum_stages(links, dw_out, g_out, (qs0, qs1, qs2), (qr0, qr1, qr2), n_v // 2, n_v // 4)
    r_st = sum_stages(links, dw_out, g_out, (rs0, rs1, rs2), (rr0, rr1, rr2), n_v // 2 + n_v // 4, n_v // 4)
    c_st = dc_stages(links, dc_out, g_dc, (ds0, ds1), (dr0, dr1))

    @pl.when(step == 0)
    def _():
        for utt in range(RING - 1):
            z_copy(utt).start()
            h_copy(utt).start()
        links.greet()
        far().start()
        w_out_t[:, :n_j] = w_out[...].T
        w_out_t[:, n_j:] = jnp.zeros((n_v, w_out_t.shape[1] - n_j), BF16)

    def logit_grads(ug):
        shift = LANES - step
        lab_grp = label_column(labels, step, ug, sub)
        masks = [lab_grp - LANES * k == lane for k in range(n_v // LANES)]
        for t in range(0, T_LOC, 2):
            pair = []
            for idx in (ug * T_LOC + t, ug * T_LOC + t + 1):
                q0, q1, norm = [jnp.broadcast_to(pltpu.roll(ref[idx], shift, 1)[:, 0:1], (SUB, LANES)) for ref in (q0_ref, q1_ref, norm_ref)]
                row = (idx - ug * T_LOC) * SUB
                tiles = []
                for k in range(n_v // LANES):
                    z = z_ring[z_slot, ug, row:row + SUB, k * LANES:k * LANES + LANES]
                    g = jnp.exp2(z - norm) - jnp.where(masks[k], q1, 0.0)
                    tiles.append(g - jnp.where(lane == 0, q0, 0.0) if k == 0 else g)
                pair.append(jnp.concatenate(tiles, axis=1))
            rows = pl.ds(pl.multiple_of(step * utt_rows + ug * ROWS + t * SUB, 16), 16)
            dz = jnp.concatenate(pair, axis=0).astype(BF16)
            dz_all[rows, :] = dz
            dzs[ug][t * SUB:t * SUB + 16, :] = dz

    def hidden_grads(utt, ug):
        dc = None
        for t in range(0, T_LOC, 2):
            hid = h_all[pl.ds(pl.multiple_of(utt * utt_rows + ug * ROWS + t * SUB, 16), 16), :].astype(F32)
            ds = dhs[ug][t * SUB:t * SUB + 16, :] * (1.0 - hid * hid)
            both = ds[:SUB] + ds[SUB:]
            dc = both if dc is None else dc + both
            here = slice(t * SUB, t * SUB + 2 * SUB)
            for c in range(n_j // LANES):
                tile = ds[:, c * LANES:c * LANES + LANES]
                da_part[c, here, :] = tile + da_part[c, here, :] if ug else tile
        if ug == UG - 1:
            sums = [functools.reduce(jnp.add, [da_part[c, pl.ds(k, T_LOC, stride=SUB), :] for k in range(SUB)]) for c in range(n_j // LANES)]
            da_all[pl.ds(pl.multiple_of(utt * T_LOC, SUB), T_LOC), :] = jnp.concatenate(sums, axis=1)
        dc_out[pl.ds(pl.multiple_of(utt * N_UP + ug * SUB, SUB), SUB), :] = dc

    @pl.when(step + RING - 1 < N_UTT)
    def _():
        z_copy(step + RING - 1).start()
        h_copy(step + RING - 1).start()

    @pl.when(step < N_UTT)
    def _():
        h_copy(step).wait()
        z_copy(step).wait()
        multiply(2)
        logit_grads(0)
        hidden_grads(prev, 1)
        multiply(0)
        logit_grads(1)
        hidden_grads(prev, 2)
        multiply(1)
        logit_grads(2)
        hidden_grads(step, 0)

    @pl.when(step == N_UTT)
    def _():
        multiply(2)
        hidden_grads(prev, 1)
        hidden_grads(prev, 2)
        da = da_all[...].astype(BF16)
        da_out[...] = da
        dw_enc[...] = dot(da, enc[...], ((0,), (0,)))
        e_st[0]()
        c_st[0]()

    plan = [
        ((c_st[1], e_st[1]), ()),
        ((), (c_st[2], p_st[0])),
        ((e_st[2], p_st[1]), ()),
        ((e_st[3], q_st[0]), (
            r_st[0], p_st[2], q_st[1], r_st[1], c_st[3], p_st[3], r_st[2], q_st[2], e_st[4], c_st[4], q_st[3], r_st[3], p_st[4],
            q_st[4], r_st[4], p_st[5], e_st[5], q_st[5])),
    ]
    for part, (lo, hi) in enumerate(((0, 3 * LANES), (3 * LANES, n_j))):
        @pl.when(step > N_UTT)
        def _(lo=lo, hi=hi):
            cols = pl.ds(pl.multiple_of((step - N_UTT - 1) * W_CHUNK, W_CHUNK), W_CHUNK)
            dw_out[lo:hi, cols] = dot(h_all[:, lo:hi], dz_all[:, cols], ((0,), (0,)))

        for n, stages in enumerate(plan):
            if stages[part]:
                @pl.when(step == N_UTT + 1 + n)
                def _(stages=stages[part]):
                    for stage in stages:
                        stage()

    @pl.when(step == N_UTT + len(plan))
    def _():
        p_st[6]()
        r_st[5]()
        r_st[6]()
        e_st[6]()
        out_enc = pltpu.make_async_copy(g_enc, g_enc_out, o_sem.at[1])
        out_enc.start()
        q_st[6]()
        out_out = pltpu.make_async_copy(g_out, g_out_out, o_sem.at[2])
        out_out.start()
        c_st[5]()
        out_dc = pltpu.make_async_copy(g_dc, g_dc_out, o_sem.at[0])
        out_dc.start()
        far().wait_recv()
        for cp in links.copies:
            cp().wait_send()
        out_dc.wait()
        out_enc.wait()
        out_out.wait()


def joint_backward(labels, pred, z, h, q0, q1, norm, w_out, enc):
    n_j, n_v = w_out.shape
    n_cell = N_UTT * UG * ROWS
    n_dc = N_UTT * N_UP
    full = lambda shape: pl.BlockSpec(shape, lambda i: (0,) * len(shape), pipeline_mode=pl.Buffered(1))
    return pl.pallas_call(
        backward_kernel,
        grid=(N_UTT + 1 + n_v // W_CHUNK,),
        in_specs=[
            pl.BlockSpec(memory_space=pltpu.SMEM),
            *[pl.BlockSpec(memory_space=pl.ANY)] * 3,
            full(q0.shape), full(q1.shape), full(norm.shape), full(w_out.shape), full(enc.shape),
        ],
        out_specs=[full((N_UTT * T_LOC, n_j))] + [pl.BlockSpec(memory_space=pl.ANY)] * 4,
        out_shape=[
            jax.ShapeDtypeStruct((N_UTT * T_LOC, n_j), BF16),
            jax.ShapeDtypeStruct((n_j, n_v), BF16),
            jax.ShapeDtypeStruct((n_j, n_v), BF16),
            jax.ShapeDtypeStruct((2 * n_dc, n_j), BF16),
            jax.ShapeDtypeStruct(pred.shape, BF16),
        ],
        scratch_shapes=[
            pltpu.VMEM((n_cell, n_v), BF16), pltpu.VMEM((n_cell, n_j), BF16), pltpu.VMEM((N_UTT * T_LOC, n_j), F32),
            pltpu.VMEM((n_j // LANES, ROWS, LANES), F32),
            *[pltpu.VMEM((ROWS, n_v), BF16)] * 3, *[pltpu.VMEM((ROWS, n_j), F32)] * 3,
            pltpu.VMEM((n_v, n_j + (-n_j) % 256), BF16), pltpu.VMEM((RING, UG, ROWS, n_v), F32),
            pltpu.VMEM((n_j, n_v), F32), pltpu.VMEM((n_j, n_v), F32), pltpu.VMEM((n_dc, n_j), F32),
            pltpu.VMEM((n_j, n_v), BF16), pltpu.VMEM((n_j, n_v), BF16), pltpu.VMEM((2 * n_dc, n_j), BF16),
            *sum_scratch(n_j, n_v) * 2, *sum_scratch(n_j, n_v // 2) * 2, *sum_scratch(n_j, n_v // 4) * 4,
            *[pltpu.VMEM((n_dc // 2, n_j), BF16), pltpu.VMEM((n_dc // 4, n_j), BF16)] * 2,
            pltpu.SemaphoreType.DMA((N_UTT,)), pltpu.SemaphoreType.DMA((RING,)), pltpu.SemaphoreType.DMA((3,)),
            pltpu.SemaphoreType.DMA((N_COPY,)), pltpu.SemaphoreType.DMA((N_COPY,)),
        ],
        compiler_params=pltpu.CompilerParams(collective_id=1, has_side_effects=True, vmem_limit_bytes=VMEM_FULL),
        name="joint_backward",
    )(labels, pred, z, h.reshape(n_cell, n_j), q0, q1, norm, w_out, enc)


def finish_kernel(loss, *refs):
    ins, o_loss, outs = refs[:FIN_IN], refs[FIN_IN], refs[FIN_IN + 1:FIN_IN + 1 + FIN_OUT]
    bufs, vals, in_sem, out_sem = refs[FIN_IN + 1 + FIN_OUT:-FIN_OUT - 2], refs[-FIN_OUT - 2:-2], refs[-2], refs[-1]
    g_dc, pred, pred_far, g_out, g_enc, w_pred, da, w_enc = bufs
    v_wpred, v_wout, v_wenc, v_pred, v_enc = vals
    loads = [pltpu.make_async_copy(src, dst, in_sem.at[k]) for k, (src, dst) in enumerate(zip(ins, bufs))]
    stores = [pltpu.make_async_copy(src, dst, out_sem.at[k]) for k, (src, dst) in enumerate(zip(vals, outs))]
    for cp in loads:
        cp.start()
    y = lax.axis_index("data")
    n_r = pred.shape[0]
    o_loss[...] = loss[0:1, :N_UTT]
    for k in range(3):
        loads[k].wait()
    dc_own = g_dc[rows_at(y * n_r, n_r), :]
    dc_far = g_dc[rows_at((1 - y) * n_r, n_r), :]
    v_wpred[...] = dot(pred[...], dc_own, ((0,), (0,))) + dot(pred_far[...], dc_far, ((0,), (0,)))
    stores[0].start()
    loads[3].wait()
    v_wout[...] = g_out[...].astype(F32)
    stores[1].start()
    loads[4].wait()
    v_wenc[...] = g_enc[...].astype(F32).T
    stores[2].start()
    loads[5].wait()
    v_pred[...] = dot(dc_own, w_pred[...], ((1,), (1,)))
    stores[3].start()
    loads[6].wait()
    loads[7].wait()
    v_enc[...] = dot(da[...], w_enc[...], ((1,), (1,))).astype(BF16)
    stores[4].start()
    for cp in stores:
        cp.wait()


FIN_IN = 8
FIN_OUT = 5


def finish(loss, g_enc, g_out, g_dc, pred, pred_far, w_pred, da, w_enc):
    vm = pl.BlockSpec(memory_space=pltpu.VMEM)
    hbm = pl.BlockSpec(memory_space=pl.ANY)
    ins = (g_dc, pred, pred_far, g_out, g_enc, w_pred, da, w_enc)
    outs = [(w_pred.shape, F32), (g_out.shape, F32), (w_enc.shape, F32), (pred.shape, F32), (pred.shape, BF16)]
    loss, grad_w_pred, grad_w_out, grad_w_enc, grad_pred, grad_enc = pl.pallas_call(
        finish_kernel,
        in_specs=[vm] + [hbm] * FIN_IN,
        out_specs=[vm] + [hbm] * FIN_OUT,
        out_shape=[jax.ShapeDtypeStruct((1, N_UTT), F32)] + [jax.ShapeDtypeStruct(*o) for o in outs],
        scratch_shapes=[pltpu.VMEM(v.shape, v.dtype) for v in ins] + [pltpu.VMEM(*o) for o in outs]
        + [pltpu.SemaphoreType.DMA((FIN_IN,)), pltpu.SemaphoreType.DMA((FIN_OUT,))],
        compiler_params=pltpu.CompilerParams(vmem_limit_bytes=VMEM_FULL),
        name="finish",
    )(loss, *ins)
    return loss, grad_enc, grad_pred, grad_w_enc, grad_w_pred, grad_w_out


def solution(mesh):
    utt_rows = P(("part", "data"))
    utt_mats = P(("part", "data"), None)
    utt_cube = P(("part", "data"), None, None)
    enc_spec = P(("part", "data"), "seq", None)
    weight_in = P(None, None)
    weight_out = P("part", None)

    def body(enc_loc, pred_loc, w_enc, w_pred, w_out, labels, frame_len, label_len):
        n_h = enc_loc.shape[2]
        enc2 = enc_loc.reshape(N_UTT * T_LOC, n_h)
        pred2 = pred_loc.reshape(N_UTT * N_UP, n_h)
        z, h, stat, norm = joint_forward(labels, label_len, enc2, pred2, w_enc, w_pred, w_out)
        q0, q1, norm, loss = lattice(stat, norm, frame_len, label_len)
        da, g_enc, g_out, g_dc, pred_far = joint_backward(labels, pred2, z, h, q0, q1, norm, w_out, enc2)
        loss, grad_enc, grad_pred, grad_w_enc, grad_w_pred, grad_w_out = finish(loss, g_enc, g_out, g_dc, pred2, pred_far, w_pred, da, w_enc)
        return loss.reshape(N_UTT), grad_enc.reshape(enc_loc.shape), grad_pred.reshape(pred_loc.shape), grad_w_enc, grad_w_pred, grad_w_out

    return jax.shard_map(body, mesh=mesh, in_specs=(enc_spec, utt_cube, weight_in, weight_in, weight_in, utt_mats, utt_rows, utt_rows), out_specs=(utt_rows, enc_spec, utt_cube, weight_out, weight_out, weight_out), check_vma=False)
```

```python
import functools

import jax
import jax.numpy as jnp
from jax import lax
from jax.experimental import pallas as pl
from jax.experimental.pallas import tpu as pltpu
from jax.sharding import PartitionSpec as P

NEG = -1e30
SUB = 8
LANES = 128
LOG2E = 1.4426950408889634
LN2 = 0.6931471805599453
F32 = jnp.float32
BF16 = jnp.bfloat16
MESH = pl.DeviceIdType.MESH
VMEM_FULL = 67_000_000
N_UTT = 16
T_LOC = 24
N_UP = 24
UG = 3
N_SEQ = 4
T_ALL = T_LOC * N_SEQ
RING = 4
B_RING = 3
N_DIAG = T_ALL + N_UP - 1
ROWS = SUB * T_LOC


def dot(lhs, rhs, dims=((1,), (0,))):
    return lax.dot_general(lhs, rhs, (dims, ((), ())), preferred_element_type=F32)


def label_column(labels, utt, ug, sub):
    col = jnp.zeros((SUB, LANES), jnp.int32)
    for k in range(SUB):
        col = jnp.where(sub == k, labels[utt, jnp.minimum(ug * SUB + k, N_UP - 2)], col)
    return col


def forward_kernel(labels, llen, enc, pred, w_enc, w_pred, w_out, z_hbm, h_hbm, stat_out, norm_out, act_e, act_p, h_next, z_last, z_ring, h_ring, z_sem, h_sem):
    step = pl.program_id(0)
    lane = lax.broadcasted_iota(jnp.int32, (SUB, LANES), 1)
    sub = lax.broadcasted_iota(jnp.int32, (SUB, LANES), 0)
    n_v = w_out.shape[1]

    @pl.when(step == 0)
    def _():
        act_e[...] = dot(enc[...], w_enc[...]).astype(BF16).astype(F32)
        act_p[...] = dot(pred[...], w_pred[...]).astype(BF16).astype(F32)
        stat_out[...] = jnp.zeros_like(stat_out)
        norm_out[...] = jnp.zeros_like(norm_out)

    def hidden(utt, ug, dst):
        row = pl.multiple_of(utt * N_UP, SUB)
        c_grp = act_p[pl.ds(row + SUB * ug, SUB), :]
        a_utt = act_e[pl.ds(row, T_LOC), :]
        for t in range(0, T_LOC, 2):
            pre = jnp.concatenate([a_utt[t:t + 1, :] + c_grp, a_utt[t + 1:t + 2, :] + c_grp], axis=0)
            dst[t * SUB:t * SUB + 16, :] = jnp.tanh(pre).astype(BF16)

    def soften(utt, ug, src):
        lab_grp = label_column(labels, jnp.maximum(utt, 0), ug, sub)
        masks = [lab_grp - LANES * k == lane for k in range(n_v // LANES)]
        for t4 in range(T_LOC // 4):
            cur = stat_out[ug * 6 + t4]
            for k in range(4):
                t = t4 * 4 + k
                z = [src[t * SUB:t * SUB + SUB, c * LANES:c * LANES + LANES] for c in range(n_v // LANES)]
                top = functools.reduce(jnp.maximum, z)
                tot = functools.reduce(jnp.add, [jnp.exp2(v - top) for v in z])
                picked = functools.reduce(jnp.add, [jnp.where(m, v, 0.0) for m, v in zip(masks, z)])
                row_top = jnp.max(top, axis=1, keepdims=True)
                row_tot = jnp.sum(tot * jnp.exp2(top - row_top), axis=1, keepdims=True)
                norm = row_top + jnp.log2(row_tot)
                blank = z[0][:, 0:1] - norm
                label = jnp.sum(picked, axis=1, keepdims=True) - norm
                cur = jnp.where(lane == utt + 32 * k, blank, cur)
                cur = jnp.where(lane == utt + 32 * k + 16, label, cur)
                norm_out[ug * T_LOC + t] = jnp.where(lane == utt, norm, norm_out[ug * T_LOC + t])
            stat_out[ug * 6 + t4] = cur

    def puts(utt):
        at = lax.rem(utt, RING)
        return (pltpu.make_async_copy(z_ring.at[at], z_hbm.at[utt], z_sem.at[at]),
                pltpu.make_async_copy(h_ring.at[at], h_hbm.at[utt], h_sem.at[at]))

    @pl.when(step == 0)
    def _():
        hidden(0, 0, h_next)

    @pl.when(step >= RING)
    def _():
        for cp in puts(step - RING):
            cp.wait()

    slot = lax.rem(step, RING)
    z_out, h_out = z_ring.at[slot], h_ring.at[slot]
    groups = lax.div(llen[step], SUB) + 1
    last_of = lambda utt: lax.div(llen[utt], SUB)

    def utterance(n_grp):
        h_out[0] = h_next[...]
        for ug in range(n_grp):
            z = dot(h_out[ug] if ug else h_next[...], w_out[...]) * LOG2E
            z_out[ug] = z
            if ug == 0:
                soften(step - 1, last_of(jnp.maximum(step - 1, 0)), z_last)
            else:
                soften(step, ug - 1, z_out.at[ug - 1])
            if ug < n_grp - 1:
                hidden(step, ug + 1, h_out.at[ug + 1])
            else:
                z_last[...] = z
                hidden(jnp.minimum(step + 1, N_UTT - 1), 0, h_next)

        if n_grp < UG:
            @pl.when(step < RING)
            def _():
                for ug in range(n_grp, UG):
                    z_out[ug] = jnp.zeros(z_out.shape[1:], F32)
                    h_out[ug] = jnp.zeros(h_out.shape[1:], BF16)

    for n_grp in range(1, UG + 1):
        pl.when(groups == n_grp)(functools.partial(utterance, n_grp))
    for cp in puts(step):
        cp.start()

    @pl.when(step == N_UTT - 1)
    def _():
        soften(step, last_of(step), z_last)
        for back in range(RING - 1, -1, -1):
            for cp in puts(step - back):
                cp.wait()


def joint_forward(labels, llen, enc, pred, w_enc, w_pred, w_out):
    n_j, n_v = w_out.shape
    full = lambda shape: pl.BlockSpec(shape, lambda i: (0,) * len(shape), pipeline_mode=pl.Buffered(1))
    return pl.pallas_call(
        forward_kernel,
        grid=(N_UTT,),
        in_specs=[pl.BlockSpec(memory_space=pltpu.SMEM)] * 2 + [full(v.shape) for v in (enc, pred, w_enc, w_pred, w_out)],
        out_specs=[
            pl.BlockSpec(memory_space=pl.ANY),
            pl.BlockSpec(memory_space=pl.ANY),
            pl.BlockSpec((UG * 6, SUB, LANES), lambda i: (0, 0, 0)),
            pl.BlockSpec((UG * T_LOC, SUB, LANES), lambda i: (0, 0, 0)),
        ],
        out_shape=[
            jax.ShapeDtypeStruct((N_UTT, UG, ROWS, n_v), F32),
            jax.ShapeDtypeStruct((N_UTT, UG, ROWS, n_j), BF16),
            jax.ShapeDtypeStruct((UG * 6, SUB, LANES), F32),
            jax.ShapeDtypeStruct((UG * T_LOC, SUB, LANES), F32),
        ],
        scratch_shapes=[pltpu.VMEM((N_UTT * T_LOC, n_j), F32), pltpu.VMEM((N_UTT * N_UP, n_j), F32), pltpu.VMEM((ROWS, n_j), BF16), pltpu.VMEM((ROWS, n_v), F32),
            pltpu.VMEM((RING, UG, ROWS, n_v), F32), pltpu.VMEM((RING, UG, ROWS, n_j), BF16),
            pltpu.SemaphoreType.DMA((RING,)), pltpu.SemaphoreType.DMA((RING,))],
        compiler_params=pltpu.CompilerParams(vmem_limit_bytes=VMEM_FULL),
        name="joint_forward",
    )(labels, llen, enc, pred, w_enc, w_pred, w_out)


def lae2(x, y):
    return jnp.maximum(x, y) + jnp.log2(1.0 + jnp.exp2(-jnp.abs(x - y)))


def run_lattice(links, moves, stat, norm, flen, llen, q0_out, q1_out, norm_out, loss_out, gath, s_blank, s_label, s_alpha, s_beta):
    me = links.seq
    mate = me + 1 - 2 * links.core
    across = lax.rem(me + 2, N_SEQ)
    row_x, row_core, row_relay = moves
    sub = lax.broadcasted_iota(jnp.int32, (SUB, LANES), 0)
    sub24 = lax.broadcasted_iota(jnp.int32, (N_UP, LANES), 0)
    lane = lax.broadcasted_iota(jnp.int32, (SUB, LANES), 1)
    tb = jnp.zeros((SUB, LANES), jnp.int32)
    ub = jnp.zeros((SUB, LANES), jnp.int32)
    for b in range(N_UTT):
        at_b = lax.rem(lane, N_UTT) == b
        tb = jnp.where(at_b, flen[b], tb)
        ub = jnp.where(at_b, llen[b], ub)
    n_pad = s_blank.shape[0]

    def fill(i, c):
        s_blank[pl.ds(pl.multiple_of(i * SUB, SUB), SUB), :] = jnp.full((SUB, LANES), NEG, F32)
        s_label[pl.ds(pl.multiple_of(i * SUB, SUB), SUB), :] = jnp.full((SUB, LANES), NEG, F32)
        return c

    lax.fori_loop(0, n_pad // SUB, fill, 0, unroll=11)
    end_grp = [jnp.where(sub + SUB * ug == ub, 0.0, NEG) for ug in range(UG)]
    for d in range(T_ALL, N_DIAG + 2):
        for ug in range(UG):
            s_blank[d * N_UP + SUB * ug:d * N_UP + SUB * ug + SUB, :] = end_grp[ug]

    def place(src, src_seq):
        for t4 in range(T_LOC // 4):
            for ug in range(UG):
                val = src[ug * 6 + t4]
                in_u = sub + SUB * ug <= ub
                in_l = sub + SUB * ug < ub
                for k in range(4):
                    t = src_seq * T_LOC + t4 * 4 + k
                    bl = val if k == 0 else pltpu.roll(val, LANES - 32 * k, 1)
                    la = pltpu.roll(val, 112 - 32 * k, 1)
                    ok = t < tb
                    s_blank[pl.ds(t * N_UP + 200 * ug, SUB, stride=25), :] = jnp.where(ok, jnp.where(in_u, bl, NEG), end_grp[ug])
                    s_label[pl.ds(t * N_UP + 200 * ug, SUB, stride=25), :] = jnp.where(ok & in_l, la, NEG)

    place(stat, me)
    row_core().wait_recv()
    place(gath.at[1], mate)
    row_x().wait_recv()
    row_relay().start()
    place(gath.at[0], across)
    row_relay().wait_recv()
    place(gath.at[2], lax.rem(mate + 2, N_SEQ))

    alpha0 = jnp.where(sub24 == 0, 0.0, NEG)
    s_alpha[pl.ds(0, N_UP), :] = alpha0
    beta_end = jnp.where(sub24 == jnp.concatenate([ub] * UG, axis=0), 0.0, NEG)
    s_beta[pl.ds(N_DIAG * N_UP, N_UP), :] = beta_end
    s_beta[pl.ds((N_DIAG + 1) * N_UP, SUB), :] = jnp.full((SUB, LANES), NEG, F32)

    def wave(i, carry):
        alpha, beta = carry
        row = pl.multiple_of(i * N_UP, SUB)
        x = alpha + s_blank[pl.ds(row, N_UP), :]
        y = alpha + s_label[pl.ds(row, N_UP), :]
        y = jnp.where(sub24 == 0, NEG, pltpu.roll(y, 1, 0))
        alpha = lae2(x, y)
        s_alpha[pl.ds(pl.multiple_of(row + N_UP, SUB), N_UP), :] = alpha
        brow = pl.multiple_of((N_DIAG - 1 - i) * N_UP, SUB)
        bx = beta + s_blank[pl.ds(brow, N_UP), :]
        by = pltpu.roll(beta, N_UP - 1, 0) + s_label[pl.ds(brow, N_UP), :]
        beta = lae2(bx, by)
        s_beta[pl.ds(brow, N_UP), :] = beta
        return alpha, beta

    _, beta = lax.fori_loop(0, N_DIAG, wave, (alpha0, beta_end), unroll=7)
    log_p = beta[0:1, :]
    loss_out[...] = jnp.broadcast_to(-LN2 * log_p, (SUB, LANES))
    for t in range(T_LOC):
        tg = me * T_LOC + t
        for ug in range(UG):
            base = tg * N_UP + 200 * ug
            grp = lambda ref, off: ref[pl.ds(base + off, SUB, stride=25), :]
            al = grp(s_alpha, 0) - log_p
            ok = (tg < tb) & (sub + SUB * ug <= ub)
            q0 = jnp.where(ok, jnp.exp2(al + grp(s_blank, 0) + grp(s_beta, 24)), 0.0)
            q1 = jnp.where(ok, jnp.exp2(al + grp(s_label, 0) + grp(s_beta, 25)), 0.0)
            idx = ug * T_LOC + t
            q0_out[idx] = q0
            q1_out[idx] = q1
            norm_out[idx] = norm[idx] - jnp.log2(q0 + q1)


class Links:
    def __init__(self, send_sem, recv_sem):
        self.send_sem, self.recv_sem, self.copies = send_sem, recv_sem, []
        seq = lax.axis_index("seq")
        self.core = lax.rem(seq, 2)
        self.x = lax.div(seq, 2)
        self.y = lax.axis_index("data")
        self.seq = seq
        self.dev = {
            "core": {"seq": seq + 1 - 2 * self.core},
            "x": {"seq": lax.rem(seq + 2, N_SEQ)},
            "y": {"data": 1 - self.y},
        }

    def greet(self):
        barrier = pltpu.get_barrier_semaphore()
        for dev in self.dev.values():
            pl.semaphore_signal(barrier, inc=1, device_id=dev, device_id_type=MESH)
        pl.semaphore_wait(barrier, 3)

    def copy(self, ends, axis):
        i = len(self.copies)

        def make():
            src, dst = ends()
            return pltpu.make_async_remote_copy(src_ref=src, dst_ref=dst, send_sem=self.send_sem.at[i], recv_sem=self.recv_sem.at[i],
                                                device_id=self.dev[axis], device_id_type=MESH)

        self.copies.append(make)
        return make


def rows_at(start, size):
    return pl.ds(pl.multiple_of(start, 16), size)


def sum_stages(links, acc, gat, stg, rcv, col0, n_col):
    half = acc.shape[0] // 2
    h0 = links.core * half
    every = pl.ds(col0, n_col)
    box = []
    for q in range(2):
        first, second = ("x", "y") if q == 0 else ("y", "x")
        k1, k2 = (links.x, links.y) if q == 0 else (links.y, links.x)
        box.append((q, first, second, k1, k2, pl.ds(col0 + q * (n_col // 2), n_col // 2)))
    n2, n4 = half // 2, half // 4

    def same(rows, cols):
        def ends():
            ref = gat.at[rows(), cols]
            return ref, ref
        return ends

    swap = links.copy(lambda: (stg[0], rcv[0]), "core")
    back = links.copy(same(lambda: rows_at(h0, half), every), "core")
    hops = [(
        links.copy(lambda q=q: (stg[1].at[q], rcv[1].at[q]), first),
        links.copy(lambda q=q: (stg[2].at[q], rcv[2].at[q]), second),
        links.copy(same(lambda k1=k1, k2=k2: rows_at(h0 + k1 * n2 + k2 * n4, n4), cols), second),
        links.copy(same(lambda k1=k1: rows_at(h0 + k1 * n2, n2), cols), first),
    ) for q, first, second, k1, k2, cols in box]

    def s1():
        stg[0][...] = acc[rows_at((1 - links.core) * half, half), every].astype(BF16)
        swap().start()

    def s2():
        swap().wait_recv()
        own = rows_at(h0, half)
        acc[own, every] = acc[own, every] + rcv[0][...].astype(F32)
        for q, first, second, k1, k2, cols in box:
            stg[1][q] = acc[rows_at(h0 + (1 - k1) * n2, n2), cols].astype(BF16)
            hops[q][0]().start()

    def s3():
        for q, first, second, k1, k2, cols in box:
            hops[q][0]().wait_recv()
            part = rows_at((1 - k2) * n4, n4)
            stg[2][q] = (acc[rows_at(h0 + k1 * n2 + (1 - k2) * n4, n4), cols] + rcv[1][q, part].astype(F32)).astype(BF16)
            hops[q][1]().start()

    def s4():
        for q, first, second, k1, k2, cols in box:
            hops[q][1]().wait_recv()
            part = rows_at(k2 * n4, n4)
            own = rows_at(h0 + k1 * n2 + k2 * n4, n4)
            gat[own, cols] = (acc[own, cols] + rcv[1][q, part].astype(F32) + rcv[2][q].astype(F32)).astype(BF16)
            hops[q][2]().start()

    def s5():
        for hop in hops:
            hop[2]().wait_recv()
            hop[3]().start()

    def s6():
        for hop in hops:
            hop[3]().wait_recv()
        back().start()

    def s7():
        back().wait_recv()

    return [s1, s2, s3, s4, s5, s6, s7]


def dc_stages(links, src, gat, stg, rcv):
    n_row = src.shape[0]
    half, quar, eigh = n_row // 2, n_row // 4, n_row // SUB
    h0 = links.core * half
    r0 = h0 + links.x * quar
    r_far = h0 + (1 - links.x) * quar
    y_own, y_far = links.y * n_row, (1 - links.y) * n_row

    def hop(start, size, axis):
        def ends():
            ref = gat.at[rows_at(start(), size), :]
            return ref, ref
        return links.copy(ends, axis)

    swap = links.copy(lambda: (stg[0], rcv[0]), "core")
    cross = links.copy(lambda: (stg[1], rcv[1]), "x")
    up_y = hop(lambda: y_own + r0, eigh, "y")
    down_x = hop(lambda: y_own + r0 + eigh, eigh, "x")
    up_x = hop(lambda: y_own + r0, eigh, "x")
    down_y = hop(lambda: y_own + r0 + eigh, eigh, "y")
    up_far = hop(lambda: y_far + r0, eigh, "x")
    down_far = hop(lambda: y_own + r_far + eigh, eigh, "y")
    back = [hop(lambda: y_own + h0, half, "core"), hop(lambda: y_far + h0, half, "core")]

    def s1():
        stg[0][...] = src[rows_at((1 - links.core) * half, half), :].astype(BF16)
        swap().start()

    def s2():
        swap().wait_recv()
        part = rows_at((1 - links.x) * quar, quar)
        stg[1][...] = (src[rows_at(r_far, quar), :] + rcv[0][part, :].astype(F32)).astype(BF16)
        cross().start()

    def s3():
        cross().wait_recv()
        part = rows_at(links.x * quar, quar)
        total = src[rows_at(r0, quar), :] + rcv[0][part, :].astype(F32) + rcv[1][...].astype(F32)
        gat[rows_at(y_own + r0, quar), :] = total.astype(BF16)
        for cp in (up_y, down_x, up_x, down_y):
            cp().start()

    def s4():
        up_y().wait_recv()
        up_far().start()
        down_x().wait_recv()
        down_far().start()

    def s5():
        for cp in (up_x, down_y, up_far, down_far):
            cp().wait_recv()
        for cp in back:
            cp().start()

    def s6():
        for cp in back:
            cp().wait_recv()

    return [s1, s2, s3, s4, s5, s6]


N_COPY = 10 * 5 + 4


def sum_scratch(n_row, n_col):
    half = n_row // 2
    return [pltpu.VMEM((half, n_col), BF16), pltpu.VMEM((2, half // 2, n_col // 2), BF16), pltpu.VMEM((2, half // 4, n_col // 2), BF16)]


W_CHUNK = 256


def backward_kernel(labels, flen, llen, stat, norm, pred, z_hbm, h_hbm, w_out, enc, loss_out, da_out, g_enc_out, g_out_out, g_dc_out, far_out,
                    dz_all, h_all, da_all, da_part, dz0, dz1, dz2, dh0, dh1, dh2, w_out_t, z_ring, dw_enc, dw_out, dc_out, g_enc, g_out, g_dc,
                    es0, es1, es2, er0, er1, er2, ps0, ps1, ps2, pr0, pr1, pr2, qs0, qs1, qs2, qr0, qr1, qr2, rs0, rs1, rs2, rr0, rr1, rr2, ds0, ds1, dr0, dr1,
                    q0_ref, q1_ref, norm_ref, gath, s_blank, s_label, s_alpha, s_beta, h_sem, z_sem, o_sem, w_sem, send_sem, recv_sem):
    step = pl.program_id(0)
    lane = lax.broadcasted_iota(jnp.int32, (SUB, LANES), 1)
    sub = lax.broadcasted_iota(jnp.int32, (SUB, LANES), 0)
    n_j, n_v = w_out.shape
    utt_rows = UG * ROWS

    dzs, dhs = (dz0, dz1, dz2), (dh0, dh1, dh2)
    prev = jnp.maximum(step - 1, 0)
    z_slot = lax.rem(step, B_RING)

    def multiply(ug):
        dhs[ug][...] = dot(dzs[ug][...], w_out_t[...])[:, :n_j]

    def h_copy(utt):
        rows = pl.ds(pl.multiple_of(utt * utt_rows, 16), utt_rows)
        return pltpu.make_async_copy(h_hbm.at[rows, :], h_all.at[rows, :], h_sem.at[utt])

    def z_copy(utt):
        slot = lax.rem(utt, B_RING)
        return pltpu.make_async_copy(z_hbm.at[utt], z_ring.at[slot], z_sem.at[slot])

    links = Links(send_sem, recv_sem)
    far = links.copy(lambda: (pred, far_out), "y")
    moves = (links.copy(lambda: (stat, gath.at[0]), "x"), links.copy(lambda: (stat, gath.at[1]), "core"),
             links.copy(lambda: (gath.at[0], gath.at[2]), "core"))
    n_enc = enc.shape[0]

    def weight_copies():
        return (pltpu.make_async_copy(w_out, dz_all.at[dz_all.shape[0] - n_j:, :], w_sem.at[0]),
                pltpu.make_async_copy(enc, g_out.at[:n_enc, :], w_sem.at[1]))
    e_st = sum_stages(links, dw_enc, g_enc, (es0, es1, es2), (er0, er1, er2), 0, n_v)
    p_st = sum_stages(links, dw_out, g_out, (ps0, ps1, ps2), (pr0, pr1, pr2), 0, n_v // 2)
    q_st = sum_stages(links, dw_out, g_out, (qs0, qs1, qs2), (qr0, qr1, qr2), n_v // 2, n_v // 4)
    r_st = sum_stages(links, dw_out, g_out, (rs0, rs1, rs2), (rr0, rr1, rr2), n_v // 2 + n_v // 4, n_v // 4)
    c_st = dc_stages(links, dc_out, g_dc, (ds0, ds1), (dr0, dr1))

    @pl.when(step == 0)
    def _():
        for utt in range(B_RING - 1):
            z_copy(utt).start()
            h_copy(utt).start()
        for cp in weight_copies():
            cp.start()
        links.greet()
        moves[0]().start()
        moves[1]().start()
        far().start()
        weight_copies()[0].wait()
        w_out_t[:, :n_j] = dz_all[dz_all.shape[0] - n_j:, :].T
        w_out_t[:, n_j:] = jnp.zeros((n_v, w_out_t.shape[1] - n_j), BF16)
        run_lattice(links, moves, stat, norm, flen, llen, q0_ref, q1_ref, norm_ref, loss_out, gath, s_blank, s_label, s_alpha, s_beta)

    def logit_grads(ug):
        shift = LANES - step
        lab_grp = label_column(labels, step, ug, sub)
        masks = [lab_grp - LANES * k == lane for k in range(n_v // LANES)]
        for t in range(0, T_LOC, 2):
            pair = []
            for idx in (ug * T_LOC + t, ug * T_LOC + t + 1):
                q0, q1, norm = [jnp.broadcast_to(pltpu.roll(ref[idx], shift, 1)[:, 0:1], (SUB, LANES)) for ref in (q0_ref, q1_ref, norm_ref)]
                row = (idx - ug * T_LOC) * SUB
                tiles = []
                for k in range(n_v // LANES):
                    z = z_ring[z_slot, ug, row:row + SUB, k * LANES:k * LANES + LANES]
                    g = jnp.exp2(z - norm) - jnp.where(masks[k], q1, 0.0)
                    tiles.append(g - jnp.where(lane == 0, q0, 0.0) if k == 0 else g)
                pair.append(jnp.concatenate(tiles, axis=1))
            rows = pl.ds(pl.multiple_of(step * utt_rows + ug * ROWS + t * SUB, 16), 16)
            dz = jnp.concatenate(pair, axis=0).astype(BF16)
            dz_all[rows, :] = dz
            dzs[ug][t * SUB:t * SUB + 16, :] = dz

    def hidden_grads(utt, ug):
        dc = None
        for t in range(0, T_LOC, 2):
            hid = h_all[pl.ds(pl.multiple_of(utt * utt_rows + ug * ROWS + t * SUB, 16), 16), :].astype(F32)
            ds = dhs[ug][t * SUB:t * SUB + 16, :] * (1.0 - hid * hid)
            both = ds[:SUB] + ds[SUB:]
            dc = both if dc is None else dc + both
            here = slice(t * SUB, t * SUB + 2 * SUB)
            for c in range(n_j // LANES):
                tile = ds[:, c * LANES:c * LANES + LANES]
                da_part[c, here, :] = tile + da_part[c, here, :] if ug else tile
        if ug == UG - 1:
            sums = [functools.reduce(jnp.add, [da_part[c, pl.ds(k, T_LOC, stride=SUB), :] for k in range(SUB)]) for c in range(n_j // LANES)]
            da_all[pl.ds(pl.multiple_of(utt * T_LOC, SUB), T_LOC), :] = jnp.concatenate(sums, axis=1)
        dc_out[pl.ds(pl.multiple_of(utt * N_UP + ug * SUB, SUB), SUB), :] = dc

    @pl.when(step + B_RING - 1 < N_UTT)
    def _():
        z_copy(step + B_RING - 1).start()
        h_copy(step + B_RING - 1).start()

    @pl.when(step < N_UTT)
    def _():
        h_copy(step).wait()
        z_copy(step).wait()
        multiply(2)
        logit_grads(0)
        hidden_grads(prev, 1)
        multiply(0)
        logit_grads(1)
        hidden_grads(prev, 2)
        multiply(1)
        logit_grads(2)
        hidden_grads(step, 0)

    @pl.when(step == N_UTT)
    def _():
        multiply(2)
        hidden_grads(prev, 1)
        hidden_grads(prev, 2)
        da = da_all[...].astype(BF16)
        da_out[...] = da
        weight_copies()[1].wait()
        dw_enc[...] = dot(da, g_out[:n_enc, :], ((0,), (0,)))
        e_st[0]()
        c_st[0]()

    plan = [
        ((c_st[1], e_st[1]), ()),
        ((), (c_st[2], p_st[0])),
        ((e_st[2], p_st[1]), ()),
        ((e_st[3], q_st[0]), (
            r_st[0], p_st[2], q_st[1], r_st[1], c_st[3], p_st[3], r_st[2], q_st[2], e_st[4], c_st[4], q_st[3], r_st[3], p_st[4],
            q_st[4], r_st[4], p_st[5], e_st[5], q_st[5])),
    ]
    for part, (lo, hi) in enumerate(((0, 3 * LANES), (3 * LANES, n_j))):
        @pl.when(step > N_UTT)
        def _(lo=lo, hi=hi):
            cols = pl.ds(pl.multiple_of((step - N_UTT - 1) * W_CHUNK, W_CHUNK), W_CHUNK)
            dw_out[lo:hi, cols] = dot(h_all[:, lo:hi], dz_all[:, cols], ((0,), (0,)))

        for n, stages in enumerate(plan):
            if stages[part]:
                @pl.when(step == N_UTT + 1 + n)
                def _(stages=stages[part]):
                    for stage in stages:
                        stage()

    @pl.when(step == N_UTT + len(plan))
    def _():
        p_st[6]()
        r_st[5]()
        r_st[6]()
        e_st[6]()
        out_enc = pltpu.make_async_copy(g_enc, g_enc_out, o_sem.at[1])
        out_enc.start()
        q_st[6]()
        out_out = pltpu.make_async_copy(g_out, g_out_out, o_sem.at[2])
        out_out.start()
        c_st[5]()
        out_dc = pltpu.make_async_copy(g_dc, g_dc_out, o_sem.at[0])
        out_dc.start()
        far().wait_recv()
        for cp in links.copies:
            cp().wait_send()
        out_dc.wait()
        out_enc.wait()
        out_out.wait()


def joint_backward(labels, flen, llen, stat, norm, pred, z, h, w_out, enc):
    n_j, n_v = w_out.shape
    n_cell = N_UTT * UG * ROWS
    n_dc = N_UTT * N_UP
    full = lambda shape: pl.BlockSpec(shape, lambda i: (0,) * len(shape), pipeline_mode=pl.Buffered(1))
    return pl.pallas_call(
        backward_kernel,
        grid=(N_UTT + 1 + n_v // W_CHUNK,),
        in_specs=[pl.BlockSpec(memory_space=pltpu.SMEM)] * 3 + [full(stat.shape), full(norm.shape)] + [pl.BlockSpec(memory_space=pl.ANY)] * 5,
        out_specs=[full((SUB, LANES)), full((N_UTT * T_LOC, n_j))] + [pl.BlockSpec(memory_space=pl.ANY)] * 4,
        out_shape=[
            jax.ShapeDtypeStruct((SUB, LANES), F32),
            jax.ShapeDtypeStruct((N_UTT * T_LOC, n_j), BF16),
            jax.ShapeDtypeStruct((n_j, n_v), BF16),
            jax.ShapeDtypeStruct((n_j, n_v), BF16),
            jax.ShapeDtypeStruct((2 * n_dc, n_j), BF16),
            jax.ShapeDtypeStruct(pred.shape, BF16),
        ],
        scratch_shapes=[
            pltpu.VMEM((n_cell, n_v), BF16), pltpu.VMEM((n_cell, n_j), BF16), pltpu.VMEM((N_UTT * T_LOC, n_j), F32),
            pltpu.VMEM((n_j // LANES, ROWS, LANES), F32),
            *[pltpu.VMEM((ROWS, n_v), BF16)] * 3, *[pltpu.VMEM((ROWS, n_j), F32)] * 3,
            pltpu.VMEM((n_v, n_j + (-n_j) % 256), BF16), pltpu.VMEM((B_RING, UG, ROWS, n_v), F32),
            pltpu.VMEM((n_j, n_v), F32), pltpu.VMEM((n_j, n_v), F32), pltpu.VMEM((n_dc, n_j), F32),
            pltpu.VMEM((n_j, n_v), BF16), pltpu.VMEM((n_j, n_v), BF16), pltpu.VMEM((2 * n_dc, n_j), BF16),
            *sum_scratch(n_j, n_v) * 2, *sum_scratch(n_j, n_v // 2) * 2, *sum_scratch(n_j, n_v // 4) * 4,
            *[pltpu.VMEM((n_dc // 2, n_j), BF16), pltpu.VMEM((n_dc // 4, n_j), BF16)] * 2,
            *[pltpu.VMEM(norm.shape, F32)] * 3, pltpu.VMEM((N_SEQ - 1,) + stat.shape, F32),
            *[pltpu.VMEM(((N_DIAG + 2) * N_UP, LANES), F32)] * 4,
            pltpu.SemaphoreType.DMA((N_UTT,)), pltpu.SemaphoreType.DMA((B_RING,)), pltpu.SemaphoreType.DMA((3,)), pltpu.SemaphoreType.DMA((2,)),
            pltpu.SemaphoreType.DMA((N_COPY,)), pltpu.SemaphoreType.DMA((N_COPY,)),
        ],
        compiler_params=pltpu.CompilerParams(collective_id=1, has_side_effects=True, vmem_limit_bytes=VMEM_FULL),
        name="joint_backward",
    )(labels, flen, llen, stat, norm, pred, z, h.reshape(n_cell, n_j), w_out, enc)


def finish_kernel(loss, *refs):
    ins, o_loss, outs = refs[:FIN_IN], refs[FIN_IN], refs[FIN_IN + 1:FIN_IN + 1 + FIN_OUT]
    bufs, vals, in_sem, out_sem = refs[FIN_IN + 1 + FIN_OUT:-FIN_OUT - 2], refs[-FIN_OUT - 2:-2], refs[-2], refs[-1]
    g_dc, pred, pred_far, g_out, g_enc, w_pred, da, w_enc = bufs
    v_wpred, v_wout, v_wenc, v_pred, v_enc = vals
    loads = [pltpu.make_async_copy(src, dst, in_sem.at[k]) for k, (src, dst) in enumerate(zip(ins, bufs))]
    stores = [pltpu.make_async_copy(src, dst, out_sem.at[k]) for k, (src, dst) in enumerate(zip(vals, outs))]
    for cp in loads:
        cp.start()
    y = lax.axis_index("data")
    n_r = pred.shape[0]
    o_loss[...] = loss[0:1, :N_UTT]
    for k in range(3):
        loads[k].wait()
    dc_own = g_dc[rows_at(y * n_r, n_r), :]
    dc_far = g_dc[rows_at((1 - y) * n_r, n_r), :]
    v_wpred[...] = dot(pred[...], dc_own, ((0,), (0,))) + dot(pred_far[...], dc_far, ((0,), (0,)))
    stores[0].start()
    loads[3].wait()
    v_wout[...] = g_out[...].astype(F32)
    stores[1].start()
    loads[4].wait()
    v_wenc[...] = g_enc[...].astype(F32).T
    stores[2].start()
    loads[5].wait()
    v_pred[...] = dot(dc_own, w_pred[...], ((1,), (1,)))
    stores[3].start()
    loads[6].wait()
    loads[7].wait()
    v_enc[...] = dot(da[...], w_enc[...], ((1,), (1,))).astype(BF16)
    stores[4].start()
    for cp in stores:
        cp.wait()


FIN_IN = 8
FIN_OUT = 5


def finish(loss, g_enc, g_out, g_dc, pred, pred_far, w_pred, da, w_enc):
    vm = pl.BlockSpec(memory_space=pltpu.VMEM)
    hbm = pl.BlockSpec(memory_space=pl.ANY)
    ins = (g_dc, pred, pred_far, g_out, g_enc, w_pred, da, w_enc)
    outs = [(w_pred.shape, F32), (g_out.shape, F32), (w_enc.shape, F32), (pred.shape, F32), (pred.shape, BF16)]
    loss, grad_w_pred, grad_w_out, grad_w_enc, grad_pred, grad_enc = pl.pallas_call(
        finish_kernel,
        in_specs=[vm] + [hbm] * FIN_IN,
        out_specs=[vm] + [hbm] * FIN_OUT,
        out_shape=[jax.ShapeDtypeStruct((1, N_UTT), F32)] + [jax.ShapeDtypeStruct(*o) for o in outs],
        scratch_shapes=[pltpu.VMEM(v.shape, v.dtype) for v in ins] + [pltpu.VMEM(*o) for o in outs]
        + [pltpu.SemaphoreType.DMA((FIN_IN,)), pltpu.SemaphoreType.DMA((FIN_OUT,))],
        compiler_params=pltpu.CompilerParams(vmem_limit_bytes=VMEM_FULL),
        name="finish",
    )(loss, *ins)
    return loss, grad_enc, grad_pred, grad_w_enc, grad_w_pred, grad_w_out


def solution(mesh):
    utt_rows = P(("part", "data"))
    utt_mats = P(("part", "data"), None)
    utt_cube = P(("part", "data"), None, None)
    enc_spec = P(("part", "data"), "seq", None)
    weight_in = P(None, None)
    weight_out = P("part", None)

    def body(enc_loc, pred_loc, w_enc, w_pred, w_out, labels, frame_len, label_len):
        n_h = enc_loc.shape[2]
        enc2 = enc_loc.reshape(N_UTT * T_LOC, n_h)
        pred2 = pred_loc.reshape(N_UTT * N_UP, n_h)
        z, h, stat, norm = joint_forward(labels, label_len, enc2, pred2, w_enc, w_pred, w_out)
        loss, da, g_enc, g_out, g_dc, pred_far = joint_backward(labels, frame_len, label_len, stat, norm, pred2, z, h, w_out, enc2)
        loss, grad_enc, grad_pred, grad_w_enc, grad_w_pred, grad_w_out = finish(loss, g_enc, g_out, g_dc, pred2, pred_far, w_pred, da, w_enc)
        return loss.reshape(N_UTT), grad_enc.reshape(enc_loc.shape), grad_pred.reshape(pred_loc.shape), grad_w_enc, grad_w_pred, grad_w_out

    return jax.shard_map(body, mesh=mesh, in_specs=(enc_spec, utt_cube, weight_in, weight_in, weight_in, utt_mats, utt_rows, utt_rows), out_specs=(utt_rows, enc_spec, utt_cube, weight_out, weight_out, weight_out), check_vma=False)
```

```python
import functools

import jax
import jax.numpy as jnp
from jax import lax
from jax.experimental import pallas as pl
from jax.experimental.pallas import tpu as pltpu
from jax.sharding import PartitionSpec as P

NEG = -1e30
SUB = 8
LANES = 128
LOG2E = 1.4426950408889634
LN2 = 0.6931471805599453
F32 = jnp.float32
BF16 = jnp.bfloat16
MESH = pl.DeviceIdType.MESH
VMEM_FULL = 67_000_000
N_UTT = 16
T_LOC = 24
N_UP = 24
UG = 3
N_SEQ = 4
T_ALL = T_LOC * N_SEQ
RING = 4
B_RING = 3
N_DIAG = T_ALL + N_UP - 1
ROWS = SUB * T_LOC


def dot(lhs, rhs, dims=((1,), (0,))):
    return lax.dot_general(lhs, rhs, (dims, ((), ())), preferred_element_type=F32)


def label_column(labels, utt, ug, sub):
    col = jnp.zeros((SUB, LANES), jnp.int32)
    for k in range(SUB):
        col = jnp.where(sub == k, labels[utt, jnp.minimum(ug * SUB + k, N_UP - 2)], col)
    return col


def forward_kernel(labels, llen, enc, pred, w_enc, w_pred, w_out, z_hbm, h_hbm, stat_out, norm_out, act_e, act_p, h_next, z_last, z_ring, h_ring, z_sem, h_sem):
    step = pl.program_id(0)
    lane = lax.broadcasted_iota(jnp.int32, (SUB, LANES), 1)
    sub = lax.broadcasted_iota(jnp.int32, (SUB, LANES), 0)
    n_v = w_out.shape[1]

    @pl.when(step == 0)
    def _():
        act_e[...] = dot(enc[...], w_enc[...]).astype(BF16).astype(F32)
        act_p[...] = dot(pred[...], w_pred[...]).astype(BF16).astype(F32)
        stat_out[...] = jnp.zeros_like(stat_out)
        norm_out[...] = jnp.zeros_like(norm_out)

    def hidden(utt, ug, dst):
        row = pl.multiple_of(utt * N_UP, SUB)
        c_grp = act_p[pl.ds(row + SUB * ug, SUB), :]
        a_utt = act_e[pl.ds(row, T_LOC), :]
        for t in range(0, T_LOC, 2):
            pre = jnp.concatenate([a_utt[t:t + 1, :] + c_grp, a_utt[t + 1:t + 2, :] + c_grp], axis=0)
            dst[t * SUB:t * SUB + 16, :] = jnp.tanh(pre).astype(BF16)

    def soften(utt, ug, src):
        lab_grp = label_column(labels, jnp.maximum(utt, 0), ug, sub)
        masks = [lab_grp - LANES * k == lane for k in range(n_v // LANES)]
        for t4 in range(T_LOC // 4):
            cur = stat_out[ug * 6 + t4]
            for k in range(4):
                t = t4 * 4 + k
                z = [src[t * SUB:t * SUB + SUB, c * LANES:c * LANES + LANES] for c in range(n_v // LANES)]
                top = functools.reduce(jnp.maximum, z)
                tot = functools.reduce(jnp.add, [jnp.exp2(v - top) for v in z])
                picked = functools.reduce(jnp.add, [jnp.where(m, v, 0.0) for m, v in zip(masks, z)])
                row_top = jnp.max(top, axis=1, keepdims=True)
                row_tot = jnp.sum(tot * jnp.exp2(top - row_top), axis=1, keepdims=True)
                norm = row_top + jnp.log2(row_tot)
                blank = z[0][:, 0:1] - norm
                label = jnp.sum(picked, axis=1, keepdims=True) - norm
                cur = jnp.where(lane == utt + 32 * k, blank, cur)
                cur = jnp.where(lane == utt + 32 * k + 16, label, cur)
                norm_out[ug * T_LOC + t] = jnp.where(lane == utt, norm, norm_out[ug * T_LOC + t])
            stat_out[ug * 6 + t4] = cur

    def puts(utt):
        at = lax.rem(utt, RING)
        return (pltpu.make_async_copy(z_ring.at[at], z_hbm.at[utt], z_sem.at[at]),
                pltpu.make_async_copy(h_ring.at[at], h_hbm.at[utt], h_sem.at[at]))

    @pl.when(step == 0)
    def _():
        hidden(0, 0, h_next)

    @pl.when(step >= RING)
    def _():
        for cp in puts(step - RING):
            cp.wait()

    slot = lax.rem(step, RING)
    z_out, h_out = z_ring.at[slot], h_ring.at[slot]
    groups = lax.div(llen[step], SUB) + 1
    last_of = lambda utt: lax.div(llen[utt], SUB)

    def utterance(n_grp):
        h_out[0] = h_next[...]
        for ug in range(n_grp):
            z = dot(h_out[ug] if ug else h_next[...], w_out[...]) * LOG2E
            z_out[ug] = z
            if ug == 0:
                soften(step - 1, last_of(jnp.maximum(step - 1, 0)), z_last)
            else:
                soften(step, ug - 1, z_out.at[ug - 1])
            if ug < n_grp - 1:
                hidden(step, ug + 1, h_out.at[ug + 1])
            else:
                z_last[...] = z
                hidden(jnp.minimum(step + 1, N_UTT - 1), 0, h_next)

        if n_grp < UG:
            @pl.when(step < RING)
            def _():
                for ug in range(n_grp, UG):
                    z_out[ug] = jnp.zeros(z_out.shape[1:], F32)
                    h_out[ug] = jnp.zeros(h_out.shape[1:], BF16)

    for n_grp in range(1, UG + 1):
        pl.when(groups == n_grp)(functools.partial(utterance, n_grp))
    for cp in puts(step):
        cp.start()

    @pl.when(step == N_UTT - 1)
    def _():
        soften(step, last_of(step), z_last)
        for back in range(RING - 1, -1, -1):
            for cp in puts(step - back):
                cp.wait()


def joint_forward(labels, llen, enc, pred, w_enc, w_pred, w_out):
    n_j, n_v = w_out.shape
    full = lambda shape: pl.BlockSpec(shape, lambda i: (0,) * len(shape), pipeline_mode=pl.Buffered(1))
    return pl.pallas_call(
        forward_kernel,
        grid=(N_UTT,),
        in_specs=[pl.BlockSpec(memory_space=pltpu.SMEM)] * 2 + [full(v.shape) for v in (enc, pred, w_enc, w_pred, w_out)],
        out_specs=[
            pl.BlockSpec(memory_space=pl.ANY),
            pl.BlockSpec(memory_space=pl.ANY),
            pl.BlockSpec((UG * 6, SUB, LANES), lambda i: (0, 0, 0)),
            pl.BlockSpec((UG * T_LOC, SUB, LANES), lambda i: (0, 0, 0)),
        ],
        out_shape=[
            jax.ShapeDtypeStruct((N_UTT, UG, ROWS, n_v), F32),
            jax.ShapeDtypeStruct((N_UTT, UG, ROWS, n_j), BF16),
            jax.ShapeDtypeStruct((UG * 6, SUB, LANES), F32),
            jax.ShapeDtypeStruct((UG * T_LOC, SUB, LANES), F32),
        ],
        scratch_shapes=[pltpu.VMEM((N_UTT * T_LOC, n_j), F32), pltpu.VMEM((N_UTT * N_UP, n_j), F32), pltpu.VMEM((ROWS, n_j), BF16), pltpu.VMEM((ROWS, n_v), F32),
            pltpu.VMEM((RING, UG, ROWS, n_v), F32), pltpu.VMEM((RING, UG, ROWS, n_j), BF16),
            pltpu.SemaphoreType.DMA((RING,)), pltpu.SemaphoreType.DMA((RING,))],
        compiler_params=pltpu.CompilerParams(vmem_limit_bytes=VMEM_FULL),
        name="joint_forward",
    )(labels, llen, enc, pred, w_enc, w_pred, w_out)


def lae2(x, y):
    return jnp.maximum(x, y) + jnp.log2(1.0 + jnp.exp2(-jnp.abs(x - y)))


def run_lattice(links, moves, stat, norm, flen, llen, q0_out, q1_out, norm_out, loss_out, gath, s_blank, s_label, s_alpha, s_beta):
    me = links.seq
    mate = me + 1 - 2 * links.core
    across = lax.rem(me + 2, N_SEQ)
    row_x, row_core, row_relay = moves
    sub = lax.broadcasted_iota(jnp.int32, (SUB, LANES), 0)
    sub24 = lax.broadcasted_iota(jnp.int32, (N_UP, LANES), 0)
    lane = lax.broadcasted_iota(jnp.int32, (SUB, LANES), 1)
    tb = jnp.zeros((SUB, LANES), jnp.int32)
    ub = jnp.zeros((SUB, LANES), jnp.int32)
    for b in range(N_UTT):
        at_b = lax.rem(lane, N_UTT) == b
        tb = jnp.where(at_b, flen[b], tb)
        ub = jnp.where(at_b, llen[b], ub)
    n_pad = s_blank.shape[0]

    def fill(i, c):
        s_blank[pl.ds(pl.multiple_of(i * SUB, SUB), SUB), :] = jnp.full((SUB, LANES), NEG, F32)
        s_label[pl.ds(pl.multiple_of(i * SUB, SUB), SUB), :] = jnp.full((SUB, LANES), NEG, F32)
        return c

    lax.fori_loop(0, n_pad // SUB, fill, 0, unroll=11)
    end_grp = [jnp.where(sub + SUB * ug == ub, 0.0, NEG) for ug in range(UG)]
    for d in range(T_ALL, N_DIAG + 2):
        for ug in range(UG):
            s_blank[d * N_UP + SUB * ug:d * N_UP + SUB * ug + SUB, :] = end_grp[ug]

    def place(src, src_seq):
        for t4 in range(T_LOC // 4):
            for ug in range(UG):
                val = src[ug * 6 + t4]
                in_u = sub + SUB * ug <= ub
                in_l = sub + SUB * ug < ub
                for k in range(4):
                    t = src_seq * T_LOC + t4 * 4 + k
                    bl = val if k == 0 else pltpu.roll(val, LANES - 32 * k, 1)
                    la = pltpu.roll(val, 112 - 32 * k, 1)
                    ok = t < tb
                    s_blank[pl.ds(t * N_UP + 200 * ug, SUB, stride=25), :] = jnp.where(ok, jnp.where(in_u, bl, NEG), end_grp[ug])
                    s_label[pl.ds(t * N_UP + 200 * ug, SUB, stride=25), :] = jnp.where(ok & in_l, la, NEG)

    place(stat, me)
    row_core().wait_recv()
    place(gath.at[1], mate)
    row_x().wait_recv()
    row_relay().start()
    place(gath.at[0], across)
    row_relay().wait_recv()
    place(gath.at[2], lax.rem(mate + 2, N_SEQ))

    alpha0 = jnp.where(sub24 == 0, 0.0, NEG)
    s_alpha[pl.ds(0, N_UP), :] = alpha0
    beta_end = jnp.where(sub24 == jnp.concatenate([ub] * UG, axis=0), 0.0, NEG)
    s_beta[pl.ds(N_DIAG * N_UP, N_UP), :] = beta_end
    s_beta[pl.ds((N_DIAG + 1) * N_UP, SUB), :] = jnp.full((SUB, LANES), NEG, F32)

    def wave(i, carry):
        alpha, beta = carry
        row = pl.multiple_of(i * N_UP, SUB)
        x = alpha + s_blank[pl.ds(row, N_UP), :]
        y = alpha + s_label[pl.ds(row, N_UP), :]
        y = jnp.where(sub24 == 0, NEG, pltpu.roll(y, 1, 0))
        alpha = lae2(x, y)
        s_alpha[pl.ds(pl.multiple_of(row + N_UP, SUB), N_UP), :] = alpha
        brow = pl.multiple_of((N_DIAG - 1 - i) * N_UP, SUB)
        bx = beta + s_blank[pl.ds(brow, N_UP), :]
        by = pltpu.roll(beta, N_UP - 1, 0) + s_label[pl.ds(brow, N_UP), :]
        beta = lae2(bx, by)
        s_beta[pl.ds(brow, N_UP), :] = beta
        return alpha, beta

    _, beta = lax.fori_loop(0, N_DIAG, wave, (alpha0, beta_end), unroll=7)
    log_p = beta[0:1, :]
    loss_out[...] = jnp.broadcast_to(-LN2 * log_p, (SUB, LANES))
    for t in range(T_LOC):
        tg = me * T_LOC + t
        for ug in range(UG):
            base = tg * N_UP + 200 * ug
            grp = lambda ref, off: ref[pl.ds(base + off, SUB, stride=25), :]
            al = grp(s_alpha, 0) - log_p
            ok = (tg < tb) & (sub + SUB * ug <= ub)
            q0 = jnp.where(ok, jnp.exp2(al + grp(s_blank, 0) + grp(s_beta, 24)), 0.0)
            q1 = jnp.where(ok, jnp.exp2(al + grp(s_label, 0) + grp(s_beta, 25)), 0.0)
            idx = ug * T_LOC + t
            q0_out[idx] = q0
            q1_out[idx] = q1
            norm_out[idx] = norm[idx] - jnp.log2(q0 + q1)


class Links:
    def __init__(self, send_sem, recv_sem):
        self.send_sem, self.recv_sem, self.copies = send_sem, recv_sem, []
        seq = lax.axis_index("seq")
        self.core = lax.rem(seq, 2)
        self.x = lax.div(seq, 2)
        self.y = lax.axis_index("data")
        self.seq = seq
        self.dev = {
            "core": {"seq": seq + 1 - 2 * self.core},
            "x": {"seq": lax.rem(seq + 2, N_SEQ)},
            "y": {"data": 1 - self.y},
        }

    def greet(self):
        barrier = pltpu.get_barrier_semaphore()
        for dev in self.dev.values():
            pl.semaphore_signal(barrier, inc=1, device_id=dev, device_id_type=MESH)
        pl.semaphore_wait(barrier, 3)

    def copy(self, ends, axis):
        i = len(self.copies)

        def make():
            src, dst = ends()
            return pltpu.make_async_remote_copy(src_ref=src, dst_ref=dst, send_sem=self.send_sem.at[i], recv_sem=self.recv_sem.at[i],
                                                device_id=self.dev[axis], device_id_type=MESH)

        self.copies.append(make)
        return make


def rows_at(start, size):
    return pl.ds(pl.multiple_of(start, 16), size)


def sum_stages(links, acc, gat, stg, rcv, col0, n_col):
    half = acc.shape[0] // 2
    h0 = links.core * half
    every = pl.ds(col0, n_col)
    box = []
    for q in range(2):
        first, second = ("x", "y") if q == 0 else ("y", "x")
        k1, k2 = (links.x, links.y) if q == 0 else (links.y, links.x)
        box.append((q, first, second, k1, k2, pl.ds(col0 + q * (n_col // 2), n_col // 2)))
    n2, n4 = half // 2, half // 4

    def same(rows, cols):
        def ends():
            ref = gat.at[rows(), cols]
            return ref, ref
        return ends

    swap = links.copy(lambda: (stg[0], rcv[0]), "core")
    back = links.copy(same(lambda: rows_at(h0, half), every), "core")
    hops = [(
        links.copy(lambda q=q: (stg[1].at[q], rcv[1].at[q]), first),
        links.copy(lambda q=q: (stg[2].at[q], rcv[2].at[q]), second),
        links.copy(same(lambda k1=k1, k2=k2: rows_at(h0 + k1 * n2 + k2 * n4, n4), cols), second),
        links.copy(same(lambda k1=k1: rows_at(h0 + k1 * n2, n2), cols), first),
    ) for q, first, second, k1, k2, cols in box]

    def s1():
        stg[0][...] = acc[rows_at((1 - links.core) * half, half), every].astype(BF16)
        swap().start()

    def s2():
        swap().wait_recv()
        own = rows_at(h0, half)
        acc[own, every] = acc[own, every] + rcv[0][...].astype(F32)
        for q, first, second, k1, k2, cols in box:
            stg[1][q] = acc[rows_at(h0 + (1 - k1) * n2, n2), cols].astype(BF16)
            hops[q][0]().start()

    def s3():
        for q, first, second, k1, k2, cols in box:
            hops[q][0]().wait_recv()
            part = rows_at((1 - k2) * n4, n4)
            stg[2][q] = (acc[rows_at(h0 + k1 * n2 + (1 - k2) * n4, n4), cols] + rcv[1][q, part].astype(F32)).astype(BF16)
            hops[q][1]().start()

    def s4():
        for q, first, second, k1, k2, cols in box:
            hops[q][1]().wait_recv()
            part = rows_at(k2 * n4, n4)
            own = rows_at(h0 + k1 * n2 + k2 * n4, n4)
            gat[own, cols] = (acc[own, cols] + rcv[1][q, part].astype(F32) + rcv[2][q].astype(F32)).astype(BF16)
            hops[q][2]().start()

    def s5():
        for hop in hops:
            hop[2]().wait_recv()
            hop[3]().start()

    def s6():
        for hop in hops:
            hop[3]().wait_recv()
        back().start()

    def s7():
        back().wait_recv()

    return [s1, s2, s3, s4, s5, s6, s7]


def dc_stages(links, src, gat, stg, rcv):
    n_row = src.shape[0]
    half, quar, eigh = n_row // 2, n_row // 4, n_row // SUB
    h0 = links.core * half
    r0 = h0 + links.x * quar
    r_far = h0 + (1 - links.x) * quar
    y_own, y_far = links.y * n_row, (1 - links.y) * n_row

    def hop(start, size, axis):
        def ends():
            ref = gat.at[rows_at(start(), size), :]
            return ref, ref
        return links.copy(ends, axis)

    swap = links.copy(lambda: (stg[0], rcv[0]), "core")
    cross = links.copy(lambda: (stg[1], rcv[1]), "x")
    up_y = hop(lambda: y_own + r0, eigh, "y")
    down_x = hop(lambda: y_own + r0 + eigh, eigh, "x")
    up_x = hop(lambda: y_own + r0, eigh, "x")
    down_y = hop(lambda: y_own + r0 + eigh, eigh, "y")
    up_far = hop(lambda: y_far + r0, eigh, "x")
    down_far = hop(lambda: y_own + r_far + eigh, eigh, "y")
    back = [hop(lambda: y_own + h0, half, "core"), hop(lambda: y_far + h0, half, "core")]

    def s1():
        stg[0][...] = src[rows_at((1 - links.core) * half, half), :].astype(BF16)
        swap().start()

    def s2():
        swap().wait_recv()
        part = rows_at((1 - links.x) * quar, quar)
        stg[1][...] = (src[rows_at(r_far, quar), :] + rcv[0][part, :].astype(F32)).astype(BF16)
        cross().start()

    def s3():
        cross().wait_recv()
        part = rows_at(links.x * quar, quar)
        total = src[rows_at(r0, quar), :] + rcv[0][part, :].astype(F32) + rcv[1][...].astype(F32)
        gat[rows_at(y_own + r0, quar), :] = total.astype(BF16)
        for cp in (up_y, down_x, up_x, down_y):
            cp().start()

    def s4():
        up_y().wait_recv()
        up_far().start()
        down_x().wait_recv()
        down_far().start()

    def s5():
        for cp in (up_x, down_y, up_far, down_far):
            cp().wait_recv()
        for cp in back:
            cp().start()

    def s6():
        for cp in back:
            cp().wait_recv()

    return [s1, s2, s3, s4, s5, s6]


N_COPY = 10 * 5 + 4


def sum_scratch(n_row, n_col):
    half = n_row // 2
    return [pltpu.VMEM((half, n_col), BF16), pltpu.VMEM((2, half // 2, n_col // 2), BF16), pltpu.VMEM((2, half // 4, n_col // 2), BF16)]


W_CHUNK = 256


def backward_kernel(labels, flen, llen, stat, norm, pred, z_hbm, h_hbm, w_out, enc, loss_out, da_out, g_enc_out, g_out_out, g_dc_out, far_out,
                    dz_all, h_all, da_all, da_part, dz0, dz1, dz2, dh0, dh1, dh2, w_out_t, z_ring, dw_enc, dw_out, dc_out, g_enc, g_out, g_dc,
                    es0, es1, es2, er0, er1, er2, ps0, ps1, ps2, pr0, pr1, pr2, qs0, qs1, qs2, qr0, qr1, qr2, rs0, rs1, rs2, rr0, rr1, rr2, ds0, ds1, dr0, dr1,
                    q0_ref, q1_ref, norm_ref, gath, s_blank, s_label, s_alpha, s_beta, h_sem, z_sem, o_sem, w_sem, send_sem, recv_sem):
    step = pl.program_id(0)
    lane = lax.broadcasted_iota(jnp.int32, (SUB, LANES), 1)
    sub = lax.broadcasted_iota(jnp.int32, (SUB, LANES), 0)
    n_j, n_v = w_out.shape
    utt_rows = UG * ROWS

    dzs, dhs = (dz0, dz1, dz2), (dh0, dh1, dh2)
    prev = jnp.maximum(step - 1, 0)
    z_slot = lax.rem(step, B_RING)

    def multiply(ug):
        dhs[ug][...] = dot(dzs[ug][...], w_out_t[...])[:, :n_j]

    def h_copy(utt):
        rows = pl.ds(pl.multiple_of(utt * utt_rows, 16), utt_rows)
        return pltpu.make_async_copy(h_hbm.at[rows, :], h_all.at[rows, :], h_sem.at[utt])

    def z_copy(utt):
        slot = lax.rem(utt, B_RING)
        return pltpu.make_async_copy(z_hbm.at[utt], z_ring.at[slot], z_sem.at[slot])

    links = Links(send_sem, recv_sem)
    far = links.copy(lambda: (pred, far_out), "y")
    moves = (links.copy(lambda: (stat, gath.at[0]), "x"), links.copy(lambda: (stat, gath.at[1]), "core"),
             links.copy(lambda: (gath.at[0], gath.at[2]), "core"))
    n_enc = enc.shape[0]

    def weight_copies():
        return (pltpu.make_async_copy(w_out, dz_all.at[dz_all.shape[0] - n_j:, :], w_sem.at[0]),
                pltpu.make_async_copy(enc, g_out.at[:n_enc, :], w_sem.at[1]))
    e_st = sum_stages(links, dw_enc, g_enc, (es0, es1, es2), (er0, er1, er2), 0, n_v)
    p_st = sum_stages(links, dw_out, g_out, (ps0, ps1, ps2), (pr0, pr1, pr2), 0, n_v // 2)
    q_st = sum_stages(links, dw_out, g_out, (qs0, qs1, qs2), (qr0, qr1, qr2), n_v // 2, n_v // 4)
    r_st = sum_stages(links, dw_out, g_out, (rs0, rs1, rs2), (rr0, rr1, rr2), n_v // 2 + n_v // 4, n_v // 4)
    c_st = dc_stages(links, dc_out, g_dc, (ds0, ds1), (dr0, dr1))

    @pl.when(step == 0)
    def _():
        for utt in range(B_RING - 1):
            z_copy(utt).start()
            h_copy(utt).start()
        for cp in weight_copies():
            cp.start()
        links.greet()
        moves[0]().start()
        moves[1]().start()
        far().start()
        weight_copies()[0].wait()
        w_out_t[:, :n_j] = dz_all[dz_all.shape[0] - n_j:, :].T
        w_out_t[:, n_j:] = jnp.zeros((n_v, w_out_t.shape[1] - n_j), BF16)
        run_lattice(links, moves, stat, norm, flen, llen, q0_ref, q1_ref, norm_ref, loss_out, gath, s_blank, s_label, s_alpha, s_beta)

    def logit_grads(ug):
        shift = LANES - step
        lab_grp = label_column(labels, step, ug, sub)
        masks = [lab_grp - LANES * k == lane for k in range(n_v // LANES)]
        for t in range(0, T_LOC, 2):
            pair = []
            for idx in (ug * T_LOC + t, ug * T_LOC + t + 1):
                q0, q1, norm = [jnp.broadcast_to(pltpu.roll(ref[idx], shift, 1)[:, 0:1], (SUB, LANES)) for ref in (q0_ref, q1_ref, norm_ref)]
                row = (idx - ug * T_LOC) * SUB
                tiles = []
                for k in range(n_v // LANES):
                    z = z_ring[z_slot, ug, row:row + SUB, k * LANES:k * LANES + LANES]
                    g = jnp.exp2(z - norm) - jnp.where(masks[k], q1, 0.0)
                    tiles.append(g - jnp.where(lane == 0, q0, 0.0) if k == 0 else g)
                pair.append(jnp.concatenate(tiles, axis=1))
            rows = pl.ds(pl.multiple_of(step * utt_rows + ug * ROWS + t * SUB, 16), 16)
            dz = jnp.concatenate(pair, axis=0).astype(BF16)
            dz_all[rows, :] = dz
            dzs[ug][t * SUB:t * SUB + 16, :] = dz

    def hidden_grads(utt, ug):
        dc = None
        for t in range(0, T_LOC, 2):
            hid = h_all[pl.ds(pl.multiple_of(utt * utt_rows + ug * ROWS + t * SUB, 16), 16), :].astype(F32)
            ds = dhs[ug][t * SUB:t * SUB + 16, :] * (1.0 - hid * hid)
            both = ds[:SUB] + ds[SUB:]
            dc = both if dc is None else dc + both
            here = slice(t * SUB, t * SUB + 2 * SUB)
            for c in range(n_j // LANES):
                tile = ds[:, c * LANES:c * LANES + LANES]
                da_part[c, here, :] = tile + da_part[c, here, :] if ug else tile
        if ug == UG - 1:
            sums = [functools.reduce(jnp.add, [da_part[c, pl.ds(k, T_LOC, stride=SUB), :] for k in range(SUB)]) for c in range(n_j // LANES)]
            da_all[pl.ds(pl.multiple_of(utt * T_LOC, SUB), T_LOC), :] = jnp.concatenate(sums, axis=1)
        dc_out[pl.ds(pl.multiple_of(utt * N_UP + ug * SUB, SUB), SUB), :] = dc

    @pl.when(step + B_RING - 1 < N_UTT)
    def _():
        z_copy(step + B_RING - 1).start()
        h_copy(step + B_RING - 1).start()

    @pl.when(step < N_UTT)
    def _():
        h_copy(step).wait()
        z_copy(step).wait()
        multiply(2)
        logit_grads(0)
        hidden_grads(prev, 1)
        multiply(0)
        logit_grads(1)
        hidden_grads(prev, 2)
        multiply(1)
        logit_grads(2)
        hidden_grads(step, 0)

    @pl.when(step >= N_UTT)
    def _():
        @pl.when(step == N_UTT)
        def _():
            multiply(2)
            hidden_grads(prev, 1)
            hidden_grads(prev, 2)
            da = da_all[...].astype(BF16)
            da_out[...] = da
            weight_copies()[1].wait()
            dw_enc[...] = dot(da, g_out[:n_enc, :], ((0,), (0,)))
            e_st[0]()
            c_st[0]()

        plan = [
            ((c_st[1], e_st[1]), ()),
            ((), (c_st[2], p_st[0])),
            ((e_st[2], p_st[1]), ()),
            ((e_st[3], q_st[0]), (
                r_st[0], p_st[2], q_st[1], r_st[1], c_st[3], p_st[3], r_st[2], q_st[2], e_st[4], c_st[4], q_st[3], r_st[3], p_st[4],
                q_st[4], r_st[4], p_st[5], e_st[5], q_st[5])),
        ]
        for part, (lo, hi) in enumerate(((0, 3 * LANES), (3 * LANES, n_j))):
            @pl.when(step > N_UTT)
            def _(lo=lo, hi=hi):
                cols = pl.ds(pl.multiple_of((step - N_UTT - 1) * W_CHUNK, W_CHUNK), W_CHUNK)
                dw_out[lo:hi, cols] = dot(h_all[:, lo:hi], dz_all[:, cols], ((0,), (0,)))

            for n, stages in enumerate(plan):
                if stages[part]:
                    @pl.when(step == N_UTT + 1 + n)
                    def _(stages=stages[part]):
                        for stage in stages:
                            stage()

        @pl.when(step == N_UTT + len(plan))
        def _():
            def put(src, dst, k):
                cp = pltpu.make_async_copy(src, dst, o_sem.at[k])
                cp.start()
                return cp

            def put_cols(lo, hi, k):
                return put(g_out.at[:, lo:hi], g_out_out.at[:, lo:hi], k)

            p_st[6]()
            puts = [put_cols(0, n_v // 2, 0)]
            r_st[5]()
            r_st[6]()
            puts.append(put_cols(n_v // 2 + n_v // 4, n_v, 1))
            e_st[6]()
            puts.append(put(g_enc, g_enc_out, 2))
            q_st[6]()
            puts.append(put_cols(n_v // 2, n_v // 2 + n_v // 4, 3))
            c_st[5]()
            puts.append(put(g_dc, g_dc_out, 4))
            far().wait_recv()
            for cp in links.copies:
                cp().wait_send()
            for cp in puts:
                cp.wait()


def joint_backward(labels, flen, llen, stat, norm, pred, z, h, w_out, enc):
    n_j, n_v = w_out.shape
    n_cell = N_UTT * UG * ROWS
    n_dc = N_UTT * N_UP
    full = lambda shape: pl.BlockSpec(shape, lambda i: (0,) * len(shape), pipeline_mode=pl.Buffered(1))
    return pl.pallas_call(
        backward_kernel,
        grid=(N_UTT + 1 + n_v // W_CHUNK,),
        in_specs=[pl.BlockSpec(memory_space=pltpu.SMEM)] * 3 + [full(stat.shape), full(norm.shape)] + [pl.BlockSpec(memory_space=pl.ANY)] * 5,
        out_specs=[full((SUB, LANES)), full((N_UTT * T_LOC, n_j))] + [pl.BlockSpec(memory_space=pl.ANY)] * 4,
        out_shape=[
            jax.ShapeDtypeStruct((SUB, LANES), F32),
            jax.ShapeDtypeStruct((N_UTT * T_LOC, n_j), BF16),
            jax.ShapeDtypeStruct((n_j, n_v), BF16),
            jax.ShapeDtypeStruct((n_j, n_v), BF16),
            jax.ShapeDtypeStruct((2 * n_dc, n_j), BF16),
            jax.ShapeDtypeStruct(pred.shape, BF16),
        ],
        scratch_shapes=[
            pltpu.VMEM((n_cell, n_v), BF16), pltpu.VMEM((n_cell, n_j), BF16), pltpu.VMEM((N_UTT * T_LOC, n_j), F32),
            pltpu.VMEM((n_j // LANES, ROWS, LANES), F32),
            *[pltpu.VMEM((ROWS, n_v), BF16)] * 3, *[pltpu.VMEM((ROWS, n_j), F32)] * 3,
            pltpu.VMEM((n_v, n_j + (-n_j) % 256), BF16), pltpu.VMEM((B_RING, UG, ROWS, n_v), F32),
            pltpu.VMEM((n_j, n_v), F32), pltpu.VMEM((n_j, n_v), F32), pltpu.VMEM((n_dc, n_j), F32),
            pltpu.VMEM((n_j, n_v), BF16), pltpu.VMEM((n_j, n_v), BF16), pltpu.VMEM((2 * n_dc, n_j), BF16),
            *sum_scratch(n_j, n_v) * 2, *sum_scratch(n_j, n_v // 2) * 2, *sum_scratch(n_j, n_v // 4) * 4,
            *[pltpu.VMEM((n_dc // 2, n_j), BF16), pltpu.VMEM((n_dc // 4, n_j), BF16)] * 2,
            *[pltpu.VMEM(norm.shape, F32)] * 3, pltpu.VMEM((N_SEQ - 1,) + stat.shape, F32),
            *[pltpu.VMEM(((N_DIAG + 2) * N_UP, LANES), F32)] * 4,
            pltpu.SemaphoreType.DMA((N_UTT,)), pltpu.SemaphoreType.DMA((B_RING,)), pltpu.SemaphoreType.DMA((5,)), pltpu.SemaphoreType.DMA((2,)),
            pltpu.SemaphoreType.DMA((N_COPY,)), pltpu.SemaphoreType.DMA((N_COPY,)),
        ],
        compiler_params=pltpu.CompilerParams(collective_id=1, has_side_effects=True, vmem_limit_bytes=VMEM_FULL),
        name="joint_backward",
    )(labels, flen, llen, stat, norm, pred, z, h.reshape(n_cell, n_j), w_out, enc)


def finish_kernel(loss, *refs):
    ins, o_loss, outs = refs[:FIN_IN], refs[FIN_IN], refs[FIN_IN + 1:FIN_IN + 1 + FIN_OUT]
    bufs, vals, in_sem, out_sem = refs[FIN_IN + 1 + FIN_OUT:-FIN_OUT - 2], refs[-FIN_OUT - 2:-2], refs[-2], refs[-1]
    g_dc, pred, pred_far, g_out, g_enc, w_pred, da, w_enc = bufs
    v_wpred, v_wout, v_wenc, v_pred, v_enc = vals
    loads = [pltpu.make_async_copy(src, dst, in_sem.at[k]) for k, (src, dst) in enumerate(zip(ins, bufs))]
    stores = [pltpu.make_async_copy(src, dst, out_sem.at[k]) for k, (src, dst) in enumerate(zip(vals, outs))]
    for cp in loads:
        cp.start()
    y = lax.axis_index("data")
    n_r = pred.shape[0]
    o_loss[...] = loss[0:1, :N_UTT]
    for k in range(3):
        loads[k].wait()
    dc_own = g_dc[rows_at(y * n_r, n_r), :]
    dc_far = g_dc[rows_at((1 - y) * n_r, n_r), :]
    v_wpred[...] = dot(pred[...], dc_own, ((0,), (0,))) + dot(pred_far[...], dc_far, ((0,), (0,)))
    stores[0].start()
    loads[3].wait()
    v_wout[...] = g_out[...].astype(F32)
    stores[1].start()
    loads[4].wait()
    v_wenc[...] = g_enc[...].astype(F32).T
    stores[2].start()
    loads[5].wait()
    v_pred[...] = dot(dc_own, w_pred[...], ((1,), (1,)))
    stores[3].start()
    loads[6].wait()
    loads[7].wait()
    v_enc[...] = dot(da[...], w_enc[...], ((1,), (1,))).astype(BF16)
    stores[4].start()
    for cp in stores:
        cp.wait()


FIN_IN = 8
FIN_OUT = 5


def finish(loss, g_enc, g_out, g_dc, pred, pred_far, w_pred, da, w_enc):
    vm = pl.BlockSpec(memory_space=pltpu.VMEM)
    hbm = pl.BlockSpec(memory_space=pl.ANY)
    ins = (g_dc, pred, pred_far, g_out, g_enc, w_pred, da, w_enc)
    outs = [(w_pred.shape, F32), (g_out.shape, F32), (w_enc.shape, F32), (pred.shape, F32), (pred.shape, BF16)]
    loss, grad_w_pred, grad_w_out, grad_w_enc, grad_pred, grad_enc = pl.pallas_call(
        finish_kernel,
        in_specs=[vm] + [hbm] * FIN_IN,
        out_specs=[vm] + [hbm] * FIN_OUT,
        out_shape=[jax.ShapeDtypeStruct((1, N_UTT), F32)] + [jax.ShapeDtypeStruct(*o) for o in outs],
        scratch_shapes=[pltpu.VMEM(v.shape, v.dtype) for v in ins] + [pltpu.VMEM(*o) for o in outs]
        + [pltpu.SemaphoreType.DMA((FIN_IN,)), pltpu.SemaphoreType.DMA((FIN_OUT,))],
        compiler_params=pltpu.CompilerParams(vmem_limit_bytes=VMEM_FULL),
        name="finish",
    )(loss, *ins)
    return loss, grad_enc, grad_pred, grad_w_enc, grad_w_pred, grad_w_out


def solution(mesh):
    utt_rows = P(("part", "data"))
    utt_mats = P(("part", "data"), None)
    utt_cube = P(("part", "data"), None, None)
    enc_spec = P(("part", "data"), "seq", None)
    weight_in = P(None, None)
    weight_out = P("part", None)

    def body(enc_loc, pred_loc, w_enc, w_pred, w_out, labels, frame_len, label_len):
        n_h = enc_loc.shape[2]
        enc2 = enc_loc.reshape(N_UTT * T_LOC, n_h)
        pred2 = pred_loc.reshape(N_UTT * N_UP, n_h)
        z, h, stat, norm = joint_forward(labels, label_len, enc2, pred2, w_enc, w_pred, w_out)
        loss, da, g_enc, g_out, g_dc, pred_far = joint_backward(labels, frame_len, label_len, stat, norm, pred2, z, h, w_out, enc2)
        loss, grad_enc, grad_pred, grad_w_enc, grad_w_pred, grad_w_out = finish(loss, g_enc, g_out, g_dc, pred2, pred_far, w_pred, da, w_enc)
        return loss.reshape(N_UTT), grad_enc.reshape(enc_loc.shape), grad_pred.reshape(pred_loc.shape), grad_w_enc, grad_w_pred, grad_w_out

    return jax.shard_map(body, mesh=mesh, in_specs=(enc_spec, utt_cube, weight_in, weight_in, weight_in, utt_mats, utt_rows, utt_rows), out_specs=(utt_rows, enc_spec, utt_cube, weight_out, weight_out, weight_out), check_vma=False)
```
